32 devices in a mesh: dp: 1 (over z), sp: 4 (over y), tp: 8 (over x, core).
Axes of the slice: x: 4, y: 4, z: 1, core: 2. Of those that a mesh axis runs over, the one named last changes fastest.
The devices are a block of a 4x4x8 slice.
Arguments:
- hidden: bfloat16 [256, 3072], P('dp')
- new_pos: int32 [256], P('dp')
- k_self: bfloat16 [256, 256, 8, 128], P('dp', 'sp', 'tp')
- v_self: bfloat16 [256, 256, 8, 128], P('dp', 'sp', 'tp')
- k_cross: bfloat16 [256, 512, 8, 128], P('dp', None, 'tp')
- v_cross: bfloat16 [256, 512, 8, 128], P('dp', None, 'tp')
- xvalid: int32 [256, 512], P('dp')
- rowmask: int32 [256], P('dp')
- self_attn_norm: bfloat16 [3072], replicated
- self_wq: bfloat16 [3072, 3072], P(None, 'tp')
- self_wk: bfloat16 [3072, 1024], P(None, 'tp')
- self_wv: bfloat16 [3072, 1024], P(None, 'tp')
- self_wo: bfloat16 [3072, 3072], P('tp')
- self_mlp_norm: bfloat16 [3072], replicated
- self_wgate: bfloat16 [3072, 8192], P(None, 'tp')
- self_wup: bfloat16 [3072, 8192], P(None, 'tp')
- self_wdown: bfloat16 [8192, 3072], P('tp')
- cross_attn_norm: bfloat16 [3072], replicated
- cross_wq: bfloat16 [3072, 3072], P(None, 'tp')
- cross_qnorm: bfloat16 [128], replicated
- cross_wo: bfloat16 [3072, 3072], P('tp')
- cross_gates: float32 [2], replicated
- cross_mlp_norm: bfloat16 [3072], replicated
- cross_wgate: bfloat16 [3072, 8192], P(None, 'tp')
- cross_wup: bfloat16 [3072, 8192], P(None, 'tp')
- cross_wdown: bfloat16 [8192, 3072], P('tp')
Outputs:
- output 1: bfloat16 [256, 3072], P('dp')
- output 2: bfloat16 [256, 256, 8, 128], P('dp', 'sp', 'tp')
- output 3: bfloat16 [256, 256, 8, 128], P('dp', 'sp', 'tp')
All inputs are finite; a program needn't handle non-finite values.
Results may differ from the reference program's by a relative error of at most 0.0147007.
Values sent between devices are 32-bit elements.
A program may use at most 768 MiB of HBM per device.

```python
import math
import jax
import jax.numpy as jnp
from jax import lax

BATCH = 256
SEQ_LEN = 256
VIS_TOKENS = 512
HIDDEN = 3072
HEADS = 24
KV_HEADS = 8
HEAD_DIM = 128
MLP_DIM = 8192

GROUP_SIZE = HEADS // KV_HEADS
Q_WIDTH = HEADS * HEAD_DIM
KV_WIDTH = KV_HEADS * HEAD_DIM
NORM_EPS = 1e-5
ROPE_THETA = 500000.0
ROPE_FACTOR = 8.0
LOW_FREQ = 1.0
HIGH_FREQ = 4.0
ORIG_CTX = 8192.0
NEG_BIG = -1e30
KEY_SCALE = 1.6


def rope_freqs():
    inv_freq = 1.0 / (ROPE_THETA ** (jnp.arange(0, HEAD_DIM, 2).astype(jnp.float32) / HEAD_DIM))
    wavelen = 2.0 * math.pi / inv_freq
    smooth = (ORIG_CTX / wavelen - LOW_FREQ) / (HIGH_FREQ - LOW_FREQ)
    mid_freq = (1.0 - smooth) * inv_freq / ROPE_FACTOR + smooth * inv_freq
    scaled = jnp.where(wavelen > ORIG_CTX / LOW_FREQ, inv_freq / ROPE_FACTOR, mid_freq)
    return jnp.where(wavelen < ORIG_CTX / HIGH_FREQ, inv_freq, scaled)


def apply_rope(vectors, positions):
    half_dim = HEAD_DIM // 2
    angles = positions.astype(jnp.float32)[:, None] * rope_freqs()[None, :]
    cos_t = jnp.cos(angles)[:, None, :]
    sin_t = jnp.sin(angles)[:, None, :]
    first_half = vectors[..., :half_dim]
    second_half = vectors[..., half_dim:]
    return jnp.concatenate([first_half * cos_t - second_half * sin_t, second_half * cos_t + first_half * sin_t], axis=-1)


def rms_norm(values, gain_vec):
    vals32 = values.astype(jnp.float32)
    inv_rms = lax.rsqrt(jnp.mean(vals32 * vals32, axis=-1, keepdims=True) + NORM_EPS)
    return (vals32 * inv_rms * gain_vec.astype(jnp.float32)).astype(jnp.bfloat16)


def gated_mlp(normed, w_gate, w_up, w_down):
    gate_val = jnp.dot(normed, w_gate, preferred_element_type=jnp.float32).astype(jnp.bfloat16)
    up_val = jnp.dot(normed, w_up, preferred_element_type=jnp.float32).astype(jnp.bfloat16)
    hidden_act = (jax.nn.silu(gate_val.astype(jnp.float32)) * up_val.astype(jnp.float32)).astype(jnp.bfloat16)
    return jnp.dot(hidden_act, w_down, preferred_element_type=jnp.float32)


def attend_row(queries, key_rows, val_rows, valid_mask):
    scores = jnp.einsum('kgd,tkd->kgt', queries.astype(jnp.float32), key_rows.astype(jnp.float32)) * (HEAD_DIM ** -0.5)
    scores = jnp.where(valid_mask[None, None, :], scores, NEG_BIG)
    weights = jax.nn.softmax(scores, axis=-1)
    return jnp.einsum('kgt,tkd->kgd', weights, val_rows.astype(jnp.float32))


def attend_item(item):
    return attend_row(item[0], item[1], item[2], item[3])


def dense_weight(rand_key, rows, cols):
    return (jax.random.normal(rand_key, (rows, cols), jnp.float32) * (rows ** -0.5)).astype(jnp.bfloat16)


def norm_gain(rand_key, width, center):
    return (center + 0.35 * jax.random.normal(rand_key, (width,), jnp.float32)).astype(jnp.bfloat16)


def drifting_values(rand_key, length):
    noise_key, walk_key, dir_key = jax.random.split(rand_key, 3)
    noise_part = 0.6 * jax.random.normal(noise_key, (BATCH, length, KV_HEADS, HEAD_DIM), jnp.float32)
    walk_path = jnp.cumsum(jax.random.normal(walk_key, (BATCH, KV_HEADS, length), jnp.float32), axis=-1) * (length ** -0.5)
    direction = jax.random.normal(dir_key, (BATCH, KV_HEADS, HEAD_DIM), jnp.float32)
    return (noise_part + jnp.transpose(walk_path, (0, 2, 1))[:, :, :, None] * direction[:, None, :, :]).astype(jnp.bfloat16)


def setup_inputs(seed: int = 0, part: int = 0) -> dict:
    data_keys = jax.random.split(jax.random.fold_in(jax.random.key(seed), part), 12)
    weight_keys = jax.random.split(jax.random.key(seed + 1), 20)
    row_ids = jnp.arange(BATCH)
    new_pos = jax.random.randint(data_keys[0], (BATCH,), SEQ_LEN // 4, SEQ_LEN)
    new_pos = jnp.where(row_ids == 0, SEQ_LEN - 1, new_pos).astype(jnp.int32)
    rowmask = (jax.random.randint(data_keys[1], (BATCH,), 0, 4) > 0).astype(jnp.int32)
    rowmask = jnp.where(row_ids == 0, 1, jnp.where(row_ids == 1, 0, rowmask)).astype(jnp.int32)
    valid_len = jax.random.randint(data_keys[2], (BATCH,), VIS_TOKENS // 4, VIS_TOKENS + 1)
    valid_len = jnp.where(row_ids == 0, VIS_TOKENS, valid_len)
    xvalid = (jnp.arange(VIS_TOKENS)[None, :] < valid_len[:, None]).astype(jnp.int32)
    hidden = jax.random.normal(data_keys[3], (BATCH, HIDDEN), jnp.float32).astype(jnp.bfloat16)
    k_self = (KEY_SCALE * jax.random.normal(data_keys[4], (BATCH, SEQ_LEN, KV_HEADS, HEAD_DIM), jnp.float32)).astype(jnp.bfloat16)
    v_self = drifting_values(data_keys[5], SEQ_LEN)
    k_cross = (KEY_SCALE * jax.random.normal(data_keys[6], (BATCH, VIS_TOKENS, KV_HEADS, HEAD_DIM), jnp.float32)).astype(jnp.bfloat16)
    v_cross = drifting_values(data_keys[7], VIS_TOKENS)
    return dict(
        hidden=hidden,
        new_pos=new_pos,
        k_self=k_self,
        v_self=v_self,
        k_cross=k_cross,
        v_cross=v_cross,
        xvalid=xvalid,
        rowmask=rowmask,
        self_attn_norm=norm_gain(weight_keys[0], HIDDEN, 1.0),
        self_wq=dense_weight(weight_keys[1], HIDDEN, Q_WIDTH),
        self_wk=dense_weight(weight_keys[2], HIDDEN, KV_WIDTH),
        self_wv=dense_weight(weight_keys[3], HIDDEN, KV_WIDTH),
        self_wo=dense_weight(weight_keys[4], Q_WIDTH, HIDDEN),
        self_mlp_norm=norm_gain(weight_keys[5], HIDDEN, 1.0),
        self_wgate=dense_weight(weight_keys[6], HIDDEN, MLP_DIM),
        self_wup=dense_weight(weight_keys[7], HIDDEN, MLP_DIM),
        self_wdown=dense_weight(weight_keys[8], MLP_DIM, HIDDEN),
        cross_attn_norm=norm_gain(weight_keys[9], HIDDEN, 1.0),
        cross_wq=dense_weight(weight_keys[10], HIDDEN, Q_WIDTH),
        cross_qnorm=norm_gain(weight_keys[11], HEAD_DIM, 1.5),
        cross_wo=dense_weight(weight_keys[12], Q_WIDTH, HIDDEN),
        cross_gates=jax.random.uniform(weight_keys[13], (2,), jnp.float32, 0.5, 1.5),
        cross_mlp_norm=norm_gain(weight_keys[14], HIDDEN, 1.0),
        cross_wgate=dense_weight(weight_keys[15], HIDDEN, MLP_DIM),
        cross_wup=dense_weight(weight_keys[16], HIDDEN, MLP_DIM),
        cross_wdown=dense_weight(weight_keys[17], MLP_DIM, HIDDEN),
    )


def reference(hidden, new_pos, k_self, v_self, k_cross, v_cross, xvalid, rowmask,
              self_attn_norm, self_wq, self_wk, self_wv, self_wo, self_mlp_norm,
              self_wgate, self_wup, self_wdown, cross_attn_norm, cross_wq, cross_qnorm,
              cross_wo, cross_gates, cross_mlp_norm, cross_wgate, cross_wup, cross_wdown):
    normed = rms_norm(hidden, self_attn_norm)
    queries = jnp.dot(normed, self_wq, preferred_element_type=jnp.float32).astype(jnp.bfloat16)
    key_new = jnp.dot(normed, self_wk, preferred_element_type=jnp.float32).astype(jnp.bfloat16)
    val_new = jnp.dot(normed, self_wv, preferred_element_type=jnp.float32).astype(jnp.bfloat16)
    queries = apply_rope(queries.reshape(BATCH, HEADS, HEAD_DIM).astype(jnp.float32), new_pos).astype(jnp.bfloat16)
    key_new = apply_rope(key_new.reshape(BATCH, KV_HEADS, HEAD_DIM).astype(jnp.float32), new_pos).astype(jnp.bfloat16)
    val_new = val_new.reshape(BATCH, KV_HEADS, HEAD_DIM)
    slot_ids = jnp.arange(SEQ_LEN)
    hit_mask = (slot_ids[None, :] == new_pos[:, None])[:, :, None, None]
    k_new_cache = jnp.where(hit_mask, key_new[:, None], k_self)
    v_new_cache = jnp.where(hit_mask, val_new[:, None], v_self)
    seen_mask = slot_ids[None, :] <= new_pos[:, None]
    self_out = lax.map(attend_item, (queries.reshape(BATCH, KV_HEADS, GROUP_SIZE, HEAD_DIM), k_new_cache, v_new_cache, seen_mask))
    self_flat = self_out.astype(jnp.bfloat16).reshape(BATCH, Q_WIDTH)
    after_attn = (hidden.astype(jnp.float32) + jnp.dot(self_flat, self_wo, preferred_element_type=jnp.float32)).astype(jnp.bfloat16)
    mlp_out = gated_mlp(rms_norm(after_attn, self_mlp_norm), self_wgate, self_wup, self_wdown)
    after_mlp = (after_attn.astype(jnp.float32) + mlp_out).astype(jnp.bfloat16)
    normed = rms_norm(after_mlp, cross_attn_norm)
    cross_q = jnp.dot(normed, cross_wq, preferred_element_type=jnp.float32).astype(jnp.bfloat16)
    cross_q = rms_norm(cross_q.reshape(BATCH, HEADS, HEAD_DIM), cross_qnorm)
    cross_out = lax.map(attend_item, (cross_q.reshape(BATCH, KV_HEADS, GROUP_SIZE, HEAD_DIM), k_cross, v_cross, xvalid > 0))
    cross_flat = cross_out.astype(jnp.bfloat16).reshape(BATCH, Q_WIDTH)
    gate_vals = jnp.tanh(cross_gates.astype(jnp.float32))
    row_scale = rowmask.astype(jnp.float32)[:, None]
    cross_proj = jnp.dot(cross_flat, cross_wo, preferred_element_type=jnp.float32)
    after_cross = (after_mlp.astype(jnp.float32) + gate_vals[0] * row_scale * cross_proj).astype(jnp.bfloat16)
    xmlp_out = gated_mlp(rms_norm(after_cross, cross_mlp_norm), cross_wgate, cross_wup, cross_wdown)
    after_xmlp = (after_cross.astype(jnp.float32) + gate_vals[1] * row_scale * xmlp_out).astype(jnp.bfloat16)
    return (after_xmlp, k_new_cache, v_new_cache)
```

```python
import functools
import math
import jax
import jax.numpy as jnp
from jax import lax
from jax.experimental import pallas as pl
from jax.experimental.pallas import tpu as pltpu
from jax.sharding import PartitionSpec as P

NORM_EPS = 1e-5
ROPE_THETA = 500000.0
ROPE_FACTOR = 8.0
LOW_FREQ = 1.0
HIGH_FREQ = 4.0
ORIG_CTX = 8192.0
NEG_BIG = -1e30
NC = 4
MESH = pl.DeviceIdType.MESH


def rope_freqs(head_dim):
    inv_freq = 1.0 / (ROPE_THETA ** (jnp.arange(0, head_dim, 2).astype(jnp.float32) / head_dim))
    wavelen = 2.0 * math.pi / inv_freq
    smooth = (ORIG_CTX / wavelen - LOW_FREQ) / (HIGH_FREQ - LOW_FREQ)
    mid_freq = (1.0 - smooth) * inv_freq / ROPE_FACTOR + smooth * inv_freq
    scaled = jnp.where(wavelen > ORIG_CTX / LOW_FREQ, inv_freq / ROPE_FACTOR, mid_freq)
    return jnp.where(wavelen < ORIG_CTX / HIGH_FREQ, inv_freq, scaled)


def apply_rope(vectors, positions):
    head_dim = vectors.shape[-1]
    half_dim = head_dim // 2
    angles = positions.astype(jnp.float32)[:, None] * rope_freqs(head_dim)[None, :]
    cos_t = jnp.cos(angles)[:, None, :]
    sin_t = jnp.sin(angles)[:, None, :]
    first_half = vectors[..., :half_dim]
    second_half = vectors[..., half_dim:]
    return jnp.concatenate([first_half * cos_t - second_half * sin_t, second_half * cos_t + first_half * sin_t], axis=-1)


def rms_norm(values, gain_vec):
    vals32 = values.astype(jnp.float32)
    inv_rms = lax.rsqrt(jnp.mean(vals32 * vals32, axis=-1, keepdims=True) + NORM_EPS)
    return (vals32 * inv_rms * gain_vec.astype(jnp.float32)).astype(jnp.bfloat16)


def local_softmax(queries, key_rows, val_rows, valid_mask, score_scale):
    scores = jnp.einsum('bkgd,btkd->bkgt', queries, key_rows, preferred_element_type=jnp.float32) * score_scale
    scores = jnp.where(valid_mask, scores, NEG_BIG)
    part_max = jnp.max(scores, axis=-1)
    probs_loc = jnp.where(valid_mask, jnp.exp(scores - part_max[..., None]), 0.0)
    part_sum = jnp.sum(probs_loc, axis=-1)
    part_out = jnp.einsum('bkgt,btkd->bkgd', probs_loc.astype(jnp.bfloat16), val_rows, preferred_element_type=jnp.float32)
    return part_max, part_sum, part_out


def fdot(a, b):
    return jnp.dot(a, b, preferred_element_type=jnp.float32)


def tail_kernel(cfg, blk_h, hid_h, gains_v, rowm_v, gate_s, xv_h, kc_h, vc_h,
                wo_h, wg_h, wu_h, wd_h, cq_h, cwo_h, cg_h, cu_h, cd_h, out_v,
                bk, yr, yd, yt, yf, ob, hrow, hst,
                wo_v, wg_v, wu_v, wd_v, cq_v, cwo_v, kc_v, vc_v, xv_v,
                pbuf, dbuf, sbuf, rbuf, ebuf, tbuf, fbuf, xa, og, acc, act, q3, oc,
                ld_sem, w_sem, kv_sem, ys, yrs, rs_s, rs_r, ag_s, ag_r, fg_s, fg_r):
    heads, hd, dim, mlp, ntok = cfg
    cw = dim // NC
    hw = heads * hd
    half = 32
    x = lax.axis_index('tp') // 2
    c = lax.axis_index('tp') % 2
    y = lax.axis_index('sp')
    slot = c * 4 + x
    scale = hd ** -0.5

    def ring(v):
        return lax.rem(v + 8, 4)

    def xdev(d):
        return {'tp': 2 * ring(x + d) + c}

    def ydev(d):
        return {'sp': ring(y + d)}

    sib = {'tp': 2 * x + 1 - c}

    def rcopy(src, dst, ss, rs, dev):
        return pltpu.make_async_remote_copy(src_ref=src, dst_ref=dst, send_sem=ss, recv_sem=rs,
                                            device_id=dev, device_id_type=MESH)

    def loop(n, body):
        def step(i, carry):
            body(i)
            return carry
        lax.fori_loop(0, n, step, 0)

    blk_cp = pltpu.make_async_copy(blk_h, bk, ld_sem.at[0])
    hid_cp = pltpu.make_async_copy(hid_h.at[y * 8 + slot], hrow, ld_sem.at[1])
    xv_cp = pltpu.make_async_copy(xv_h.at[y], xv_v, ld_sem.at[2])

    def cols(h, v, k, j):
        return pltpu.make_async_copy(h.at[:, pl.ds(pl.multiple_of(j * cw, 128), cw)], v.at[j], w_sem.at[k, j])

    def rows(h, v, k, j):
        return pltpu.make_async_copy(h.at[pl.ds(pl.multiple_of(j * cw, 128), cw)], v.at[j], w_sem.at[k, j])

    def ld_wo(j):
        return cols(wo_h, wo_v, 0, j)

    def ld_wg(j):
        return rows(wg_h, wg_v, 1, j)

    def ld_wu(j):
        return rows(wu_h, wu_v, 2, j)

    def ld_wd(j):
        return cols(wd_h, wd_v, 3, j)

    def ld_cq(j):
        return rows(cq_h, cq_v, 4, j)

    def ld_cwo(j):
        return cols(cwo_h, cwo_v, 5, j)

    def ld_cg(j):
        return rows(cg_h, wg_v, 6, j)

    def ld_cu(j):
        return rows(cu_h, wu_v, 7, j)

    def ld_cd(j):
        return cols(cd_h, wd_v, 8, j)

    def ld_kc(g):
        return pltpu.make_async_copy(kc_h.at[y, pl.ds(g * 8, 8)], kc_v.at[pl.ds(g * 8, 8)], kv_sem.at[0, g])

    def ld_vc(g):
        return pltpu.make_async_copy(vc_h.at[y, pl.ds(g * 8, 8)], vc_v.at[pl.ds(g * 8, 8)], kv_sem.at[1, g])

    blk_cp.start()
    hid_cp.start()
    xv_cp.start()
    loop(NC, lambda j: ld_wo(j).start())

    barrier = pltpu.get_barrier_semaphore()
    for dev in (sib, xdev(1), xdev(-1), ydev(1), ydev(-1)):
        pl.semaphore_signal(barrier, inc=1, device_id=dev, device_id_type=MESH)

    def start_gu(j):
        ld_wg(j).start()
        ld_wu(j).start()

    loop(NC, start_gu)
    loop(NC, lambda j: ld_wd(j).start())
    loop(NC, lambda j: ld_cq(j).start())

    def start_kv(g):
        ld_kc(g).start()
        ld_vc(g).start()

    loop(8, start_kv)
    loop(NC, lambda j: ld_cwo(j).start())
    q3[...] = jnp.zeros_like(q3)
    pl.semaphore_wait(barrier, 5)

    lane = lax.broadcasted_iota(jnp.int32, (half, hd), 1)

    def merge(a, b):
        outs, ms, ls = [], [], []
        for h in range(heads):
            ma, mb = a[:, hw + h:hw + h + 1], b[:, hw + h:hw + h + 1]
            la, lb = a[:, hw + 8 + h:hw + 9 + h], b[:, hw + 8 + h:hw + 9 + h]
            mm = jnp.maximum(ma, mb)
            ea, eb = jnp.exp(ma - mm), jnp.exp(mb - mm)
            outs.append(a[:, h * hd:(h + 1) * hd] * ea + b[:, h * hd:(h + 1) * hd] * eb)
            ms.append(mm)
            ls.append(la * ea + lb * eb)
        stat = jnp.zeros((half, hd), jnp.float32)
        for h in range(heads):
            stat = jnp.where(lane == h, ms[h], stat)
            stat = jnp.where(lane == 8 + h, ls[h], stat)
        return jnp.concatenate(outs + [stat], axis=1), ls

    def y_relay(j, d):
        return rcopy(bk.at[ring(y + 2), j], yr.at[j], ys.at[0, j], yrs.at[0, j], ydev(d))

    def y_direct(j, d):
        return rcopy(bk.at[ring(y - d), j], yd.at[j], ys.at[1, j], yrs.at[1, j], ydev(-d))

    def y_final(j, d):
        return rcopy(yt.at[j], yf.at[j], ys.at[2, j], yrs.at[2, j], ydev(d))

    blk_cp.wait()
    for j, d in ((0, 1), (1, -1)):
        y_relay(j, d).start()
    for j, d in ((0, 1), (1, -1)):
        y_direct(j, d).start()
    for j, d in ((0, 1), (1, -1)):
        y_relay(j, d).wait_recv()
        yt[j] = merge(bk[ring(y + d), j], yr[j])[0]
        y_final(j, d).start()
    for j, d in ((0, 1), (1, -1)):
        y_direct(j, d).wait_recv()
        first = merge(bk[y, j], yd[j])[0]
        y_final(j, d).wait_recv()
        both, sums = merge(first, yf[j])
        for h in range(heads):
            ob[j * half:(j + 1) * half, h * hd:(h + 1) * hd] = (both[:, h * hd:(h + 1) * hd] / sums[h]).astype(jnp.bfloat16)

    def rs_pair(p, j):
        return rcopy(pbuf.at[p, j, 1 - c], dbuf.at[p, j], rs_s.at[p, 0, j], rs_r.at[p, 0, j], sib)

    def turn(j):
        return 1 - 2 * lax.rem(j, 2)

    def rs_relay(p, j):
        return rcopy(sbuf.at[p, j, ring(x + 2)], rbuf.at[p, j], rs_s.at[p, 1, j], rs_r.at[p, 1, j], xdev(turn(j)))

    def rs_direct(p, j):
        return rcopy(sbuf.at[p, j, ring(x - turn(j))], ebuf.at[p, j], rs_s.at[p, 2, j], rs_r.at[p, 2, j], xdev(-turn(j)))

    def rs_final(p, j):
        return rcopy(tbuf.at[p, j], fbuf.at[p, j], rs_s.at[p, 3, j], rs_r.at[p, 3, j], xdev(turn(j)))

    def reduce_scatter(p, partial):
        def second(j):
            rs_pair(p, j).wait_recv()
            sbuf[p, j] = (pbuf[p, j, c] + dbuf[p, j]).reshape(4, 8, cw)
            rs_relay(p, j).start()
            rs_direct(p, j).start()

        def body(j):
            @pl.when(j < NC)
            def _():
                pbuf[p, j] = partial(j).reshape(2, half, cw)
                rs_pair(p, j).start()

            @pl.when(j >= 1)
            def _():
                second(j - 1)

        loop(NC + 1, body)

        def third(j):
            rs_relay(p, j).wait_recv()
            tbuf[p, j] = sbuf[p, j, ring(x + turn(j))] + rbuf[p, j]
            rs_final(p, j).start()

        loop(NC, third)

    def reduced(p, j):
        rs_direct(p, j).wait_recv()
        rs_final(p, j).wait_recv()
        return sbuf[p, j, x] + ebuf[p, j] + fbuf[p, j]

    def new_rows(p, factor):
        sq = jnp.zeros((8, 1), jnp.float32)
        for j in range(NC):
            add = reduced(p, j)
            if factor is not None:
                add = factor * add
            old = hrow[:, j * cw:(j + 1) * cw].astype(jnp.float32) if p == 0 else hst[j]
            new = (old + add).astype(jnp.bfloat16).astype(jnp.float32)
            hst[j] = new
            sq = sq + jnp.sum(new * new, axis=1, keepdims=True)
        return sq

    def ag_send(q, j, s, k, dev):
        return rcopy(xa.at[q, j, s], xa.at[q, j, s], ag_s.at[q, j, k], ag_r.at[q, j, s], dev)

    def ag_got(q, j, s):
        return rcopy(xa.at[q, j, s], xa.at[q, j, s], ag_s.at[q, j, 0], ag_r.at[q, j, s], sib)

    def at(d):
        return c * 4 + ring(x + d)

    def ag_copy(q, j, i):
        d = turn(j)
        s = (0, 0, 0, -d, -d, d, 2)[i]
        dev = (xdev(d), xdev(-d), sib, xdev(d), sib, sib, sib)[i]
        return ag_send(q, j, slot if i < 3 else at(s), i, dev)

    def all_gather(q, sq, gain_row, consume):
        inv = lax.rsqrt(sq / dim + NORM_EPS)
        for j in range(NC):
            gain = gains_v[gain_row:gain_row + 1, j * cw:(j + 1) * cw]
            xa[q, j, slot] = (hst[j] * inv * gain).astype(jnp.bfloat16).astype(jnp.float32)
            for k in range(3):
                ag_copy(q, j, k).start()

        def first(j):
            d = turn(j)
            ag_got(q, j, at(-d)).wait_recv()
            ag_copy(q, j, 3).start()
            ag_copy(q, j, 4).start()
            ag_got(q, j, at(d)).wait_recv()
            ag_copy(q, j, 5).start()

        loop(NC, first)

        def body(j):
            @pl.when(j < NC)
            def _():
                ag_got(q, j, at(2)).wait_recv()
                ag_copy(q, j, 6).start()

            @pl.when(j >= 1)
            def _():
                for k in range(4):
                    ag_got(q, j - 1, (1 - c) * 4 + k).wait_recv()
                consume(j - 1, xa[q, j - 1].reshape(2 * half, cw).astype(jnp.bfloat16))

        loop(NC + 1, body)

    def mlp_hidden(q, sq, gain_row, wait_gu):
        acc[...] = jnp.zeros_like(acc)

        def consume(j, xs):
            wait_gu(j)
            acc[:, :mlp] += fdot(xs, wg_v[j])
            acc[:, mlp:] += fdot(xs, wu_v[j])

        all_gather(q, sq, gain_row, consume)
        gv = acc[:, :mlp].astype(jnp.bfloat16).astype(jnp.float32)
        uv = acc[:, mlp:].astype(jnp.bfloat16).astype(jnp.float32)
        act[...] = (jax.nn.silu(gv) * uv).astype(jnp.bfloat16)

    def part_wo(j):
        ld_wo(j).wait()
        return fdot(ob[...], wo_v[j])

    reduce_scatter(0, part_wo)
    hid_cp.wait()
    sq = new_rows(0, None)

    def wait_self(j):
        ld_wg(j).wait()
        ld_wu(j).wait()

    mlp_hidden(0, sq, 0, wait_self)

    def start_cgu(j):
        ld_cg(j).start()
        ld_cu(j).start()

    loop(NC, start_cgu)

    def part_wd(j):
        ld_wd(j).wait()
        return fdot(act[...], wd_v[j])

    reduce_scatter(1, part_wd)
    loop(NC, lambda j: ld_cd(j).start())
    sq = new_rows(1, None)

    acc[:, :hw] = jnp.zeros((2 * half, hw), jnp.float32)

    def consume_q(j, xs):
        ld_cq(j).wait()
        acc[:, :hw] += fdot(xs, cq_v[j])

    all_gather(1, sq, 1, consume_q)
    qgain = gains_v[3:4, :hd]
    for h in range(heads):
        qh = acc[:, h * hd:(h + 1) * hd].astype(jnp.bfloat16).astype(jnp.float32)
        qinv = lax.rsqrt(jnp.mean(qh * qh, axis=1, keepdims=True) + NORM_EPS)
        q3[:, h, :] = (qh * qinv * qgain).astype(jnp.bfloat16).astype(jnp.float32)
    xv_cp.wait()

    def attend(g):
        ld_kc(g).wait()
        ld_vc(g).wait()
        xv = xv_v[pl.ds(pl.multiple_of(g * 8, 8), 8), :]
        for i in range(8):
            b = g * 8 + i
            sc = lax.dot_general(q3[b].astype(jnp.bfloat16), kc_v[b], (((1,), (1,)), ((), ())),
                                 preferred_element_type=jnp.float32) * scale
            valid = jnp.broadcast_to(xv[i:i + 1], (8, ntok)) > 0
            sc = jnp.where(valid, sc, NEG_BIG)
            mx = jnp.max(sc, axis=1, keepdims=True)
            pr = jnp.where(valid, jnp.exp(sc - mx), 0.0)
            ls = jnp.sum(pr, axis=1, keepdims=True)
            oc[b] = fdot(pr.astype(jnp.bfloat16), vc_v[b]) / ls

    loop(8, attend)
    for h in range(heads):
        ob[:, h * hd:(h + 1) * hd] = oc[:, h, :].astype(jnp.bfloat16)

    def part_cwo(j):
        ld_cwo(j).wait()
        return fdot(ob[...], cwo_v[j])

    reduce_scatter(2, part_cwo)
    nrow = rowm_v.shape[1]
    mine = (y * 8 + slot) * 8 + lax.broadcasted_iota(jnp.int32, (8, nrow), 0)
    pick = lax.broadcasted_iota(jnp.int32, (8, nrow), 1) == mine
    rmask = jnp.sum(jnp.where(pick, jnp.broadcast_to(rowm_v[...], (8, nrow)), 0).astype(jnp.float32), axis=1, keepdims=True)
    factor = [jnp.tanh(jnp.full((8, 128), gate_s[k], jnp.float32))[:, :1] * rmask for k in range(2)]
    sq = new_rows(2, factor[0])

    def wait_cross(j):
        ld_cg(j).wait()
        ld_cu(j).wait()

    mlp_hidden(2, sq, 2, wait_cross)

    def part_cd(j):
        ld_cd(j).wait()
        return fdot(act[...], wd_v[j])

    reduce_scatter(3, part_cd)
    new_rows(3, factor[1])

    def parts_of(j):
        if j < NC // 2:
            return (lambda k: og.at[j, c, y, ring(x + k)], xdev), (lambda k: og.at[j, c, ring(y + k)], ydev)
        return (lambda k: og.at[j, c, ring(y + k), x], ydev), (lambda k: og.at[j, c, :, ring(x + k)], xdev)

    def fg(j, stage, k, s, what, dev):
        return rcopy(what, what, fg_s.at[j, stage, s], fg_r.at[j, stage, k], dev)

    fg_all = []
    plans = []
    for j in range(NC):
        d = 1 - 2 * (j % 2)
        stages = []
        for stage, (region, dev) in enumerate(parts_of(j)):
            stages.append(dict(
                own=[fg(j, stage, 0, 0, region(0), dev(d)), fg(j, stage, 1, 1, region(0), dev(-d))],
                relay=fg(j, stage, 2, 2, region(-d), dev(d)),
                got=[fg(j, stage, 0, 0, region(-d), sib), fg(j, stage, 1, 1, region(d), sib), fg(j, stage, 2, 2, region(2), sib)],
                pair=[fg(j, 2, i, i, region(k), sib) for i, k in enumerate((0, -d, d, 2))],
            ))
        plans.append(stages)
    order = []
    for j in range(NC // 2):
        order += [j, j + NC // 2]
    for j in order:
        og[j, c, y, x] = hst[j]
        for cp in plans[j][0]['own']:
            cp.start()
    for j in order:
        st = plans[j][0]
        st['got'][0].wait_recv()
        st['relay'].start()
    for j in order:
        st, nx = plans[j]
        st['got'][1].wait_recv()
        st['got'][2].wait_recv()
        for cp in nx['own']:
            cp.start()
        nx['pair'][0].start()
    for j in order:
        st = plans[j][1]
        st['got'][0].wait_recv()
        st['relay'].start()
        st['pair'][1].start()
        st['got'][1].wait_recv()
        st['pair'][2].start()
    for j in order:
        st = plans[j][1]
        st['got'][2].wait_recv()
        st['pair'][3].start()
    for j in order:
        for cp in plans[j][1]['pair']:
            cp.wait_recv()
        for yy in range(4):
            for cc in range(2):
                out_v[yy * 8 + cc * 4:yy * 8 + cc * 4 + 4, :, j * cw:(j + 1) * cw] = og[j, cc, yy].astype(jnp.bfloat16)

    for j, d in ((0, 1), (1, -1)):
        y_relay(j, d).wait_send()
        y_direct(j, d).wait_send()
        y_final(j, d).wait_send()

    def drain_rs(j):
        for p in range(4):
            rs_pair(p, j).wait_send()
            rs_relay(p, j).wait_send()
            rs_direct(p, j).wait_send()
            rs_final(p, j).wait_send()
        for q in range(3):
            for i in range(7):
                ag_copy(q, j, i).wait_send()

    loop(NC, drain_rs)
    for j in range(NC):
        for st in plans[j]:
            for cp in st['own']:
                cp.wait_send()
            st['relay'].wait_send()
        for cp in plans[j][1]['pair']:
            cp.wait_send()


def tail(blk, hidden, gains, rowmask, gates, xvalid, k_cross, v_cross, wo, wg, wu, wd, cq, cwo, cg, cu, cd, heads, hd):
    batch, dim = hidden.shape
    mlp = wg.shape[1]
    ntok = xvalid.shape[1]
    cw = dim // NC
    hw = heads * hd
    bl = batch // 4
    half = bl // 2
    f32, bf16 = jnp.float32, jnp.bfloat16
    anyspec = pl.BlockSpec(memory_space=pl.ANY)
    vmem = pl.BlockSpec(memory_space=pltpu.VMEM)
    smem = pl.BlockSpec(memory_space=pltpu.SMEM)
    dma = pltpu.SemaphoreType.DMA
    scratch = [
        pltpu.VMEM((4, 2, half, hw + hd), f32),
        pltpu.VMEM((2, half, hw + hd), f32),
        pltpu.VMEM((2, half, hw + hd), f32),
        pltpu.VMEM((2, half, hw + hd), f32),
        pltpu.VMEM((2, half, hw + hd), f32),
        pltpu.VMEM((bl, hw), bf16),
        pltpu.VMEM((8, dim), bf16),
        pltpu.VMEM((NC, 8, cw), f32),
        pltpu.VMEM((NC, hw, cw), bf16),
        pltpu.VMEM((NC, cw, mlp), bf16),
        pltpu.VMEM((NC, cw, mlp), bf16),
        pltpu.VMEM((NC, mlp, cw), bf16),
        pltpu.VMEM((NC, cw, hw), bf16),
        pltpu.VMEM((NC, hw, cw), bf16),
        pltpu.VMEM((bl, ntok, hd), bf16),
        pltpu.VMEM((bl, ntok, hd), bf16),
        pltpu.VMEM((bl, ntok), jnp.int32),
        pltpu.VMEM((4, NC, 2, half, cw), f32),
        pltpu.VMEM((4, NC, half, cw), f32),
        pltpu.VMEM((4, NC, 4, 8, cw), f32),
        pltpu.VMEM((4, NC, 8, cw), f32),
        pltpu.VMEM((4, NC, 8, cw), f32),
        pltpu.VMEM((4, NC, 8, cw), f32),
        pltpu.VMEM((4, NC, 8, cw), f32),
        pltpu.VMEM((3, NC, 8, 8, cw), f32),
        pltpu.VMEM((NC, 2, 4, 4, 8, cw), f32),
        pltpu.VMEM((bl, 2 * mlp), f32),
        pltpu.VMEM((bl, mlp), bf16),
        pltpu.VMEM((bl, 8, hd), f32),
        pltpu.VMEM((bl, 8, hd), f32),
        dma((3,)),
        dma((9, NC)),
        dma((2, 8)),
        dma((3, 2)),
        dma((3, 2)),
        dma((4, 4, NC)),
        dma((4, 4, NC)),
        dma((3, NC, 7)),
        dma((3, NC, 8)),
        dma((NC, 3, 4)),
        dma((NC, 3, 4)),
    ]
    out = pl.pallas_call(
        functools.partial(tail_kernel, (heads, hd, dim, mlp, ntok)),
        out_shape=jax.ShapeDtypeStruct((batch // 8, 8, dim), bf16),
        in_specs=[anyspec, anyspec, vmem, vmem, smem] + [anyspec] * 12,
        out_specs=vmem,
        scratch_shapes=scratch,
        compiler_params=pltpu.CompilerParams(collective_id=0, has_side_effects=True, vmem_limit_bytes=67043328),
        name='tail',
    )(blk.reshape(4, 2, half, hw + hd), hidden.reshape(batch // 8, 8, dim), gains, rowmask.reshape(1, batch), gates,
      xvalid.reshape(4, bl, ntok), k_cross.reshape(4, bl, ntok, hd), v_cross.reshape(4, bl, ntok, hd),
      wo, wg, wu, wd, cq, cwo, cg, cu, cd)
    return out.reshape(batch, dim)


def solution(mesh):
    cache_spec = P('dp', 'sp', 'tp', None)
    cross_spec = P('dp', None, 'tp', None)
    row_spec = P('dp', None)
    vec_spec = P('dp')
    full_spec = P(None)
    col_spec = P(None, 'tp')
    split_rows = P('tp', None)
    in_specs = (row_spec, vec_spec, cache_spec, cache_spec, cross_spec, cross_spec, row_spec, vec_spec,
                full_spec, col_spec, col_spec, col_spec, split_rows, full_spec, col_spec, col_spec, split_rows,
                full_spec, col_spec, full_spec, split_rows, full_spec, full_spec, col_spec, col_spec, split_rows)
    out_specs = (row_spec, cache_spec, cache_spec)

    def local_step(hidden, new_pos, k_self, v_self, k_cross, v_cross, xvalid, rowmask,
                   self_attn_norm, self_wq, self_wk, self_wv, self_wo, self_mlp_norm,
                   self_wgate, self_wup, self_wdown, cross_attn_norm, cross_wq, cross_qnorm,
                   cross_wo, cross_gates, cross_mlp_norm, cross_wgate, cross_wup, cross_wdown):
        batch_rows = hidden.shape[0]
        len_local = k_self.shape[1]
        kv_local = k_self.shape[2]
        head_dim = k_self.shape[3]
        heads_local = self_wq.shape[1] // head_dim
        group_size = heads_local // kv_local
        score_scale = head_dim ** -0.5
        normed = rms_norm(hidden, self_attn_norm)
        queries = jnp.dot(normed, self_wq, preferred_element_type=jnp.float32).astype(jnp.bfloat16)
        key_new = jnp.dot(normed, self_wk, preferred_element_type=jnp.float32).astype(jnp.bfloat16)
        val_new = jnp.dot(normed, self_wv, preferred_element_type=jnp.float32).astype(jnp.bfloat16)
        queries = apply_rope(queries.reshape(batch_rows, heads_local, head_dim).astype(jnp.float32), new_pos).astype(jnp.bfloat16)
        key_new = apply_rope(key_new.reshape(batch_rows, kv_local, head_dim).astype(jnp.float32), new_pos).astype(jnp.bfloat16)
        val_new = val_new.reshape(batch_rows, kv_local, head_dim)
        local_pos = new_pos - lax.axis_index('sp') * len_local
        slot_ids = jnp.arange(len_local)
        hit_mask = (slot_ids[None, :] == local_pos[:, None])[:, :, None, None]
        k_new_cache = jnp.where(hit_mask, key_new[:, None], k_self)
        v_new_cache = jnp.where(hit_mask, val_new[:, None], v_self)
        seen_mask = (slot_ids[None, :] <= local_pos[:, None])[:, None, None, :]
        m, l, o = local_softmax(queries.reshape(batch_rows, kv_local, group_size, head_dim), k_new_cache, v_new_cache, seen_mask, score_scale)
        pad = jnp.zeros((batch_rows, 8 - heads_local), jnp.float32)
        blk = jnp.concatenate([o.reshape(batch_rows, -1), m.reshape(batch_rows, -1), pad, l.reshape(batch_rows, -1),
                               jnp.zeros((batch_rows, head_dim - 8 - heads_local), jnp.float32)], axis=1)
        dim = hidden.shape[1]
        gains = jnp.stack([self_mlp_norm, cross_attn_norm, cross_mlp_norm,
                           jnp.pad(cross_qnorm, (0, dim - head_dim))]).astype(jnp.float32)
        h4 = tail(blk, hidden, gains, rowmask, cross_gates, xvalid, k_cross, v_cross, self_wo, self_wgate, self_wup, self_wdown,
                  cross_wq, cross_wo, cross_wgate, cross_wup, cross_wdown, heads_local, head_dim)
        return h4, k_new_cache, v_new_cache

    return jax.shard_map(local_step, mesh=mesh, in_specs=in_specs, out_specs=out_specs, check_vma=False)
```

```python
import functools
import math
import jax
import jax.numpy as jnp
import numpy as np
from jax import lax
from jax.experimental import pallas as pl
from jax.experimental.pallas import tpu as pltpu
from jax.sharding import PartitionSpec as P

NORM_EPS = 1e-5
ROPE_THETA = 500000.0
ROPE_FACTOR = 8.0
LOW_FREQ = 1.0
HIGH_FREQ = 4.0
ORIG_CTX = 8192.0
NEG_BIG = -1e30
NC = 4
MESH = pl.DeviceIdType.MESH


def rope_freqs(head_dim):
    inv_freq = (1.0 / (ROPE_THETA ** (np.arange(0, head_dim, 2).astype(np.float32) / np.float32(head_dim)))).astype(np.float32)
    wavelen = 2.0 * math.pi / inv_freq
    smooth = (ORIG_CTX / wavelen - LOW_FREQ) / (HIGH_FREQ - LOW_FREQ)
    mid_freq = (1.0 - smooth) * inv_freq / ROPE_FACTOR + smooth * inv_freq
    scaled = np.where(wavelen > ORIG_CTX / LOW_FREQ, inv_freq / ROPE_FACTOR, mid_freq)
    half = np.where(wavelen < ORIG_CTX / HIGH_FREQ, inv_freq, scaled).astype(np.float32)
    return np.concatenate([half, half])[None, :]


def fdot(a, b):
    return jnp.dot(a, b, preferred_element_type=jnp.float32)


def front_kernel(cfg, hid_h, posr_v, pos_s, gain_v, freq_v, wq_h, wk_h, wv_h, k_h, v_h, ko_h, vo_h, blk_v,
                 hid_v, xn, wq_v, wk_v, wv_v, kc, vc, q3, o3, st3, kn, vn, in_sem, kv_sem, out_sem):
    heads, hd, dim, batch, slots = cfg
    f32, bf16 = jnp.float32, jnp.bfloat16
    per = 32
    nch = batch // per
    scale = hd ** -0.5
    first_slot = lax.axis_index('sp') * slots

    def loop(n, body):
        def step(i, carry):
            body(i)
            return carry
        lax.fori_loop(0, n, step, 0)

    def ld_hid(r):
        span = pl.ds(pl.multiple_of(r * per, per), per)
        return pltpu.make_async_copy(hid_h.at[span], hid_v.at[span], in_sem.at[3 + r])

    weights = [pltpu.make_async_copy(h, v, in_sem.at[i]) for i, (h, v) in enumerate(((wq_h, wq_v), (wk_h, wk_v), (wv_h, wv_v)))]

    def ld_kv(g):
        span = pl.ds(g * per, per)
        return (pltpu.make_async_copy(k_h.at[span], kc.at[span], kv_sem.at[0, g]),
                pltpu.make_async_copy(v_h.at[span], vc.at[span], kv_sem.at[1, g]))

    def st_kv(g):
        span = pl.ds(g * per, per)
        return (pltpu.make_async_copy(kc.at[span], ko_h.at[span], out_sem.at[0, g]),
                pltpu.make_async_copy(vc.at[span], vo_h.at[span], out_sem.at[1, g]))

    def start_both(pair):
        pair[0].start()
        pair[1].start()

    def wait_both(pair):
        pair[0].wait()
        pair[1].wait()

    loop(nch, lambda r: ld_hid(r).start())
    for cp in weights:
        cp.start()
    loop(nch, lambda g: start_both(ld_kv(g)))
    q3[...] = jnp.zeros_like(q3)

    gain = gain_v[...].astype(f32)

    def norm(r):
        ld_hid(r).wait()
        span = pl.ds(pl.multiple_of(r * per, per), per)
        xs = hid_v[span, :].astype(f32)
        inv = lax.rsqrt(jnp.sum(xs * xs, axis=1, keepdims=True) / dim + NORM_EPS)
        for k in range(dim // 128):
            xn[span, k * 128:(k + 1) * 128] = (xs[:, k * 128:(k + 1) * 128] * inv * gain[k:k + 1]).astype(bf16)

    loop(nch, norm)
    eye = lax.broadcasted_iota(jnp.int32, (batch, batch), 0) == lax.broadcasted_iota(jnp.int32, (batch, batch), 1)
    posc = jnp.sum(jnp.where(eye, jnp.broadcast_to(posr_v[...], (batch, batch)).astype(f32), 0.0), axis=1, keepdims=True)
    angles = posc * freq_v[...]
    cos_t = jnp.cos(angles)
    low = lax.broadcasted_iota(jnp.int32, (batch, hd), 1) < hd // 2
    sin_t = jnp.where(low, -jnp.sin(angles), jnp.sin(angles))

    def rope(v):
        r = v.astype(bf16).astype(f32)
        return (r * cos_t + pltpu.roll(r, hd // 2, 1) * sin_t).astype(bf16).astype(f32)

    for cp in weights:
        cp.wait()
    q = fdot(xn[...], wq_v[...])
    for h in range(heads):
        q3[:, h, :] = rope(q[:, h * hd:(h + 1) * hd])
    kn[...] = rope(fdot(xn[...], wk_v[...]))
    vn[...] = fdot(xn[...], wv_v[...]).astype(bf16).astype(f32)

    lane = lax.broadcasted_iota(jnp.int32, (8, 128), 1)
    sub = lax.broadcasted_iota(jnp.int32, (8, 128), 0)
    row16 = lax.broadcasted_iota(jnp.int32, (16, hd), 0)
    zero = jnp.zeros((8, 128), f32)

    def attend(g):
        wait_both(ld_kv(g))
        lps = []
        for i in range(per):
            b = g * per + i
            lp = pos_s[b] - first_slot
            lps.append(lp)
            base = pl.multiple_of(lax.shift_left(lax.shift_right_logical(jnp.clip(lp, 0, slots - 1), 4), 4), 16)
            hit = row16 + base == lp
            for ref, new in ((kc, kn), (vc, vn)):
                old = ref[b, pl.ds(base, 16), :].astype(f32)
                fresh = jnp.broadcast_to(new[pl.ds(b, 1), :], (16, hd))
                ref[b, pl.ds(base, 16), :] = jnp.where(hit, fresh, old).astype(bf16)
        start_both(st_kv(g))
        for t in range(per // 4):
            four = pl.ds(g * per + 4 * t, 4)
            sg = lax.dot_general(q3[four].reshape(32, hd).astype(bf16), kc[four].reshape(4 * slots, hd),
                                 (((1,), (1,)), ((), ())), preferred_element_type=f32) * scale
            probs = []
            for i in range(4):
                off = slots * (i % 2)
                lp = jnp.minimum(lps[4 * t + i], slots - 1)
                seen = (lane >= off) & (lane <= off + lp)
                sc = jnp.where(seen, sg[8 * i:8 * i + 8, 128 * (i // 2):128 * (i // 2) + 128], NEG_BIG)
                mx = jnp.max(sc, axis=1, keepdims=True)
                pr = jnp.where(seen, jnp.exp(sc - mx), 0.0)
                ls = jnp.sum(pr, axis=1, keepdims=True)
                st3[g * per + 4 * t + i] = jnp.where(lane == sub, mx, jnp.where(lane == sub + 8, ls, 0.0))
                probs.append(jnp.concatenate([pr, zero] if i < 2 else [zero, pr], axis=1))
            pg = jnp.concatenate(probs, axis=0).astype(bf16)
            o3[four] = fdot(pg, vc[four].reshape(4 * slots, hd)).reshape(4, 8, hd)

    loop(nch, attend)
    stat = st3[:, 0, :]
    for h in range(1, heads):
        stat = stat + st3[:, h, :]
    for h in range(heads):
        blk_v[:, h * hd:(h + 1) * hd] = o3[:, h, :]
    blk_v[:, heads * hd:] = stat
    loop(nch, lambda g: wait_both(st_kv(g)))


def front(hidden, new_pos, k_self, v_self, gain, wq, wk, wv, heads, hd):
    batch, dim = hidden.shape
    slots = k_self.shape[1]
    f32, bf16 = jnp.float32, jnp.bfloat16
    anyspec = pl.BlockSpec(memory_space=pl.ANY)
    vmem = pl.BlockSpec(memory_space=pltpu.VMEM)
    smem = pl.BlockSpec(memory_space=pltpu.SMEM)
    dma = pltpu.SemaphoreType.DMA
    nch = batch // 32
    cache = jax.ShapeDtypeStruct((batch, slots, hd), bf16)
    ko, vo, blk = pl.pallas_call(
        functools.partial(front_kernel, (heads, hd, dim, batch, slots)),
        out_shape=(cache, cache, jax.ShapeDtypeStruct((batch, heads * hd + hd), f32)),
        in_specs=[anyspec, vmem, smem, vmem, vmem] + [anyspec] * 5,
        out_specs=(anyspec, anyspec, vmem),
        scratch_shapes=[
            pltpu.VMEM((batch, dim), bf16),
            pltpu.VMEM((batch, dim), bf16),
            pltpu.VMEM(wq.shape, bf16),
            pltpu.VMEM(wk.shape, bf16),
            pltpu.VMEM(wv.shape, bf16),
            pltpu.VMEM((batch, slots, hd), bf16),
            pltpu.VMEM((batch, slots, hd), bf16),
            pltpu.VMEM((batch, 8, hd), f32),
            pltpu.VMEM((batch, 8, hd), f32),
            pltpu.VMEM((batch, 8, hd), f32),
            pltpu.VMEM((batch, hd), f32),
            pltpu.VMEM((batch, hd), f32),
            dma((3 + nch,)),
            dma((2, nch)),
            dma((2, nch)),
        ],
        compiler_params=pltpu.CompilerParams(vmem_limit_bytes=60000000),
        name='front',
    )(hidden, new_pos.reshape(1, batch), new_pos, gain.reshape(dim // 128, 128), jnp.asarray(rope_freqs(hd)),
      wq, wk, wv, k_self.reshape(batch, slots, hd), v_self.reshape(batch, slots, hd))
    return ko.reshape(k_self.shape), vo.reshape(v_self.shape), blk


def tail_kernel(cfg, blk_h, hid_h, g2_v, g3_v, g4_v, qn_v, rowm_v, gate_s, xv_h, kc_h, vc_h,
                wo_h, wg_h, wu_h, wd_h, cq_h, cwo_h, cg_h, cu_h, cd_h, out_v,
                bk, yr, yd, yt, yf, ob, hrow, hst,
                wo_v, wg_v, wu_v, wd_v, cq_v, cwo_v, kc_v, vc_v, xv_v,
                pbuf, dbuf, sbuf, rbuf, ebuf, tbuf, fbuf, xa, og, acc, act, q3, oc,
                ld_sem, w_sem, kv_sem, ys, yrs, rs_s, rs_r, ag_s, ag_r, fg_s, fg_r):
    heads, hd, dim, mlp, ntok = cfg
    cw = dim // NC
    hw = heads * hd
    half = 32
    x = lax.axis_index('tp') // 2
    c = lax.axis_index('tp') % 2
    y = lax.axis_index('sp')
    slot = c * 4 + x
    scale = hd ** -0.5

    def ring(v):
        return lax.rem(v + 8, 4)

    def xdev(d):
        return {'tp': 2 * ring(x + d) + c}

    def ydev(d):
        return {'sp': ring(y + d)}

    sib = {'tp': 2 * x + 1 - c}

    def rcopy(src, dst, ss, rs, dev):
        return pltpu.make_async_remote_copy(src_ref=src, dst_ref=dst, send_sem=ss, recv_sem=rs,
                                            device_id=dev, device_id_type=MESH)

    def loop(n, body):
        def step(i, carry):
            body(i)
            return carry
        lax.fori_loop(0, n, step, 0)

    blk_cp = pltpu.make_async_copy(blk_h, bk, ld_sem.at[0])
    hid_cp = pltpu.make_async_copy(hid_h.at[y * 8 + slot], hrow, ld_sem.at[1])
    xv_cp = pltpu.make_async_copy(xv_h.at[y], xv_v, ld_sem.at[2])

    def cols(h, v, k, j):
        return pltpu.make_async_copy(h.at[:, pl.ds(pl.multiple_of(j * cw, 128), cw)], v.at[j], w_sem.at[k, j])

    def rows(h, v, k, j):
        return pltpu.make_async_copy(h.at[pl.ds(pl.multiple_of(j * cw, 128), cw)], v.at[j], w_sem.at[k, j])

    def ld_wo(j):
        return cols(wo_h, wo_v, 0, j)

    def ld_wg(j):
        return rows(wg_h, wg_v, 1, j)

    def ld_wu(j):
        return rows(wu_h, wu_v, 2, j)

    def ld_wd(j):
        return cols(wd_h, wd_v, 3, j)

    def ld_cq(j):
        return rows(cq_h, cq_v, 4, j)

    def ld_cwo(j):
        return cols(cwo_h, cwo_v, 5, j)

    def ld_cg(j):
        return rows(cg_h, wg_v, 6, j)

    def ld_cu(j):
        return rows(cu_h, wu_v, 7, j)

    def ld_cd(j):
        return cols(cd_h, wd_v, 8, j)

    def ld_kc(g):
        return pltpu.make_async_copy(kc_h.at[y, pl.ds(g * 8, 8)], kc_v.at[pl.ds(g * 8, 8)], kv_sem.at[0, g])

    def ld_vc(g):
        return pltpu.make_async_copy(vc_h.at[y, pl.ds(g * 8, 8)], vc_v.at[pl.ds(g * 8, 8)], kv_sem.at[1, g])

    blk_cp.start()
    hid_cp.start()
    xv_cp.start()
    loop(NC, lambda j: ld_wo(j).start())

    barrier = pltpu.get_barrier_semaphore()
    for dev in (sib, xdev(1), xdev(-1), ydev(1), ydev(-1)):
        pl.semaphore_signal(barrier, inc=1, device_id=dev, device_id_type=MESH)

    def start_gu(j):
        ld_wg(j).start()
        ld_wu(j).start()

    loop(NC, start_gu)
    loop(NC, lambda j: ld_wd(j).start())
    loop(NC, lambda j: ld_cq(j).start())

    def start_kv(g):
        ld_kc(g).start()
        ld_vc(g).start()

    loop(8, start_kv)
    loop(NC, lambda j: ld_cwo(j).start())
    q3[...] = jnp.zeros_like(q3)
    pl.semaphore_wait(barrier, 5)

    lane = lax.broadcasted_iota(jnp.int32, (half, hd), 1)

    def merge(a, b):
        outs, ms, ls = [], [], []
        for h in range(heads):
            ma, mb = a[:, hw + h:hw + h + 1], b[:, hw + h:hw + h + 1]
            la, lb = a[:, hw + 8 + h:hw + 9 + h], b[:, hw + 8 + h:hw + 9 + h]
            mm = jnp.maximum(ma, mb)
            ea, eb = jnp.exp(ma - mm), jnp.exp(mb - mm)
            outs.append(a[:, h * hd:(h + 1) * hd] * ea + b[:, h * hd:(h + 1) * hd] * eb)
            ms.append(mm)
            ls.append(la * ea + lb * eb)
        stat = jnp.zeros((half, hd), jnp.float32)
        for h in range(heads):
            stat = jnp.where(lane == h, ms[h], stat)
            stat = jnp.where(lane == 8 + h, ls[h], stat)
        return jnp.concatenate(outs + [stat], axis=1), ls

    def y_relay(j, d):
        return rcopy(bk.at[ring(y + 2), j], yr.at[j], ys.at[0, j], yrs.at[0, j], ydev(d))

    def y_direct(j, d):
        return rcopy(bk.at[ring(y - d), j], yd.at[j], ys.at[1, j], yrs.at[1, j], ydev(-d))

    def y_final(j, d):
        return rcopy(yt.at[j], yf.at[j], ys.at[2, j], yrs.at[2, j], ydev(d))

    blk_cp.wait()
    for j, d in ((0, 1), (1, -1)):
        y_relay(j, d).start()
    for j, d in ((0, 1), (1, -1)):
        y_direct(j, d).start()
    for j, d in ((0, 1), (1, -1)):
        y_relay(j, d).wait_recv()
        yt[j] = merge(bk[ring(y + d), j], yr[j])[0]
        y_final(j, d).start()
    for j, d in ((0, 1), (1, -1)):
        y_direct(j, d).wait_recv()
        first = merge(bk[y, j], yd[j])[0]
        y_final(j, d).wait_recv()
        both, sums = merge(first, yf[j])
        for h in range(heads):
            ob[j * half:(j + 1) * half, h * hd:(h + 1) * hd] = (both[:, h * hd:(h + 1) * hd] / sums[h]).astype(jnp.bfloat16)

    def rs_pair(p, j):
        return rcopy(pbuf.at[p, j, 1 - c], dbuf.at[p, j], rs_s.at[p, 0, j], rs_r.at[p, 0, j], sib)

    def turn(j):
        return 1 - 2 * lax.rem(j, 2)

    def rs_relay(p, j):
        return rcopy(sbuf.at[p, j, ring(x + 2)], rbuf.at[p, j], rs_s.at[p, 1, j], rs_r.at[p, 1, j], xdev(turn(j)))

    def rs_direct(p, j):
        return rcopy(sbuf.at[p, j, ring(x - turn(j))], ebuf.at[p, j], rs_s.at[p, 2, j], rs_r.at[p, 2, j], xdev(-turn(j)))

    def rs_final(p, j):
        return rcopy(tbuf.at[p, j], fbuf.at[p, j], rs_s.at[p, 3, j], rs_r.at[p, 3, j], xdev(turn(j)))

    def reduce_scatter(p, partial):
        def second(j):
            rs_pair(p, j).wait_recv()
            sbuf[p, j] = (pbuf[p, j, c] + dbuf[p, j]).reshape(4, 8, cw)
            rs_relay(p, j).start()
            rs_direct(p, j).start()

        def body(j):
            @pl.when(j < NC)
            def _():
                pbuf[p, j] = partial(j).reshape(2, half, cw)
                rs_pair(p, j).start()

            @pl.when(j >= 1)
            def _():
                second(j - 1)

        loop(NC + 1, body)

        def third(j):
            rs_relay(p, j).wait_recv()
            tbuf[p, j] = sbuf[p, j, ring(x + turn(j))] + rbuf[p, j]
            rs_final(p, j).start()

        loop(NC, third)

    def reduced(p, j):
        rs_direct(p, j).wait_recv()
        rs_final(p, j).wait_recv()
        return sbuf[p, j, x] + ebuf[p, j] + fbuf[p, j]

    def new_rows(p, factor):
        sq = jnp.zeros((8, 1), jnp.float32)
        for j in range(NC):
            add = reduced(p, j)
            if factor is not None:
                add = factor * add
            old = hrow[:, j * cw:(j + 1) * cw].astype(jnp.float32) if p == 0 else hst[j]
            new = (old + add).astype(jnp.bfloat16).astype(jnp.float32)
            hst[j] = new
            sq = sq + jnp.sum(new * new, axis=1, keepdims=True)
        return sq

    def ag_send(q, j, s, k, dev):
        return rcopy(xa.at[q, j, s], xa.at[q, j, s], ag_s.at[q, j, k], ag_r.at[q, j, s], dev)

    def ag_got(q, j, s):
        return rcopy(xa.at[q, j, s], xa.at[q, j, s], ag_s.at[q, j, 0], ag_r.at[q, j, s], sib)

    def at(d):
        return c * 4 + ring(x + d)

    def ag_copy(q, j, i):
        d = turn(j)
        s = (0, 0, 0, -d, -d, d, 2)[i]
        dev = (xdev(d), xdev(-d), sib, xdev(d), sib, sib, sib)[i]
        return ag_send(q, j, slot if i < 3 else at(s), i, dev)

    def all_gather(q, sq, gain_row, consume):
        inv = lax.rsqrt(sq / dim + NORM_EPS)
        rows_of = (g2_v, g3_v, g4_v)[gain_row][...].astype(jnp.float32)
        for j in range(NC):
            gain = jnp.concatenate([rows_of[i:i + 1] for i in range(j * cw // 128, (j + 1) * cw // 128)], axis=1)
            xa[q, j, slot] = (hst[j] * inv * gain).astype(jnp.bfloat16).astype(jnp.float32)
            for k in range(3):
                ag_copy(q, j, k).start()

        def first(j):
            d = turn(j)
            ag_got(q, j, at(-d)).wait_recv()
            ag_copy(q, j, 3).start()
            ag_copy(q, j, 4).start()
            ag_got(q, j, at(d)).wait_recv()
            ag_copy(q, j, 5).start()

        loop(NC, first)

        def body(j):
            @pl.when(j < NC)
            def _():
                ag_got(q, j, at(2)).wait_recv()
                ag_copy(q, j, 6).start()

            @pl.when(j >= 1)
            def _():
                for k in range(4):
                    ag_got(q, j - 1, (1 - c) * 4 + k).wait_recv()
                consume(j - 1, xa[q, j - 1].reshape(2 * half, cw).astype(jnp.bfloat16))

        loop(NC + 1, body)

    def mlp_hidden(q, sq, gain_row, wait_gu):
        acc[...] = jnp.zeros_like(acc)

        def consume(j, xs):
            wait_gu(j)
            acc[:, :mlp] += fdot(xs, wg_v[j])
            acc[:, mlp:] += fdot(xs, wu_v[j])

        all_gather(q, sq, gain_row, consume)
        gv = acc[:, :mlp].astype(jnp.bfloat16).astype(jnp.float32)
        uv = acc[:, mlp:].astype(jnp.bfloat16).astype(jnp.float32)
        act[...] = (jax.nn.silu(gv) * uv).astype(jnp.bfloat16)

    def part_wo(j):
        ld_wo(j).wait()
        return fdot(ob[...], wo_v[j])

    reduce_scatter(0, part_wo)
    hid_cp.wait()
    sq = new_rows(0, None)

    def wait_self(j):
        ld_wg(j).wait()
        ld_wu(j).wait()

    mlp_hidden(0, sq, 0, wait_self)

    def start_cgu(j):
        ld_cg(j).start()
        ld_cu(j).start()

    loop(NC, start_cgu)

    def part_wd(j):
        ld_wd(j).wait()
        return fdot(act[...], wd_v[j])

    reduce_scatter(1, part_wd)
    loop(NC, lambda j: ld_cd(j).start())
    sq = new_rows(1, None)

    acc[:, :hw] = jnp.zeros((2 * half, hw), jnp.float32)

    def consume_q(j, xs):
        ld_cq(j).wait()
        acc[:, :hw] += fdot(xs, cq_v[j])

    all_gather(1, sq, 1, consume_q)
    qgain = qn_v[...].astype(jnp.float32)
    for h in range(heads):
        qh = acc[:, h * hd:(h + 1) * hd].astype(jnp.bfloat16).astype(jnp.float32)
        qinv = lax.rsqrt(jnp.mean(qh * qh, axis=1, keepdims=True) + NORM_EPS)
        q3[:, h, :] = (qh * qinv * qgain).astype(jnp.bfloat16).astype(jnp.float32)
    xv_cp.wait()

    def attend(g):
        ld_kc(g).wait()
        ld_vc(g).wait()
        xv = xv_v[pl.ds(pl.multiple_of(g * 8, 8), 8), :]
        for i in range(8):
            b = g * 8 + i
            sc = lax.dot_general(q3[b].astype(jnp.bfloat16), kc_v[b], (((1,), (1,)), ((), ())),
                                 preferred_element_type=jnp.float32) * scale
            valid = jnp.broadcast_to(xv[i:i + 1], (8, ntok)) > 0
            sc = jnp.where(valid, sc, NEG_BIG)
            mx = jnp.max(sc, axis=1, keepdims=True)
            pr = jnp.where(valid, jnp.exp(sc - mx), 0.0)
            ls = jnp.sum(pr, axis=1, keepdims=True)
            oc[b] = fdot(pr.astype(jnp.bfloat16), vc_v[b]) / ls

    loop(8, attend)
    for h in range(heads):
        ob[:, h * hd:(h + 1) * hd] = oc[:, h, :].astype(jnp.bfloat16)

    def part_cwo(j):
        ld_cwo(j).wait()
        return fdot(ob[...], cwo_v[j])

    reduce_scatter(2, part_cwo)
    nrow = rowm_v.shape[1]
    mine = (y * 8 + slot) * 8 + lax.broadcasted_iota(jnp.int32, (8, nrow), 0)
    pick = lax.broadcasted_iota(jnp.int32, (8, nrow), 1) == mine
    rmask = jnp.sum(jnp.where(pick, jnp.broadcast_to(rowm_v[...], (8, nrow)), 0).astype(jnp.float32), axis=1, keepdims=True)
    factor = [jnp.tanh(jnp.full((8, 128), gate_s[k], jnp.float32))[:, :1] * rmask for k in range(2)]
    sq = new_rows(2, factor[0])

    def wait_cross(j):
        ld_cg(j).wait()
        ld_cu(j).wait()

    mlp_hidden(2, sq, 2, wait_cross)

    def part_cd(j):
        ld_cd(j).wait()
        return fdot(act[...], wd_v[j])

    reduce_scatter(3, part_cd)
    new_rows(3, factor[1])

    def parts_of(j):
        if j < NC // 2:
            return (lambda k: og.at[j, c, y, ring(x + k)], xdev), (lambda k: og.at[j, c, ring(y + k)], ydev)
        return (lambda k: og.at[j, c, ring(y + k), x], ydev), (lambda k: og.at[j, c, :, ring(x + k)], xdev)

    def fg(j, stage, k, s, what, dev):
        return rcopy(what, what, fg_s.at[j, stage, s], fg_r.at[j, stage, k], dev)

    fg_all = []
    plans = []
    for j in range(NC):
        d = 1 - 2 * (j % 2)
        stages = []
        for stage, (region, dev) in enumerate(parts_of(j)):
            stages.append(dict(
                own=[fg(j, stage, 0, 0, region(0), dev(d)), fg(j, stage, 1, 1, region(0), dev(-d))],
                relay=fg(j, stage, 2, 2, region(-d), dev(d)),
                got=[fg(j, stage, 0, 0, region(-d), sib), fg(j, stage, 1, 1, region(d), sib), fg(j, stage, 2, 2, region(2), sib)],
                pair=[fg(j, 2, i, i, region(k), sib) for i, k in enumerate((0, -d, d, 2))],
            ))
        plans.append(stages)
    order = []
    for j in range(NC // 2):
        order += [j, j + NC // 2]
    for j in order:
        og[j, c, y, x] = hst[j]
        for cp in plans[j][0]['own']:
            cp.start()
    for j in order:
        st = plans[j][0]
        st['got'][0].wait_recv()
        st['relay'].start()
    for j in order:
        st, nx = plans[j]
        st['got'][1].wait_recv()
        st['got'][2].wait_recv()
        for cp in nx['own']:
            cp.start()
        nx['pair'][0].start()
    for j in order:
        st = plans[j][1]
        st['got'][0].wait_recv()
        st['relay'].start()
        st['pair'][1].start()
        st['got'][1].wait_recv()
        st['pair'][2].start()
    for j in order:
        st = plans[j][1]
        st['got'][2].wait_recv()
        st['pair'][3].start()
    for j in order:
        for cp in plans[j][1]['pair']:
            cp.wait_recv()
        for yy in range(4):
            for cc in range(2):
                out_v[yy * 8 + cc * 4:yy * 8 + cc * 4 + 4, :, j * cw:(j + 1) * cw] = og[j, cc, yy].astype(jnp.bfloat16)

    for j, d in ((0, 1), (1, -1)):
        y_relay(j, d).wait_send()
        y_direct(j, d).wait_send()
        y_final(j, d).wait_send()

    def drain_rs(j):
        for p in range(4):
            rs_pair(p, j).wait_send()
            rs_relay(p, j).wait_send()
            rs_direct(p, j).wait_send()
            rs_final(p, j).wait_send()
        for q in range(3):
            for i in range(7):
                ag_copy(q, j, i).wait_send()

    loop(NC, drain_rs)
    for j in range(NC):
        for st in plans[j]:
            for cp in st['own']:
                cp.wait_send()
            st['relay'].wait_send()
        for cp in plans[j][1]['pair']:
            cp.wait_send()


def tail(blk, hidden, gains, rowmask, gates, xvalid, k_cross, v_cross, wo, wg, wu, wd, cq, cwo, cg, cu, cd, heads, hd):
    batch, dim = hidden.shape
    mlp = wg.shape[1]
    ntok = xvalid.shape[1]
    cw = dim // NC
    hw = heads * hd
    bl = batch // 4
    half = bl // 2
    f32, bf16 = jnp.float32, jnp.bfloat16
    anyspec = pl.BlockSpec(memory_space=pl.ANY)
    vmem = pl.BlockSpec(memory_space=pltpu.VMEM)
    smem = pl.BlockSpec(memory_space=pltpu.SMEM)
    dma = pltpu.SemaphoreType.DMA
    scratch = [
        pltpu.VMEM((4, 2, half, hw + hd), f32),
        pltpu.VMEM((2, half, hw + hd), f32),
        pltpu.VMEM((2, half, hw + hd), f32),
        pltpu.VMEM((2, half, hw + hd), f32),
        pltpu.VMEM((2, half, hw + hd), f32),
        pltpu.VMEM((bl, hw), bf16),
        pltpu.VMEM((8, dim), bf16),
        pltpu.VMEM((NC, 8, cw), f32),
        pltpu.VMEM((NC, hw, cw), bf16),
        pltpu.VMEM((NC, cw, mlp), bf16),
        pltpu.VMEM((NC, cw, mlp), bf16),
        pltpu.VMEM((NC, mlp, cw), bf16),
        pltpu.VMEM((NC, cw, hw), bf16),
        pltpu.VMEM((NC, hw, cw), bf16),
        pltpu.VMEM((bl, ntok, hd), bf16),
        pltpu.VMEM((bl, ntok, hd), bf16),
        pltpu.VMEM((bl, ntok), jnp.int32),
        pltpu.VMEM((4, NC, 2, half, cw), f32),
        pltpu.VMEM((4, NC, half, cw), f32),
        pltpu.VMEM((4, NC, 4, 8, cw), f32),
        pltpu.VMEM((4, NC, 8, cw), f32),
        pltpu.VMEM((4, NC, 8, cw), f32),
        pltpu.VMEM((4, NC, 8, cw), f32),
        pltpu.VMEM((4, NC, 8, cw), f32),
        pltpu.VMEM((3, NC, 8, 8, cw), f32),
        pltpu.VMEM((NC, 2, 4, 4, 8, cw), f32),
        pltpu.VMEM((bl, 2 * mlp), f32),
        pltpu.VMEM((bl, mlp), bf16),
        pltpu.VMEM((bl, 8, hd), f32),
        pltpu.VMEM((bl, 8, hd), f32),
        dma((3,)),
        dma((9, NC)),
        dma((2, 8)),
        dma((3, 2)),
        dma((3, 2)),
        dma((4, 4, NC)),
        dma((4, 4, NC)),
        dma((3, NC, 7)),
        dma((3, NC, 8)),
        dma((NC, 3, 4)),
        dma((NC, 3, 4)),
    ]
    out = pl.pallas_call(
        functools.partial(tail_kernel, (heads, hd, dim, mlp, ntok)),
        out_shape=jax.ShapeDtypeStruct((batch // 8, 8, dim), bf16),
        in_specs=[anyspec, anyspec] + [vmem] * 5 + [smem] + [anyspec] * 12,
        out_specs=vmem,
        scratch_shapes=scratch,
        compiler_params=pltpu.CompilerParams(collective_id=0, has_side_effects=True, vmem_limit_bytes=67043328),
        name='tail',
    )(blk.reshape(4, 2, half, hw + hd), hidden.reshape(batch // 8, 8, dim),
      *[g.reshape(-1, 128) for g in gains], rowmask.reshape(1, batch), gates,
      xvalid.reshape(4, bl, ntok), k_cross.reshape(4, bl, ntok, hd), v_cross.reshape(4, bl, ntok, hd),
      wo, wg, wu, wd, cq, cwo, cg, cu, cd)
    return out.reshape(batch, dim)


def solution(mesh):
    cache_spec = P('dp', 'sp', 'tp', None)
    cross_spec = P('dp', None, 'tp', None)
    row_spec = P('dp', None)
    vec_spec = P('dp')
    full_spec = P(None)
    col_spec = P(None, 'tp')
    split_rows = P('tp', None)
    in_specs = (row_spec, vec_spec, cache_spec, cache_spec, cross_spec, cross_spec, row_spec, vec_spec,
                full_spec, col_spec, col_spec, col_spec, split_rows, full_spec, col_spec, col_spec, split_rows,
                full_spec, col_spec, full_spec, split_rows, full_spec, full_spec, col_spec, col_spec, split_rows)
    out_specs = (row_spec, cache_spec, cache_spec)

    def local_step(hidden, new_pos, k_self, v_self, k_cross, v_cross, xvalid, rowmask,
                   self_attn_norm, self_wq, self_wk, self_wv, self_wo, self_mlp_norm,
                   self_wgate, self_wup, self_wdown, cross_attn_norm, cross_wq, cross_qnorm,
                   cross_wo, cross_gates, cross_mlp_norm, cross_wgate, cross_wup, cross_wdown):
        head_dim = k_self.shape[3]
        heads_local = self_wq.shape[1] // head_dim
        k_new_cache, v_new_cache, blk = front(hidden, new_pos, k_self, v_self, self_attn_norm, self_wq, self_wk, self_wv,
                                              heads_local, head_dim)
        gains = (self_mlp_norm, cross_attn_norm, cross_mlp_norm, cross_qnorm)
        h4 = tail(blk, hidden, gains, rowmask, cross_gates, xvalid, k_cross, v_cross, self_wo, self_wgate, self_wup, self_wdown,
                  cross_wq, cross_wo, cross_wgate, cross_wup, cross_wdown, heads_local, head_dim)
        return h4, k_new_cache, v_new_cache

    return jax.shard_map(local_step, mesh=mesh, in_specs=in_specs, out_specs=out_specs, check_vma=False)
```

```python
import functools
import math
import jax
import jax.numpy as jnp
import numpy as np
from jax import lax
from jax.experimental import pallas as pl
from jax.experimental.pallas import tpu as pltpu
from jax.sharding import PartitionSpec as P

NORM_EPS = 1e-5
ROPE_THETA = 500000.0
ROPE_FACTOR = 8.0
LOW_FREQ = 1.0
HIGH_FREQ = 4.0
ORIG_CTX = 8192.0
NEG_BIG = -1e30
NC = 4
MESH = pl.DeviceIdType.MESH


def rope_freqs(head_dim):
    inv_freq = (1.0 / (ROPE_THETA ** (np.arange(0, head_dim, 2).astype(np.float32) / np.float32(head_dim)))).astype(np.float32)
    wavelen = 2.0 * math.pi / inv_freq
    smooth = (ORIG_CTX / wavelen - LOW_FREQ) / (HIGH_FREQ - LOW_FREQ)
    mid_freq = (1.0 - smooth) * inv_freq / ROPE_FACTOR + smooth * inv_freq
    scaled = np.where(wavelen > ORIG_CTX / LOW_FREQ, inv_freq / ROPE_FACTOR, mid_freq)
    half = np.where(wavelen < ORIG_CTX / HIGH_FREQ, inv_freq, scaled).astype(np.float32)
    return np.concatenate([half, half])[None, :]


def fdot(a, b):
    return jnp.dot(a, b, preferred_element_type=jnp.float32)


def front_kernel(cfg, hid_h, posr_v, pos_s, gain_v, freq_v, wq_h, wk_h, wv_h, k_h, v_h, ko_h, vo_h, blk_v,
                 hid_v, xn, wq_v, wk_v, wv_v, kc, vc, q3, o3, st3, kn, vn, in_sem, kv_sem, out_sem):
    heads, hd, dim, batch, slots = cfg
    f32, bf16 = jnp.float32, jnp.bfloat16
    per = 32
    nch = batch // per
    scale = hd ** -0.5
    first_slot = lax.axis_index('sp') * slots

    def loop(n, body):
        def step(i, carry):
            body(i)
            return carry
        lax.fori_loop(0, n, step, 0)

    def ld_hid(r):
        span = pl.ds(pl.multiple_of(r * per, per), per)
        return pltpu.make_async_copy(hid_h.at[span], hid_v.at[span], in_sem.at[3 + r])

    weights = [pltpu.make_async_copy(h, v, in_sem.at[i]) for i, (h, v) in enumerate(((wq_h, wq_v), (wk_h, wk_v), (wv_h, wv_v)))]

    def ld_kv(g):
        span = pl.ds(g * per, per)
        return (pltpu.make_async_copy(k_h.at[span], kc.at[span], kv_sem.at[0, g]),
                pltpu.make_async_copy(v_h.at[span], vc.at[span], kv_sem.at[1, g]))

    def st_kv(g):
        span = pl.ds(g * per, per)
        return (pltpu.make_async_copy(kc.at[span], ko_h.at[span], out_sem.at[0, g]),
                pltpu.make_async_copy(vc.at[span], vo_h.at[span], out_sem.at[1, g]))

    def start_both(pair):
        pair[0].start()
        pair[1].start()

    def wait_both(pair):
        pair[0].wait()
        pair[1].wait()

    loop(nch, lambda r: ld_hid(r).start())
    for cp in weights:
        cp.start()
    loop(nch, lambda g: start_both(ld_kv(g)))
    q3[...] = jnp.zeros_like(q3)

    gain = gain_v[...].astype(f32)

    def norm(r):
        ld_hid(r).wait()
        span = pl.ds(pl.multiple_of(r * per, per), per)
        xs = hid_v[span, :].astype(f32)
        inv = lax.rsqrt(jnp.sum(xs * xs, axis=1, keepdims=True) / dim + NORM_EPS)
        for k in range(dim // 128):
            xn[span, k * 128:(k + 1) * 128] = (xs[:, k * 128:(k + 1) * 128] * inv * gain[k:k + 1]).astype(bf16)

    loop(nch, norm)
    eye = lax.broadcasted_iota(jnp.int32, (batch, batch), 0) == lax.broadcasted_iota(jnp.int32, (batch, batch), 1)
    posc = jnp.sum(jnp.where(eye, jnp.broadcast_to(posr_v[...], (batch, batch)).astype(f32), 0.0), axis=1, keepdims=True)
    angles = posc * freq_v[...]
    cos_t = jnp.cos(angles)
    low = lax.broadcasted_iota(jnp.int32, (batch, hd), 1) < hd // 2
    sin_t = jnp.where(low, -jnp.sin(angles), jnp.sin(angles))

    def rope(v):
        r = v.astype(bf16).astype(f32)
        return (r * cos_t + pltpu.roll(r, hd // 2, 1) * sin_t).astype(bf16).astype(f32)

    for cp in weights:
        cp.wait()
    q = fdot(xn[...], wq_v[...])
    for h in range(heads):
        q3[:, h, :] = rope(q[:, h * hd:(h + 1) * hd])
    kn[...] = rope(fdot(xn[...], wk_v[...]))
    vn[...] = fdot(xn[...], wv_v[...]).astype(bf16).astype(f32)

    lane = lax.broadcasted_iota(jnp.int32, (8, 128), 1)
    sub = lax.broadcasted_iota(jnp.int32, (8, 128), 0)
    row16 = lax.broadcasted_iota(jnp.int32, (16, hd), 0)
    zero = jnp.zeros((8, 128), f32)

    def attend(g):
        wait_both(ld_kv(g))
        lps = []
        for i in range(per):
            b = g * per + i
            lp = pos_s[b] - first_slot
            lps.append(lp)
            base = pl.multiple_of(lax.shift_left(lax.shift_right_logical(jnp.clip(lp, 0, slots - 1), 4), 4), 16)
            hit = row16 + base == lp
            for ref, new in ((kc, kn), (vc, vn)):
                old = ref[b, pl.ds(base, 16), :].astype(f32)
                fresh = jnp.broadcast_to(new[pl.ds(b, 1), :], (16, hd))
                ref[b, pl.ds(base, 16), :] = jnp.where(hit, fresh, old).astype(bf16)
        start_both(st_kv(g))
        fours = [pl.ds(g * per + 4 * t, 4) for t in range(per // 4)]

        def scores(ts):
            return [lax.dot_general(q3[fours[t]].reshape(32, hd).astype(bf16), kc[fours[t]].reshape(4 * slots, hd),
                                    (((1,), (1,)), ((), ())), preferred_element_type=f32) * scale for t in ts]

        def soften(ts, sgs):
            out = []
            for t, sg in zip(ts, sgs):
                probs, stats = [], []
                for i in range(4):
                    off = slots * (i % 2)
                    lp = jnp.minimum(lps[4 * t + i], slots - 1)
                    seen = (lane >= off) & (lane <= off + lp)
                    sc = jnp.where(seen, sg[8 * i:8 * i + 8, 128 * (i // 2):128 * (i // 2) + 128], NEG_BIG)
                    mx = jnp.max(sc, axis=1, keepdims=True)
                    pr = jnp.where(seen, jnp.exp(sc - mx), 0.0)
                    ls = jnp.sum(pr, axis=1, keepdims=True)
                    stats.append(jnp.where(lane == sub, mx, jnp.where(lane == sub + 8, ls, 0.0)))
                    probs.append(jnp.concatenate([pr, zero] if i < 2 else [zero, pr], axis=1))
                out.append((jnp.concatenate(probs, axis=0).astype(bf16), stats))
            return out

        def mix(ts, prs):
            return [fdot(pg, vc[fours[t]].reshape(4 * slots, hd)) for t, (pg, _) in zip(ts, prs)]

        one, two = range(per // 8), range(per // 8, per // 4)
        sa = scores(one)
        sb = scores(two)
        pa = soften(one, sa)
        oa = mix(one, pa)
        pb = soften(two, sb)
        o2 = mix(two, pb)
        for t, (o, (_, stats)) in enumerate(zip(oa + o2, pa + pb)):
            o3[fours[t]] = o.reshape(4, 8, hd)
            for i in range(4):
                st3[g * per + 4 * t + i] = stats[i]

    loop(nch, attend)
    stat = st3[:, 0, :]
    for h in range(1, heads):
        stat = stat + st3[:, h, :]
    for h in range(heads):
        blk_v[:, h * hd:(h + 1) * hd] = o3[:, h, :]
    blk_v[:, heads * hd:] = stat
    loop(nch, lambda g: wait_both(st_kv(g)))


def front(hidden, new_pos, k_self, v_self, gain, wq, wk, wv, heads, hd):
    batch, dim = hidden.shape
    slots = k_self.shape[1]
    f32, bf16 = jnp.float32, jnp.bfloat16
    anyspec = pl.BlockSpec(memory_space=pl.ANY)
    vmem = pl.BlockSpec(memory_space=pltpu.VMEM)
    smem = pl.BlockSpec(memory_space=pltpu.SMEM)
    dma = pltpu.SemaphoreType.DMA
    nch = batch // 32
    cache = jax.ShapeDtypeStruct((batch, slots, hd), bf16)
    ko, vo, blk = pl.pallas_call(
        functools.partial(front_kernel, (heads, hd, dim, batch, slots)),
        out_shape=(cache, cache, jax.ShapeDtypeStruct((batch, heads * hd + hd), f32)),
        in_specs=[anyspec, vmem, smem, vmem, vmem] + [anyspec] * 5,
        out_specs=(anyspec, anyspec, vmem),
        scratch_shapes=[
            pltpu.VMEM((batch, dim), bf16),
            pltpu.VMEM((batch, dim), bf16),
            pltpu.VMEM(wq.shape, bf16),
            pltpu.VMEM(wk.shape, bf16),
            pltpu.VMEM(wv.shape, bf16),
            pltpu.VMEM((batch, slots, hd), bf16),
            pltpu.VMEM((batch, slots, hd), bf16),
            pltpu.VMEM((batch, 8, hd), f32),
            pltpu.VMEM((batch, 8, hd), f32),
            pltpu.VMEM((batch, 8, hd), f32),
            pltpu.VMEM((batch, hd), f32),
            pltpu.VMEM((batch, hd), f32),
            dma((3 + nch,)),
            dma((2, nch)),
            dma((2, nch)),
        ],
        compiler_params=pltpu.CompilerParams(vmem_limit_bytes=60000000),
        name='front',
    )(hidden, new_pos.reshape(1, batch), new_pos, gain.reshape(dim // 128, 128), jnp.asarray(rope_freqs(hd)),
      wq, wk, wv, k_self.reshape(batch, slots, hd), v_self.reshape(batch, slots, hd))
    return ko.reshape(k_self.shape), vo.reshape(v_self.shape), blk


def tail_kernel(cfg, blk_h, hid_h, g2_v, g3_v, g4_v, qn_v, rowm_v, gate_s, xv_h, kc_h, vc_h,
                wo_h, wg_h, wu_h, wd_h, cq_h, cwo_h, cg_h, cu_h, cd_h, out_v,
                bk, yr, yd, yt, yf, ob, hrow, hst,
                wo_v, wg_v, wu_v, wd_v, cq_v, cwo_v, kc_v, vc_v, xv_v,
                pbuf, dbuf, sbuf, rbuf, ebuf, tbuf, fbuf, xa, og, acc, act, q3, oc,
                ld_sem, w_sem, kv_sem, ys, yrs, rs_s, rs_r, ag_s, ag_r, fg_s, fg_r):
    heads, hd, dim, mlp, ntok = cfg
    cw = dim // NC
    hw = heads * hd
    half = 32
    x = lax.axis_index('tp') // 2
    c = lax.axis_index('tp') % 2
    y = lax.axis_index('sp')
    slot = c * 4 + x
    scale = hd ** -0.5

    def ring(v):
        return lax.rem(v + 8, 4)

    def xdev(d):
        return {'tp': 2 * ring(x + d) + c}

    def ydev(d):
        return {'sp': ring(y + d)}

    sib = {'tp': 2 * x + 1 - c}

    def rcopy(src, dst, ss, rs, dev):
        return pltpu.make_async_remote_copy(src_ref=src, dst_ref=dst, send_sem=ss, recv_sem=rs,
                                            device_id=dev, device_id_type=MESH)

    def loop(n, body):
        def step(i, carry):
            body(i)
            return carry
        lax.fori_loop(0, n, step, 0)

    blk_cp = pltpu.make_async_copy(blk_h, bk, ld_sem.at[0])
    hid_cp = pltpu.make_async_copy(hid_h.at[y * 8 + slot], hrow, ld_sem.at[1])
    xv_cp = pltpu.make_async_copy(xv_h.at[y], xv_v, ld_sem.at[2])

    def cols(h, v, k, j):
        return pltpu.make_async_copy(h.at[:, pl.ds(pl.multiple_of(j * cw, 128), cw)], v.at[j], w_sem.at[k, j])

    def rows(h, v, k, j):
        return pltpu.make_async_copy(h.at[pl.ds(pl.multiple_of(j * cw, 128), cw)], v.at[j], w_sem.at[k, j])

    def ld_wo(j):
        return cols(wo_h, wo_v, 0, j)

    def ld_wg(j):
        return rows(wg_h, wg_v, 1, j)

    def ld_wu(j):
        return rows(wu_h, wu_v, 2, j)

    def ld_wd(j):
        return cols(wd_h, wd_v, 3, j)

    def ld_cq(j):
        return rows(cq_h, cq_v, 4, j)

    def ld_cwo(j):
        return cols(cwo_h, cwo_v, 5, j)

    def ld_cg(j):
        return rows(cg_h, wg_v, 6, j)

    def ld_cu(j):
        return rows(cu_h, wu_v, 7, j)

    def ld_cd(j):
        return cols(cd_h, wd_v, 8, j)

    def ld_kc(g):
        return pltpu.make_async_copy(kc_h.at[y, pl.ds(g * 8, 8)], kc_v.at[pl.ds(g * 8, 8)], kv_sem.at[0, g])

    def ld_vc(g):
        return pltpu.make_async_copy(vc_h.at[y, pl.ds(g * 8, 8)], vc_v.at[pl.ds(g * 8, 8)], kv_sem.at[1, g])

    blk_cp.start()
    hid_cp.start()
    xv_cp.start()
    loop(NC, lambda j: ld_wo(j).start())

    barrier = pltpu.get_barrier_semaphore()
    for dev in (sib, xdev(1), xdev(-1), ydev(1), ydev(-1)):
        pl.semaphore_signal(barrier, inc=1, device_id=dev, device_id_type=MESH)

    def start_gu(j):
        ld_wg(j).start()
        ld_wu(j).start()

    loop(NC, start_gu)
    loop(NC, lambda j: ld_wd(j).start())
    loop(NC, lambda j: ld_cq(j).start())

    def start_kv(g):
        ld_kc(g).start()
        ld_vc(g).start()

    loop(8, start_kv)
    loop(NC, lambda j: ld_cwo(j).start())
    q3[...] = jnp.zeros_like(q3)
    pl.semaphore_wait(barrier, 5)

    lane = lax.broadcasted_iota(jnp.int32, (half, hd), 1)

    def merge(a, b):
        outs, ms, ls = [], [], []
        for h in range(heads):
            ma, mb = a[:, hw + h:hw + h + 1], b[:, hw + h:hw + h + 1]
            la, lb = a[:, hw + 8 + h:hw + 9 + h], b[:, hw + 8 + h:hw + 9 + h]
            mm = jnp.maximum(ma, mb)
            ea, eb = jnp.exp(ma - mm), jnp.exp(mb - mm)
            outs.append(a[:, h * hd:(h + 1) * hd] * ea + b[:, h * hd:(h + 1) * hd] * eb)
            ms.append(mm)
            ls.append(la * ea + lb * eb)
        stat = jnp.zeros((half, hd), jnp.float32)
        for h in range(heads):
            stat = jnp.where(lane == h, ms[h], stat)
            stat = jnp.where(lane == 8 + h, ls[h], stat)
        return jnp.concatenate(outs + [stat], axis=1), ls

    def y_relay(j, d):
        return rcopy(bk.at[ring(y + 2), j], yr.at[j], ys.at[0, j], yrs.at[0, j], ydev(d))

    def y_direct(j, d):
        return rcopy(bk.at[ring(y - d), j], yd.at[j], ys.at[1, j], yrs.at[1, j], ydev(-d))

    def y_final(j, d):
        return rcopy(yt.at[j], yf.at[j], ys.at[2, j], yrs.at[2, j], ydev(d))

    blk_cp.wait()
    for j, d in ((0, 1), (1, -1)):
        y_relay(j, d).start()
    for j, d in ((0, 1), (1, -1)):
        y_direct(j, d).start()
    for j, d in ((0, 1), (1, -1)):
        y_relay(j, d).wait_recv()
        yt[j] = merge(bk[ring(y + d), j], yr[j])[0]
        y_final(j, d).start()
    for j, d in ((0, 1), (1, -1)):
        y_direct(j, d).wait_recv()
        first = merge(bk[y, j], yd[j])[0]
        y_final(j, d).wait_recv()
        both, sums = merge(first, yf[j])
        for h in range(heads):
            ob[j * half:(j + 1) * half, h * hd:(h + 1) * hd] = (both[:, h * hd:(h + 1) * hd] / sums[h]).astype(jnp.bfloat16)

    def rs_pair(p, j):
        return rcopy(pbuf.at[p, j, 1 - c], dbuf.at[p, j], rs_s.at[p, 0, j], rs_r.at[p, 0, j], sib)

    def turn(j):
        return 1 - 2 * lax.rem(j, 2)

    def rs_relay(p, j):
        return rcopy(sbuf.at[p, j, ring(x + 2)], rbuf.at[p, j], rs_s.at[p, 1, j], rs_r.at[p, 1, j], xdev(turn(j)))

    def rs_direct(p, j):
        return rcopy(sbuf.at[p, j, ring(x - turn(j))], ebuf.at[p, j], rs_s.at[p, 2, j], rs_r.at[p, 2, j], xdev(-turn(j)))

    def rs_final(p, j):
        return rcopy(tbuf.at[p, j], fbuf.at[p, j], rs_s.at[p, 3, j], rs_r.at[p, 3, j], xdev(turn(j)))

    def reduce_scatter(p, partial):
        def second(j):
            rs_pair(p, j).wait_recv()
            sbuf[p, j] = (pbuf[p, j, c] + dbuf[p, j]).reshape(4, 8, cw)
            rs_relay(p, j).start()
            rs_direct(p, j).start()

        def body(j):
            @pl.when(j < NC)
            def _():
                pbuf[p, j] = partial(j).reshape(2, half, cw)
                rs_pair(p, j).start()

            @pl.when(j >= 1)
            def _():
                second(j - 1)

        loop(NC + 1, body)

        def third(j):
            rs_relay(p, j).wait_recv()
            tbuf[p, j] = sbuf[p, j, ring(x + turn(j))] + rbuf[p, j]
            rs_final(p, j).start()

        loop(NC, third)

    def reduced(p, j):
        rs_direct(p, j).wait_recv()
        rs_final(p, j).wait_recv()
        return sbuf[p, j, x] + ebuf[p, j] + fbuf[p, j]

    def new_rows(p, factor):
        sq = jnp.zeros((8, 1), jnp.float32)
        for j in range(NC):
            add = reduced(p, j)
            if factor is not None:
                add = factor * add
            old = hrow[:, j * cw:(j + 1) * cw].astype(jnp.float32) if p == 0 else hst[j]
            new = (old + add).astype(jnp.bfloat16).astype(jnp.float32)
            hst[j] = new
            sq = sq + jnp.sum(new * new, axis=1, keepdims=True)
        return sq

    def ag_send(q, j, s, k, dev):
        return rcopy(xa.at[q, j, s], xa.at[q, j, s], ag_s.at[q, j, k], ag_r.at[q, j, s], dev)

    def ag_got(q, j, s):
        return rcopy(xa.at[q, j, s], xa.at[q, j, s], ag_s.at[q, j, 0], ag_r.at[q, j, s], sib)

    def at(d):
        return c * 4 + ring(x + d)

    def ag_copy(q, j, i):
        d = turn(j)
        s = (0, 0, 0, -d, -d, d, 2)[i]
        dev = (xdev(d), xdev(-d), sib, xdev(d), sib, sib, sib)[i]
        return ag_send(q, j, slot if i < 3 else at(s), i, dev)

    def all_gather(q, sq, gain_row, consume):
        inv = lax.rsqrt(sq / dim + NORM_EPS)
        rows_of = (g2_v, g3_v, g4_v)[gain_row][...].astype(jnp.float32)
        for j in range(NC):
            gain = jnp.concatenate([rows_of[i:i + 1] for i in range(j * cw // 128, (j + 1) * cw // 128)], axis=1)
            xa[q, j, slot] = (hst[j] * inv * gain).astype(jnp.bfloat16).astype(jnp.float32)
            for k in range(3):
                ag_copy(q, j, k).start()

        def first(j):
            d = turn(j)
            ag_got(q, j, at(-d)).wait_recv()
            ag_copy(q, j, 3).start()
            ag_copy(q, j, 4).start()
            ag_got(q, j, at(d)).wait_recv()
            ag_copy(q, j, 5).start()

        loop(NC, first)

        def body(j):
            @pl.when(j < NC)
            def _():
                ag_got(q, j, at(2)).wait_recv()
                ag_copy(q, j, 6).start()

            @pl.when(j >= 1)
            def _():
                for k in range(4):
                    ag_got(q, j - 1, (1 - c) * 4 + k).wait_recv()
                consume(j - 1, xa[q, j - 1].reshape(2 * half, cw).astype(jnp.bfloat16))

        loop(NC + 1, body)

    def mlp_hidden(q, sq, gain_row, wait_gu):
        acc[...] = jnp.zeros_like(acc)

        def consume(j, xs):
            wait_gu(j)
            acc[:, :mlp] += fdot(xs, wg_v[j])
            acc[:, mlp:] += fdot(xs, wu_v[j])

        all_gather(q, sq, gain_row, consume)
        gv = acc[:, :mlp].astype(jnp.bfloat16).astype(jnp.float32)
        uv = acc[:, mlp:].astype(jnp.bfloat16).astype(jnp.float32)
        act[...] = (jax.nn.silu(gv) * uv).astype(jnp.bfloat16)

    def part_wo(j):
        ld_wo(j).wait()
        return fdot(ob[...], wo_v[j])

    reduce_scatter(0, part_wo)
    hid_cp.wait()
    sq = new_rows(0, None)

    def wait_self(j):
        ld_wg(j).wait()
        ld_wu(j).wait()

    mlp_hidden(0, sq, 0, wait_self)

    def start_cgu(j):
        ld_cg(j).start()
        ld_cu(j).start()

    loop(NC, start_cgu)

    def part_wd(j):
        ld_wd(j).wait()
        return fdot(act[...], wd_v[j])

    reduce_scatter(1, part_wd)
    loop(NC, lambda j: ld_cd(j).start())
    sq = new_rows(1, None)

    acc[:, :hw] = jnp.zeros((2 * half, hw), jnp.float32)

    def consume_q(j, xs):
        ld_cq(j).wait()
        acc[:, :hw] += fdot(xs, cq_v[j])

    all_gather(1, sq, 1, consume_q)
    qgain = qn_v[...].astype(jnp.float32)
    for h in range(heads):
        qh = acc[:, h * hd:(h + 1) * hd].astype(jnp.bfloat16).astype(jnp.float32)
        qinv = lax.rsqrt(jnp.mean(qh * qh, axis=1, keepdims=True) + NORM_EPS)
        q3[:, h, :] = (qh * qinv * qgain).astype(jnp.bfloat16).astype(jnp.float32)
    xv_cp.wait()

    nat = 16

    def attend(t):
        for u in range(nat // 8):
            ld_kc(t * (nat // 8) + u).wait()
            ld_vc(t * (nat // 8) + u).wait()

        def scores(us):
            return [lax.dot_general(q3[t * nat + u].astype(jnp.bfloat16), kc_v[t * nat + u], (((1,), (1,)), ((), ())),
                                    preferred_element_type=jnp.float32) * scale for u in us]

        def soften(us, scs):
            out = []
            for u, sc in zip(us, scs):
                valid = jnp.broadcast_to(xvs[u // 8][u % 8:u % 8 + 1], (8, ntok)) > 0
                sc = jnp.where(valid, sc, NEG_BIG)
                mx = jnp.max(sc, axis=1, keepdims=True)
                pr = jnp.where(valid, jnp.exp(sc - mx), 0.0)
                out.append((pr.astype(jnp.bfloat16), jnp.sum(pr, axis=1, keepdims=True)))
            return out

        def mix(us, prs):
            return [fdot(pr, vc_v[t * nat + u]) / ls for u, (pr, ls) in zip(us, prs)]

        xvs = [xv_v[pl.ds(pl.multiple_of(t * nat + 8 * u, 8), 8), :] for u in range(nat // 8)]
        one, two = range(nat // 2), range(nat // 2, nat)
        sa = scores(one)
        sb = scores(two)
        oa = mix(one, soften(one, sa))
        o2 = mix(two, soften(two, sb))
        for u, o in enumerate(oa + o2):
            oc[t * nat + u] = o

    loop(2 * half // nat, attend)
    for h in range(heads):
        ob[:, h * hd:(h + 1) * hd] = oc[:, h, :].astype(jnp.bfloat16)

    def part_cwo(j):
        ld_cwo(j).wait()
        return fdot(ob[...], cwo_v[j])

    reduce_scatter(2, part_cwo)
    nrow = rowm_v.shape[1]
    mine = (y * 8 + slot) * 8 + lax.broadcasted_iota(jnp.int32, (8, nrow), 0)
    pick = lax.broadcasted_iota(jnp.int32, (8, nrow), 1) == mine
    rmask = jnp.sum(jnp.where(pick, jnp.broadcast_to(rowm_v[...], (8, nrow)), 0).astype(jnp.float32), axis=1, keepdims=True)
    factor = [jnp.tanh(jnp.full((8, 128), gate_s[k], jnp.float32))[:, :1] * rmask for k in range(2)]
    sq = new_rows(2, factor[0])

    def wait_cross(j):
        ld_cg(j).wait()
        ld_cu(j).wait()

    mlp_hidden(2, sq, 2, wait_cross)

    def part_cd(j):
        ld_cd(j).wait()
        return fdot(act[...], wd_v[j])

    reduce_scatter(3, part_cd)

    def parts_of(j):
        if j < NC // 2:
            return (lambda k: og.at[j, c, y, ring(x + k)], xdev), (lambda k: og.at[j, c, ring(y + k)], ydev)
        return (lambda k: og.at[j, c, ring(y + k), x], ydev), (lambda k: og.at[j, c, :, ring(x + k)], xdev)

    def fg(j, stage, k, s, what, dev):
        return rcopy(what, what, fg_s.at[j, stage, s], fg_r.at[j, stage, k], dev)

    fg_all = []
    plans = []
    for j in range(NC):
        d = 1 - 2 * (j % 2)
        stages = []
        for stage, (region, dev) in enumerate(parts_of(j)):
            stages.append(dict(
                own=[fg(j, stage, 0, 0, region(0), dev(d)), fg(j, stage, 1, 1, region(0), dev(-d))],
                relay=fg(j, stage, 2, 2, region(-d), dev(d)),
                got=[fg(j, stage, 0, 0, region(-d), sib), fg(j, stage, 1, 1, region(d), sib), fg(j, stage, 2, 2, region(2), sib)],
                pair=[fg(j, 2, i, i, region(k), sib) for i, k in enumerate((0, -d, d, 2))],
            ))
        plans.append(stages)
    order = range(NC)
    for j in order:
        og[j, c, y, x] = (hst[j] + factor[1] * reduced(3, j)).astype(jnp.bfloat16).astype(jnp.float32)
        for cp in plans[j][0]['own']:
            cp.start()
    for j in order:
        st = plans[j][0]
        st['got'][0].wait_recv()
        st['relay'].start()
    for j in order:
        st, nx = plans[j]
        st['got'][1].wait_recv()
        st['got'][2].wait_recv()
        for cp in nx['own']:
            cp.start()
        nx['pair'][0].start()
    for j in order:
        st = plans[j][1]
        st['got'][0].wait_recv()
        st['relay'].start()
        st['pair'][1].start()
        st['got'][1].wait_recv()
        st['pair'][2].start()
    for j in order:
        st = plans[j][1]
        st['got'][2].wait_recv()
        st['pair'][3].start()
    for j in order:
        for cp in plans[j][1]['pair']:
            cp.wait_recv()
        for yy in range(4):
            for cc in range(2):
                out_v[yy * 8 + cc * 4:yy * 8 + cc * 4 + 4, :, j * cw:(j + 1) * cw] = og[j, cc, yy].astype(jnp.bfloat16)

    for j, d in ((0, 1), (1, -1)):
        y_relay(j, d).wait_send()
        y_direct(j, d).wait_send()
        y_final(j, d).wait_send()

    def drain_rs(j):
        for p in range(4):
            rs_pair(p, j).wait_send()
            rs_relay(p, j).wait_send()
            rs_direct(p, j).wait_send()
            rs_final(p, j).wait_send()
        for q in range(3):
            for i in range(7):
                ag_copy(q, j, i).wait_send()

    loop(NC, drain_rs)
    for j in range(NC):
        for st in plans[j]:
            for cp in st['own']:
                cp.wait_send()
            st['relay'].wait_send()
        for cp in plans[j][1]['pair']:
            cp.wait_send()


def tail(blk, hidden, gains, rowmask, gates, xvalid, k_cross, v_cross, wo, wg, wu, wd, cq, cwo, cg, cu, cd, heads, hd):
    batch, dim = hidden.shape
    mlp = wg.shape[1]
    ntok = xvalid.shape[1]
    cw = dim // NC
    hw = heads * hd
    bl = batch // 4
    half = bl // 2
    f32, bf16 = jnp.float32, jnp.bfloat16
    anyspec = pl.BlockSpec(memory_space=pl.ANY)
    vmem = pl.BlockSpec(memory_space=pltpu.VMEM)
    smem = pl.BlockSpec(memory_space=pltpu.SMEM)
    dma = pltpu.SemaphoreType.DMA
    scratch = [
        pltpu.VMEM((4, 2, half, hw + hd), f32),
        pltpu.VMEM((2, half, hw + hd), f32),
        pltpu.VMEM((2, half, hw + hd), f32),
        pltpu.VMEM((2, half, hw + hd), f32),
        pltpu.VMEM((2, half, hw + hd), f32),
        pltpu.VMEM((bl, hw), bf16),
        pltpu.VMEM((8, dim), bf16),
        pltpu.VMEM((NC, 8, cw), f32),
        pltpu.VMEM((NC, hw, cw), bf16),
        pltpu.VMEM((NC, cw, mlp), bf16),
        pltpu.VMEM((NC, cw, mlp), bf16),
        pltpu.VMEM((NC, mlp, cw), bf16),
        pltpu.VMEM((NC, cw, hw), bf16),
        pltpu.VMEM((NC, hw, cw), bf16),
        pltpu.VMEM((bl, ntok, hd), bf16),
        pltpu.VMEM((bl, ntok, hd), bf16),
        pltpu.VMEM((bl, ntok), jnp.int32),
        pltpu.VMEM((4, NC, 2, half, cw), f32),
        pltpu.VMEM((4, NC, half, cw), f32),
        pltpu.VMEM((4, NC, 4, 8, cw), f32),
        pltpu.VMEM((4, NC, 8, cw), f32),
        pltpu.VMEM((4, NC, 8, cw), f32),
        pltpu.VMEM((4, NC, 8, cw), f32),
        pltpu.VMEM((4, NC, 8, cw), f32),
        pltpu.VMEM((3, NC, 8, 8, cw), f32),
        pltpu.VMEM((NC, 2, 4, 4, 8, cw), f32),
        pltpu.VMEM((bl, 2 * mlp), f32),
        pltpu.VMEM((bl, mlp), bf16),
        pltpu.VMEM((bl, 8, hd), f32),
        pltpu.VMEM((bl, 8, hd), f32),
        dma((3,)),
        dma((9, NC)),
        dma((2, 8)),
        dma((3, 2)),
        dma((3, 2)),
        dma((4, 4, NC)),
        dma((4, 4, NC)),
        dma((3, NC, 7)),
        dma((3, NC, 8)),
        dma((NC, 3, 4)),
        dma((NC, 3, 4)),
    ]
    out = pl.pallas_call(
        functools.partial(tail_kernel, (heads, hd, dim, mlp, ntok)),
        out_shape=jax.ShapeDtypeStruct((batch // 8, 8, dim), bf16),
        in_specs=[anyspec, anyspec] + [vmem] * 5 + [smem] + [anyspec] * 12,
        out_specs=vmem,
        scratch_shapes=scratch,
        compiler_params=pltpu.CompilerParams(collective_id=0, has_side_effects=True, vmem_limit_bytes=67043328),
        name='tail',
    )(blk.reshape(4, 2, half, hw + hd), hidden.reshape(batch // 8, 8, dim),
      *[g.reshape(-1, 128) for g in gains], rowmask.reshape(1, batch), gates,
      xvalid.reshape(4, bl, ntok), k_cross.reshape(4, bl, ntok, hd), v_cross.reshape(4, bl, ntok, hd),
      wo, wg, wu, wd, cq, cwo, cg, cu, cd)
    return out.reshape(batch, dim)


def solution(mesh):
    cache_spec = P('dp', 'sp', 'tp', None)
    cross_spec = P('dp', None, 'tp', None)
    row_spec = P('dp', None)
    vec_spec = P('dp')
    full_spec = P(None)
    col_spec = P(None, 'tp')
    split_rows = P('tp', None)
    in_specs = (row_spec, vec_spec, cache_spec, cache_spec, cross_spec, cross_spec, row_spec, vec_spec,
                full_spec, col_spec, col_spec, col_spec, split_rows, full_spec, col_spec, col_spec, split_rows,
                full_spec, col_spec, full_spec, split_rows, full_spec, full_spec, col_spec, col_spec, split_rows)
    out_specs = (row_spec, cache_spec, cache_spec)

    def local_step(hidden, new_pos, k_self, v_self, k_cross, v_cross, xvalid, rowmask,
                   self_attn_norm, self_wq, self_wk, self_wv, self_wo, self_mlp_norm,
                   self_wgate, self_wup, self_wdown, cross_attn_norm, cross_wq, cross_qnorm,
                   cross_wo, cross_gates, cross_mlp_norm, cross_wgate, cross_wup, cross_wdown):
        head_dim = k_self.shape[3]
        heads_local = self_wq.shape[1] // head_dim
        k_new_cache, v_new_cache, blk = front(hidden, new_pos, k_self, v_self, self_attn_norm, self_wq, self_wk, self_wv,
                                              heads_local, head_dim)
        gains = (self_mlp_norm, cross_attn_norm, cross_mlp_norm, cross_qnorm)
        h4 = tail(blk, hidden, gains, rowmask, cross_gates, xvalid, k_cross, v_cross, self_wo, self_wgate, self_wup, self_wdown,
                  cross_wq, cross_wo, cross_wgate, cross_wup, cross_wdown, heads_local, head_dim)
        return h4, k_new_cache, v_new_cache

    return jax.shard_map(local_step, mesh=mesh, in_specs=in_specs, out_specs=out_specs, check_vma=False)
```

```python
import functools
import math
import jax
import jax.numpy as jnp
import numpy as np
from jax import lax
from jax.experimental import pallas as pl
from jax.experimental.pallas import tpu as pltpu
from jax.sharding import PartitionSpec as P

NORM_EPS = 1e-5
ROPE_THETA = 500000.0
ROPE_FACTOR = 8.0
LOW_FREQ = 1.0
HIGH_FREQ = 4.0
ORIG_CTX = 8192.0
NEG_BIG = -1e30
NC = 4
MESH = pl.DeviceIdType.MESH


def rope_freqs(head_dim):
    inv_freq = (1.0 / (ROPE_THETA ** (np.arange(0, head_dim, 2).astype(np.float32) / np.float32(head_dim)))).astype(np.float32)
    wavelen = 2.0 * math.pi / inv_freq
    smooth = (ORIG_CTX / wavelen - LOW_FREQ) / (HIGH_FREQ - LOW_FREQ)
    mid_freq = (1.0 - smooth) * inv_freq / ROPE_FACTOR + smooth * inv_freq
    scaled = np.where(wavelen > ORIG_CTX / LOW_FREQ, inv_freq / ROPE_FACTOR, mid_freq)
    half = np.where(wavelen < ORIG_CTX / HIGH_FREQ, inv_freq, scaled).astype(np.float32)
    return np.concatenate([half, half])[None, :]


def fdot(a, b):
    return jnp.dot(a, b, preferred_element_type=jnp.float32)


def front_kernel(cfg, hid_h, posr_v, pos_s, gain_v, freq_v, wq_h, wk_h, wv_h, k_h, v_h, ko_h, vo_h, blk_v,
                 hid_v, xn, wq_v, wk_v, wv_v, kc, vc, q3, o3, st3, kn, vn, in_sem, kv_sem, out_sem):
    heads, hd, dim, batch, slots = cfg
    f32, bf16 = jnp.float32, jnp.bfloat16
    per = 32
    nch = batch // per
    scale = hd ** -0.5
    first_slot = lax.axis_index('sp') * slots

    def loop(n, body):
        def step(i, carry):
            body(i)
            return carry
        lax.fori_loop(0, n, step, 0)

    def ld_hid(r):
        span = pl.ds(pl.multiple_of(r * per, per), per)
        return pltpu.make_async_copy(hid_h.at[span], hid_v.at[span], in_sem.at[3 + r])

    weights = [pltpu.make_async_copy(h, v, in_sem.at[i]) for i, (h, v) in enumerate(((wq_h, wq_v), (wk_h, wk_v), (wv_h, wv_v)))]

    def ld_kv(g):
        span = pl.ds(g * per, per)
        return (pltpu.make_async_copy(k_h.at[span], kc.at[span], kv_sem.at[0, g]),
                pltpu.make_async_copy(v_h.at[span], vc.at[span], kv_sem.at[1, g]))

    def st_kv(g):
        span = pl.ds(g * per, per)
        return (pltpu.make_async_copy(kc.at[span], ko_h.at[span], out_sem.at[0, g]),
                pltpu.make_async_copy(vc.at[span], vo_h.at[span], out_sem.at[1, g]))

    def start_both(pair):
        pair[0].start()
        pair[1].start()

    def wait_both(pair):
        pair[0].wait()
        pair[1].wait()

    loop(nch, lambda r: ld_hid(r).start())
    for cp in weights:
        cp.start()
    loop(nch, lambda g: start_both(ld_kv(g)))
    q3[...] = jnp.zeros_like(q3)

    gain = gain_v[...].astype(f32)

    def norm(r):
        ld_hid(r).wait()
        span = pl.ds(pl.multiple_of(r * per, per), per)
        xs = hid_v[span, :].astype(f32)
        inv = lax.rsqrt(jnp.sum(xs * xs, axis=1, keepdims=True) / dim + NORM_EPS)
        for k in range(dim // 128):
            xn[span, k * 128:(k + 1) * 128] = (xs[:, k * 128:(k + 1) * 128] * inv * gain[k:k + 1]).astype(bf16)

    loop(nch, norm)
    eye = lax.broadcasted_iota(jnp.int32, (batch, batch), 0) == lax.broadcasted_iota(jnp.int32, (batch, batch), 1)
    posc = jnp.sum(jnp.where(eye, jnp.broadcast_to(posr_v[...], (batch, batch)).astype(f32), 0.0), axis=1, keepdims=True)
    angles = posc * freq_v[...]
    cos_t = jnp.cos(angles)
    low = lax.broadcasted_iota(jnp.int32, (batch, hd), 1) < hd // 2
    sin_t = jnp.where(low, -jnp.sin(angles), jnp.sin(angles))

    def rope(v):
        r = v.astype(bf16).astype(f32)
        return (r * cos_t + pltpu.roll(r, hd // 2, 1) * sin_t).astype(bf16).astype(f32)

    for cp in weights:
        cp.wait()
    q = fdot(xn[...], wq_v[...])
    for h in range(heads):
        q3[:, h, :] = rope(q[:, h * hd:(h + 1) * hd])
    kn[...] = rope(fdot(xn[...], wk_v[...]))
    vn[...] = fdot(xn[...], wv_v[...]).astype(bf16).astype(f32)

    lane = lax.broadcasted_iota(jnp.int32, (8, 128), 1)
    sub = lax.broadcasted_iota(jnp.int32, (8, 128), 0)
    row16 = lax.broadcasted_iota(jnp.int32, (16, hd), 0)
    zero = jnp.zeros((8, 128), f32)

    def attend(g):
        wait_both(ld_kv(g))
        lps = []
        for i in range(per):
            b = g * per + i
            lp = pos_s[b] - first_slot
            lps.append(lp)
            base = pl.multiple_of(lax.shift_left(lax.shift_right_logical(jnp.clip(lp, 0, slots - 1), 4), 4), 16)
            hit = row16 + base == lp
            for ref, new in ((kc, kn), (vc, vn)):
                old = ref[b, pl.ds(base, 16), :].astype(f32)
                fresh = jnp.broadcast_to(new[pl.ds(b, 1), :], (16, hd))
                ref[b, pl.ds(base, 16), :] = jnp.where(hit, fresh, old).astype(bf16)
        start_both(st_kv(g))
        fours = [pl.ds(g * per + 4 * t, 4) for t in range(per // 4)]

        def scores(ts):
            return [lax.dot_general(q3[fours[t]].reshape(32, hd).astype(bf16), kc[fours[t]].reshape(4 * slots, hd),
                                    (((1,), (1,)), ((), ())), preferred_element_type=f32) * scale for t in ts]

        def soften(ts, sgs):
            out = []
            for t, sg in zip(ts, sgs):
                probs, stats = [], []
                for i in range(4):
                    off = slots * (i % 2)
                    lp = jnp.minimum(lps[4 * t + i], slots - 1)
                    seen = (lane >= off) & (lane <= off + lp)
                    sc = jnp.where(seen, sg[8 * i:8 * i + 8, 128 * (i // 2):128 * (i // 2) + 128], NEG_BIG)
                    mx = jnp.max(sc, axis=1, keepdims=True)
                    pr = jnp.where(seen, jnp.exp(sc - mx), 0.0)
                    ls = jnp.sum(pr, axis=1, keepdims=True)
                    stats.append(jnp.where(lane == sub, mx, jnp.where(lane == sub + 8, ls, 0.0)))
                    probs.append(jnp.concatenate([pr, zero] if i < 2 else [zero, pr], axis=1))
                out.append((jnp.concatenate(probs, axis=0).astype(bf16), stats))
            return out

        def mix(ts, prs):
            return [fdot(pg, vc[fours[t]].reshape(4 * slots, hd)) for t, (pg, _) in zip(ts, prs)]

        one, two = range(per // 8), range(per // 8, per // 4)
        sa = scores(one)
        sb = scores(two)
        pa = soften(one, sa)
        oa = mix(one, pa)
        pb = soften(two, sb)
        o2 = mix(two, pb)
        for t, (o, (_, stats)) in enumerate(zip(oa + o2, pa + pb)):
            o3[fours[t]] = o.reshape(4, 8, hd)
            for i in range(4):
                st3[g * per + 4 * t + i] = stats[i]

    loop(nch, attend)
    stat = st3[:, 0, :]
    for h in range(1, heads):
        stat = stat + st3[:, h, :]
    for h in range(heads):
        blk_v[:, h * hd:(h + 1) * hd] = o3[:, h, :]
    blk_v[:, heads * hd:] = stat
    loop(nch, lambda g: wait_both(st_kv(g)))


def front(hidden, new_pos, k_self, v_self, gain, wq, wk, wv, heads, hd):
    batch, dim = hidden.shape
    slots = k_self.shape[1]
    f32, bf16 = jnp.float32, jnp.bfloat16
    anyspec = pl.BlockSpec(memory_space=pl.ANY)
    vmem = pl.BlockSpec(memory_space=pltpu.VMEM)
    smem = pl.BlockSpec(memory_space=pltpu.SMEM)
    dma = pltpu.SemaphoreType.DMA
    nch = batch // 32
    cache = jax.ShapeDtypeStruct((batch, slots, hd), bf16)
    ko, vo, blk = pl.pallas_call(
        functools.partial(front_kernel, (heads, hd, dim, batch, slots)),
        out_shape=(cache, cache, jax.ShapeDtypeStruct((batch, heads * hd + hd), f32)),
        in_specs=[anyspec, vmem, smem, vmem, vmem] + [anyspec] * 5,
        out_specs=(anyspec, anyspec, vmem),
        scratch_shapes=[
            pltpu.VMEM((batch, dim), bf16),
            pltpu.VMEM((batch, dim), bf16),
            pltpu.VMEM(wq.shape, bf16),
            pltpu.VMEM(wk.shape, bf16),
            pltpu.VMEM(wv.shape, bf16),
            pltpu.VMEM((batch, slots, hd), bf16),
            pltpu.VMEM((batch, slots, hd), bf16),
            pltpu.VMEM((batch, 8, hd), f32),
            pltpu.VMEM((batch, 8, hd), f32),
            pltpu.VMEM((batch, 8, hd), f32),
            pltpu.VMEM((batch, hd), f32),
            pltpu.VMEM((batch, hd), f32),
            dma((3 + nch,)),
            dma((2, nch)),
            dma((2, nch)),
        ],
        compiler_params=pltpu.CompilerParams(vmem_limit_bytes=60000000),
        name='front',
    )(hidden, new_pos.reshape(1, batch), new_pos, gain.reshape(dim // 128, 128), jnp.asarray(rope_freqs(hd)),
      wq, wk, wv, k_self.reshape(batch, slots, hd), v_self.reshape(batch, slots, hd))
    return ko.reshape(k_self.shape), vo.reshape(v_self.shape), blk


def tail_kernel(cfg, blk_h, hid_h, g2_v, g3_v, g4_v, qn_v, rowm_v, gate_s, xv_h, kc_h, vc_h,
                wo_h, wg_h, wu_h, wd_h, cq_h, cwo_h, cg_h, cu_h, cd_h, out_v,
                bk, yr, yd, yt, yf, ob, hrow, hst,
                wo_v, wg_v, wu_v, wd_v, cq_v, cwo_v, kc_v, vc_v, xv_v,
                pbuf, dbuf, s0, s1, r1, r2, xa, og, acc, act, q3, oc, fac,
                ld_sem, w_sem, kv_sem, ys, yrs, pr_s, pr_r, ar_s, ar_r, lr_s, lr_r, xs_s, xs_r, fg_s, fg_r):
    heads, hd, dim, mlp, ntok = cfg
    cw = dim // NC
    hw = heads * hd
    half = 32
    x = lax.axis_index('tp') // 2
    c = lax.axis_index('tp') % 2
    y = lax.axis_index('sp')
    flip = x + 1 - 2 * lax.rem(x, 2)
    cross = 3 - x
    scale = hd ** -0.5

    def ring(v):
        return lax.rem(v + 8, 4)

    def xdev(d):
        return {'tp': 2 * ring(x + d) + c}

    def ydev(d):
        return {'sp': ring(y + d)}

    sib = {'tp': 2 * x + 1 - c}

    def rcopy(src, dst, ss, rs, dev):
        return pltpu.make_async_remote_copy(src_ref=src, dst_ref=dst, send_sem=ss, recv_sem=rs,
                                            device_id=dev, device_id_type=MESH)

    def loop(n, body):
        def step(i, carry):
            body(i)
            return carry
        lax.fori_loop(0, n, step, 0)

    blk_cp = pltpu.make_async_copy(blk_h, bk, ld_sem.at[0])
    hid_cp = pltpu.make_async_copy(hid_h.at[y * 2 + c], hrow, ld_sem.at[1])
    xv_cp = pltpu.make_async_copy(xv_h.at[y], xv_v, ld_sem.at[2])

    def cols(h, v, k, j):
        return pltpu.make_async_copy(h.at[:, pl.ds(pl.multiple_of(j * cw, 128), cw)], v.at[j], w_sem.at[k, j])

    def rows(h, v, k, j):
        return pltpu.make_async_copy(h.at[pl.ds(pl.multiple_of(j * cw, 128), cw)], v.at[j], w_sem.at[k, j])

    def ld_wo(j):
        return cols(wo_h, wo_v, 0, j)

    def ld_wg(j):
        return rows(wg_h, wg_v, 1, j)

    def ld_wu(j):
        return rows(wu_h, wu_v, 2, j)

    def ld_wd(j):
        return cols(wd_h, wd_v, 3, j)

    def ld_cq(j):
        return rows(cq_h, cq_v, 4, j)

    def ld_cwo(j):
        return cols(cwo_h, cwo_v, 5, j)

    def ld_cg(j):
        return rows(cg_h, wg_v, 6, j)

    def ld_cu(j):
        return rows(cu_h, wu_v, 7, j)

    def ld_cd(j):
        return cols(cd_h, wd_v, 8, j)

    def ld_kc(g):
        return pltpu.make_async_copy(kc_h.at[y, pl.ds(g * 8, 8)], kc_v.at[pl.ds(g * 8, 8)], kv_sem.at[0, g])

    def ld_vc(g):
        return pltpu.make_async_copy(vc_h.at[y, pl.ds(g * 8, 8)], vc_v.at[pl.ds(g * 8, 8)], kv_sem.at[1, g])

    blk_cp.start()
    hid_cp.start()
    xv_cp.start()
    loop(NC, lambda j: ld_wo(j).start())

    barrier = pltpu.get_barrier_semaphore()
    for dev in (sib, xdev(1), xdev(-1), ydev(1), ydev(-1)):
        pl.semaphore_signal(barrier, inc=1, device_id=dev, device_id_type=MESH)

    def start_gu(j):
        ld_wg(j).start()
        ld_wu(j).start()

    loop(NC, start_gu)
    loop(NC, lambda j: ld_wd(j).start())
    loop(NC, lambda j: ld_cq(j).start())

    def start_kv(g):
        ld_kc(g).start()
        ld_vc(g).start()

    loop(8, start_kv)
    loop(NC, lambda j: ld_cwo(j).start())
    q3[...] = jnp.zeros_like(q3)
    nrow = rowm_v.shape[1]
    mine = (y * 2 + c) * half + lax.broadcasted_iota(jnp.int32, (half, nrow), 0)
    pick = lax.broadcasted_iota(jnp.int32, (half, nrow), 1) == mine
    rmask = jnp.sum(jnp.where(pick, jnp.broadcast_to(rowm_v[...], (half, nrow)), 0).astype(jnp.float32), axis=1, keepdims=True)
    for k in range(2):
        fac[k] = (jnp.tanh(jnp.full((half, 128), gate_s[k], jnp.float32)) * rmask).reshape(4, 8, 128)
    pl.semaphore_wait(barrier, 5)

    lane = lax.broadcasted_iota(jnp.int32, (half, hd), 1)

    def merge(a, b):
        outs, ms, ls = [], [], []
        for h in range(heads):
            ma, mb = a[:, hw + h:hw + h + 1], b[:, hw + h:hw + h + 1]
            la, lb = a[:, hw + 8 + h:hw + 9 + h], b[:, hw + 8 + h:hw + 9 + h]
            mm = jnp.maximum(ma, mb)
            ea, eb = jnp.exp(ma - mm), jnp.exp(mb - mm)
            outs.append(a[:, h * hd:(h + 1) * hd] * ea + b[:, h * hd:(h + 1) * hd] * eb)
            ms.append(mm)
            ls.append(la * ea + lb * eb)
        stat = jnp.zeros((half, hd), jnp.float32)
        for h in range(heads):
            stat = jnp.where(lane == h, ms[h], stat)
            stat = jnp.where(lane == 8 + h, ls[h], stat)
        return jnp.concatenate(outs + [stat], axis=1), ls

    def y_relay(j, d):
        return rcopy(bk.at[ring(y + 2), j], yr.at[j], ys.at[0, j], yrs.at[0, j], ydev(d))

    def y_direct(j, d):
        return rcopy(bk.at[ring(y - d), j], yd.at[j], ys.at[1, j], yrs.at[1, j], ydev(-d))

    def y_final(j, d):
        return rcopy(yt.at[j], yf.at[j], ys.at[2, j], yrs.at[2, j], ydev(d))

    blk_cp.wait()
    for j, d in ((0, 1), (1, -1)):
        y_relay(j, d).start()
    for j, d in ((0, 1), (1, -1)):
        y_direct(j, d).start()
    for j, d in ((0, 1), (1, -1)):
        y_relay(j, d).wait_recv()
        yt[j] = merge(bk[ring(y + d), j], yr[j])[0]
        y_final(j, d).start()
    for j, d in ((0, 1), (1, -1)):
        y_direct(j, d).wait_recv()
        first = merge(bk[y, j], yd[j])[0]
        y_final(j, d).wait_recv()
        both, sums = merge(first, yf[j])
        for h in range(heads):
            ob[j * half:(j + 1) * half, h * hd:(h + 1) * hd] = (both[:, h * hd:(h + 1) * hd] / sums[h]).astype(jnp.bfloat16)

    def pair_cp(j):
        return rcopy(pbuf.at[j, 1 - c], dbuf.at[j], pr_s.at[j], pr_r.at[j], sib)

    def mate(j, second):
        odd = lax.rem(j + second, 2)
        return {'tp': 2 * (flip + odd * (cross - flip)) + c}

    def one_cp(p, j):
        return rcopy(s0.at[j], r1.at[p % 2, j], ar_s.at[0, j], ar_r.at[p % 2, 0, j], mate(j, 0))

    def two_cp(p, j):
        return rcopy(s1.at[j], r2.at[p % 2, j], ar_s.at[1, j], ar_r.at[p % 2, 1, j], mate(j, 1))

    def pair_sums(p, partial, after):
        def body(j):
            @pl.when(j < NC)
            def _():
                if p > 0:
                    pair_cp(j).wait_send()
                pbuf[j] = partial(j).reshape(2, half, cw)
                pair_cp(j).start()

            @pl.when(j >= 1)
            def _():
                pair_cp(j - 1).wait_recv()
                if p > 0:
                    one_cp(p, j - 1).wait_send()
                s0[j - 1] = (pbuf[j - 1, c] + dbuf[j - 1]).reshape(4, 8, cw)
                after(j - 1)

        loop(NC + 1, body)

    def all_reduce(p, partial):
        pair_sums(p, partial, lambda j: one_cp(p, j).start())

        def step(j):
            one_cp(p, j).wait_recv()
            if p > 0:
                two_cp(p, j).wait_send()
            s1[j] = s0[j] + r1[p % 2, j]
            two_cp(p, j).start()

        loop(NC, step)

    def new_rows(p, k):
        sq = jnp.zeros((4, 8, 1), jnp.float32)
        for j in range(NC):
            two_cp(p, j).wait_recv()
            add = s1[j] + r2[p % 2, j]
            if k is not None:
                add = fac[k][:, :, :1] * add
            old = hrow[:, :, j * cw:(j + 1) * cw].astype(jnp.float32) if p == 0 else hst[j]
            new = (old + add).astype(jnp.bfloat16).astype(jnp.float32)
            hst[j] = new
            sq = sq + jnp.sum(new * new, axis=2, keepdims=True)
        return sq

    def swap_cp(j):
        return rcopy(xa.at[j, c], xa.at[j, c], xs_s.at[j], xs_r.at[j], sib)

    def all_gather(q, sq, gain_row, consume):
        inv = lax.rsqrt(sq / dim + NORM_EPS)
        rows_of = (g2_v, g3_v, g4_v)[gain_row][...].astype(jnp.float32)
        for j in range(NC):
            gain = jnp.concatenate([rows_of[i:i + 1] for i in range(j * cw // 128, (j + 1) * cw // 128)], axis=1)
            if q > 0:
                swap_cp(j).wait_send()
            xa[j, c] = (hst[j] * inv * gain.reshape(1, 1, cw)).astype(jnp.bfloat16).astype(jnp.float32).reshape(half, cw)
            swap_cp(j).start()

        def body(j):
            swap_cp(j).wait_recv()
            consume(j, xa[j].reshape(2 * half, cw).astype(jnp.bfloat16))

        loop(NC, body)

    def turn(j):
        return 1 - 2 * lax.rem(j, 2)

    def relay_cp(j):
        return rcopy(s0.at[j, ring(x + 2)], r1.at[1, j, 0], lr_s.at[0, j], lr_r.at[0, j], xdev(turn(j)))

    def direct_cp(j):
        return rcopy(s0.at[j, ring(x - turn(j))], r1.at[1, j, 1], lr_s.at[1, j], lr_r.at[1, j], xdev(-turn(j)))

    def last_cp(j):
        return rcopy(s1.at[j, 0], r1.at[1, j, 2], lr_s.at[2, j], lr_r.at[2, j], xdev(turn(j)))

    def last_scatter(partial):
        def send(j):
            relay_cp(j).start()
            direct_cp(j).start()

        pair_sums(3, partial, send)

        def step(j):
            relay_cp(j).wait_recv()
            two_cp(2, j).wait_send()
            s1[j, 0] = s0[j, ring(x + turn(j))] + r1[1, j, 0]
            last_cp(j).start()

        loop(NC, step)

    def last_rows(j):
        direct_cp(j).wait_recv()
        last_cp(j).wait_recv()
        return s0[j, x] + r1[1, j, 1] + r1[1, j, 2]

    def mlp_hidden(q, sq, gain_row, wait_gu):
        acc[...] = jnp.zeros_like(acc)

        def consume(j, xs):
            wait_gu(j)
            acc[:, :mlp] += fdot(xs, wg_v[j])
            acc[:, mlp:] += fdot(xs, wu_v[j])

        all_gather(q, sq, gain_row, consume)
        gv = acc[:, :mlp].astype(jnp.bfloat16).astype(jnp.float32)
        uv = acc[:, mlp:].astype(jnp.bfloat16).astype(jnp.float32)
        act[...] = (jax.nn.silu(gv) * uv).astype(jnp.bfloat16)

    def part_wo(j):
        ld_wo(j).wait()
        return fdot(ob[...], wo_v[j])

    all_reduce(0, part_wo)
    hid_cp.wait()
    sq = new_rows(0, None)

    def wait_self(j):
        ld_wg(j).wait()
        ld_wu(j).wait()

    mlp_hidden(0, sq, 0, wait_self)

    def start_cgu(j):
        ld_cg(j).start()
        ld_cu(j).start()

    loop(NC, start_cgu)

    def part_wd(j):
        ld_wd(j).wait()
        return fdot(act[...], wd_v[j])

    all_reduce(1, part_wd)
    loop(NC, lambda j: ld_cd(j).start())
    sq = new_rows(1, None)

    acc[:, :hw] = jnp.zeros((2 * half, hw), jnp.float32)

    def consume_q(j, xs):
        ld_cq(j).wait()
        acc[:, :hw] += fdot(xs, cq_v[j])

    all_gather(1, sq, 1, consume_q)
    qgain = qn_v[...].astype(jnp.float32)
    for h in range(heads):
        qh = acc[:, h * hd:(h + 1) * hd].astype(jnp.bfloat16).astype(jnp.float32)
        qinv = lax.rsqrt(jnp.mean(qh * qh, axis=1, keepdims=True) + NORM_EPS)
        q3[:, h, :] = (qh * qinv * qgain).astype(jnp.bfloat16).astype(jnp.float32)
    xv_cp.wait()

    nat = 16

    def attend(t):
        for u in range(nat // 8):
            ld_kc(t * (nat // 8) + u).wait()
            ld_vc(t * (nat // 8) + u).wait()

        def scores(us):
            return [lax.dot_general(q3[t * nat + u].astype(jnp.bfloat16), kc_v[t * nat + u], (((1,), (1,)), ((), ())),
                                    preferred_element_type=jnp.float32) * scale for u in us]

        def soften(us, scs):
            out = []
            for u, sc in zip(us, scs):
                valid = jnp.broadcast_to(xvs[u // 8][u % 8:u % 8 + 1], (8, ntok)) > 0
                sc = jnp.where(valid, sc, NEG_BIG)
                mx = jnp.max(sc, axis=1, keepdims=True)
                pr = jnp.where(valid, jnp.exp(sc - mx), 0.0)
                out.append((pr.astype(jnp.bfloat16), jnp.sum(pr, axis=1, keepdims=True)))
            return out

        def mix(us, prs):
            return [fdot(pr, vc_v[t * nat + u]) / ls for u, (pr, ls) in zip(us, prs)]

        xvs = [xv_v[pl.ds(pl.multiple_of(t * nat + 8 * u, 8), 8), :] for u in range(nat // 8)]
        one, two = range(nat // 2), range(nat // 2, nat)
        sa = scores(one)
        sb = scores(two)
        oa = mix(one, soften(one, sa))
        o2 = mix(two, soften(two, sb))
        for u, o in enumerate(oa + o2):
            oc[t * nat + u] = o

    loop(2 * half // nat, attend)
    for h in range(heads):
        ob[:, h * hd:(h + 1) * hd] = oc[:, h, :].astype(jnp.bfloat16)

    def part_cwo(j):
        ld_cwo(j).wait()
        return fdot(ob[...], cwo_v[j])

    all_reduce(2, part_cwo)
    sq = new_rows(2, 0)

    def wait_cross(j):
        ld_cg(j).wait()
        ld_cu(j).wait()

    mlp_hidden(2, sq, 2, wait_cross)

    def part_cd(j):
        ld_cd(j).wait()
        return fdot(act[...], wd_v[j])

    last_scatter(part_cd)

    def parts_of(j):
        if j < NC // 2:
            return (lambda k: og.at[j, c, y, ring(x + k)], xdev), (lambda k: og.at[j, c, ring(y + k)], ydev)
        return (lambda k: og.at[j, c, ring(y + k), x], ydev), (lambda k: og.at[j, c, :, ring(x + k)], xdev)

    def fg(j, stage, k, s, what, dev):
        return rcopy(what, what, fg_s.at[j, stage, s], fg_r.at[j, stage, k], dev)

    fg_all = []
    plans = []
    for j in range(NC):
        d = 1 - 2 * (j % 2)
        stages = []
        for stage, (region, dev) in enumerate(parts_of(j)):
            stages.append(dict(
                own=[fg(j, stage, 0, 0, region(0), dev(d)), fg(j, stage, 1, 1, region(0), dev(-d))],
                relay=fg(j, stage, 2, 2, region(-d), dev(d)),
                got=[fg(j, stage, 0, 0, region(-d), sib), fg(j, stage, 1, 1, region(d), sib), fg(j, stage, 2, 2, region(2), sib)],
                pair=[fg(j, 2, i, i, region(k), sib) for i, k in enumerate((0, -d, d, 2))],
            ))
        plans.append(stages)
    order = range(NC)
    for j in order:
        og[j, c, y, x] = (hst[j, x] + fac[1, x][:, :1] * last_rows(j)).astype(jnp.bfloat16).astype(jnp.float32)
        for cp in plans[j][0]['own']:
            cp.start()
    for j in order:
        st = plans[j][0]
        st['got'][0].wait_recv()
        st['relay'].start()
    for j in order:
        st, nx = plans[j]
        st['got'][1].wait_recv()
        st['got'][2].wait_recv()
        for cp in nx['own']:
            cp.start()
        nx['pair'][0].start()
    for j in order:
        st = plans[j][1]
        st['got'][0].wait_recv()
        st['relay'].start()
        st['pair'][1].start()
        st['got'][1].wait_recv()
        st['pair'][2].start()
    for j in order:
        st = plans[j][1]
        st['got'][2].wait_recv()
        st['pair'][3].start()
    for j in order:
        for cp in plans[j][1]['pair']:
            cp.wait_recv()
        for yy in range(4):
            for cc in range(2):
                out_v[yy * 8 + cc * 4:yy * 8 + cc * 4 + 4, :, j * cw:(j + 1) * cw] = og[j, cc, yy].astype(jnp.bfloat16)

    for j, d in ((0, 1), (1, -1)):
        y_relay(j, d).wait_send()
        y_direct(j, d).wait_send()
        y_final(j, d).wait_send()

    def drain(j):
        pair_cp(j).wait_send()
        swap_cp(j).wait_send()
        relay_cp(j).wait_send()
        direct_cp(j).wait_send()
        last_cp(j).wait_send()

    loop(NC, drain)
    for j in range(NC):
        for st in plans[j]:
            for cp in st['own']:
                cp.wait_send()
            st['relay'].wait_send()
        for cp in plans[j][1]['pair']:
            cp.wait_send()


def tail(blk, hidden, gains, rowmask, gates, xvalid, k_cross, v_cross, wo, wg, wu, wd, cq, cwo, cg, cu, cd, heads, hd):
    batch, dim = hidden.shape
    mlp = wg.shape[1]
    ntok = xvalid.shape[1]
    cw = dim // NC
    hw = heads * hd
    bl = batch // 4
    half = bl // 2
    f32, bf16 = jnp.float32, jnp.bfloat16
    anyspec = pl.BlockSpec(memory_space=pl.ANY)
    vmem = pl.BlockSpec(memory_space=pltpu.VMEM)
    smem = pl.BlockSpec(memory_space=pltpu.SMEM)
    dma = pltpu.SemaphoreType.DMA
    scratch = [
        pltpu.VMEM((4, 2, half, hw + hd), f32),
        pltpu.VMEM((2, half, hw + hd), f32),
        pltpu.VMEM((2, half, hw + hd), f32),
        pltpu.VMEM((2, half, hw + hd), f32),
        pltpu.VMEM((2, half, hw + hd), f32),
        pltpu.VMEM((bl, hw), bf16),
        pltpu.VMEM((4, 8, dim), bf16),
        pltpu.VMEM((NC, 4, 8, cw), f32),
        pltpu.VMEM((NC, hw, cw), bf16),
        pltpu.VMEM((NC, cw, mlp), bf16),
        pltpu.VMEM((NC, cw, mlp), bf16),
        pltpu.VMEM((NC, mlp, cw), bf16),
        pltpu.VMEM((NC, cw, hw), bf16),
        pltpu.VMEM((NC, hw, cw), bf16),
        pltpu.VMEM((bl, ntok, hd), bf16),
        pltpu.VMEM((bl, ntok, hd), bf16),
        pltpu.VMEM((bl, ntok), jnp.int32),
        pltpu.VMEM((NC, 2, half, cw), f32),
        pltpu.VMEM((NC, half, cw), f32),
        pltpu.VMEM((NC, 4, 8, cw), f32),
        pltpu.VMEM((NC, 4, 8, cw), f32),
        pltpu.VMEM((2, NC, 4, 8, cw), f32),
        pltpu.VMEM((2, NC, 4, 8, cw), f32),
        pltpu.VMEM((NC, 2, half, cw), f32),
        pltpu.VMEM((NC, 2, 4, 4, 8, cw), f32),
        pltpu.VMEM((bl, 2 * mlp), f32),
        pltpu.VMEM((bl, mlp), bf16),
        pltpu.VMEM((bl, 8, hd), f32),
        pltpu.VMEM((bl, 8, hd), f32),
        pltpu.VMEM((2, 4, 8, 128), f32),
        dma((3,)),
        dma((9, NC)),
        dma((2, 8)),
        dma((3, 2)),
        dma((3, 2)),
        dma((NC,)),
        dma((NC,)),
        dma((2, NC)),
        dma((2, 2, NC)),
        dma((3, NC)),
        dma((3, NC)),
        dma((NC,)),
        dma((NC,)),
        dma((NC, 3, 4)),
        dma((NC, 3, 4)),
    ]
    out = pl.pallas_call(
        functools.partial(tail_kernel, (heads, hd, dim, mlp, ntok)),
        out_shape=jax.ShapeDtypeStruct((batch // 8, 8, dim), bf16),
        in_specs=[anyspec, anyspec] + [vmem] * 5 + [smem] + [anyspec] * 12,
        out_specs=vmem,
        scratch_shapes=scratch,
        compiler_params=pltpu.CompilerParams(collective_id=0, has_side_effects=True, vmem_limit_bytes=67043328),
        name='tail',
    )(blk.reshape(4, 2, half, hw + hd), hidden.reshape(8, 4, 8, dim),
      *[g.reshape(-1, 128) for g in gains], rowmask.reshape(1, batch), gates,
      xvalid.reshape(4, bl, ntok), k_cross.reshape(4, bl, ntok, hd), v_cross.reshape(4, bl, ntok, hd),
      wo, wg, wu, wd, cq, cwo, cg, cu, cd)
    return out.reshape(batch, dim)


def solution(mesh):
    cache_spec = P('dp', 'sp', 'tp', None)
    cross_spec = P('dp', None, 'tp', None)
    row_spec = P('dp', None)
    vec_spec = P('dp')
    full_spec = P(None)
    col_spec = P(None, 'tp')
    split_rows = P('tp', None)
    in_specs = (row_spec, vec_spec, cache_spec, cache_spec, cross_spec, cross_spec, row_spec, vec_spec,
                full_spec, col_spec, col_spec, col_spec, split_rows, full_spec, col_spec, col_spec, split_rows,
                full_spec, col_spec, full_spec, split_rows, full_spec, full_spec, col_spec, col_spec, split_rows)
    out_specs = (row_spec, cache_spec, cache_spec)

    def local_step(hidden, new_pos, k_self, v_self, k_cross, v_cross, xvalid, rowmask,
                   self_attn_norm, self_wq, self_wk, self_wv, self_wo, self_mlp_norm,
                   self_wgate, self_wup, self_wdown, cross_attn_norm, cross_wq, cross_qnorm,
                   cross_wo, cross_gates, cross_mlp_norm, cross_wgate, cross_wup, cross_wdown):
        head_dim = k_self.shape[3]
        heads_local = self_wq.shape[1] // head_dim
        k_new_cache, v_new_cache, blk = front(hidden, new_pos, k_self, v_self, self_attn_norm, self_wq, self_wk, self_wv,
                                              heads_local, head_dim)
        gains = (self_mlp_norm, cross_attn_norm, cross_mlp_norm, cross_qnorm)
        h4 = tail(blk, hidden, gains, rowmask, cross_gates, xvalid, k_cross, v_cross, self_wo, self_wgate, self_wup, self_wdown,
                  cross_wq, cross_wo, cross_wgate, cross_wup, cross_wdown, heads_local, head_dim)
        return h4, k_new_cache, v_new_cache

    return jax.shard_map(local_step, mesh=mesh, in_specs=in_specs, out_specs=out_specs, check_vma=False)
```

```python
import functools
import math
import jax
import jax.numpy as jnp
import numpy as np
from jax import lax
from jax.experimental import pallas as pl
from jax.experimental.pallas import tpu as pltpu
from jax.sharding import PartitionSpec as P

NORM_EPS = 1e-5
ROPE_THETA = 500000.0
ROPE_FACTOR = 8.0
LOW_FREQ = 1.0
HIGH_FREQ = 4.0
ORIG_CTX = 8192.0
NEG_BIG = -1e30
NC = 6
MESH = pl.DeviceIdType.MESH


def rope_freqs(head_dim):
    inv_freq = (1.0 / (ROPE_THETA ** (np.arange(0, head_dim, 2).astype(np.float32) / np.float32(head_dim)))).astype(np.float32)
    wavelen = 2.0 * math.pi / inv_freq
    smooth = (ORIG_CTX / wavelen - LOW_FREQ) / (HIGH_FREQ - LOW_FREQ)
    mid_freq = (1.0 - smooth) * inv_freq / ROPE_FACTOR + smooth * inv_freq
    scaled = np.where(wavelen > ORIG_CTX / LOW_FREQ, inv_freq / ROPE_FACTOR, mid_freq)
    half = np.where(wavelen < ORIG_CTX / HIGH_FREQ, inv_freq, scaled).astype(np.float32)
    return np.concatenate([half, half])[None, :]


def fdot(a, b):
    return jnp.dot(a, b, preferred_element_type=jnp.float32)


def front_kernel(cfg, hid_h, posr_v, pos_s, gain_v, freq_v, wq_h, wk_h, wv_h, k_h, v_h, ko_h, vo_h, blk_v,
                 hid_v, xn, wq_v, wkv_v, kc, vc, q3, o3, st3, kn, vn, in_sem, kv_sem, out_sem):
    heads, hd, dim, batch, slots = cfg
    f32, bf16 = jnp.float32, jnp.bfloat16
    per = 64
    nch = batch // per
    nrm = 32
    scale = hd ** -0.5
    first_slot = lax.axis_index('sp') * slots

    def loop(n, body):
        def step(i, carry):
            body(i)
            return carry
        lax.fori_loop(0, n, step, 0)

    def ld_hid(r):
        span = pl.ds(pl.multiple_of(r * nrm, nrm), nrm)
        return pltpu.make_async_copy(hid_h.at[span], hid_v.at[span], in_sem.at[3 + r])

    weights = [pltpu.make_async_copy(h, v, in_sem.at[i])
               for i, (h, v) in enumerate(((wq_h, wq_v), (wk_h, wkv_v.at[:, :hd]), (wv_h, wkv_v.at[:, hd:])))]

    def ld_kv(g):
        span = pl.ds(g * per, per)
        return (pltpu.make_async_copy(k_h.at[span], kc.at[span], kv_sem.at[0, g]),
                pltpu.make_async_copy(v_h.at[span], vc.at[span], kv_sem.at[1, g]))

    def st_kv(g):
        span = pl.ds(g * per, per)
        return (pltpu.make_async_copy(kc.at[span], ko_h.at[span], out_sem.at[0, g]),
                pltpu.make_async_copy(vc.at[span], vo_h.at[span], out_sem.at[1, g]))

    def start_both(pair):
        pair[0].start()
        pair[1].start()

    def wait_both(pair):
        pair[0].wait()
        pair[1].wait()

    loop(batch // nrm, lambda r: ld_hid(r).start())
    for cp in weights:
        cp.start()
    loop(nch, lambda g: start_both(ld_kv(g)))
    q3[...] = jnp.zeros_like(q3)

    gain = gain_v[...].astype(f32)

    def norm(r):
        ld_hid(r).wait()
        span = pl.ds(pl.multiple_of(r * nrm, nrm), nrm)
        xs = hid_v[span, :].astype(f32)
        inv = lax.rsqrt(jnp.sum(xs * xs, axis=1, keepdims=True) / dim + NORM_EPS)
        for k in range(dim // 128):
            xn[span, k * 128:(k + 1) * 128] = (xs[:, k * 128:(k + 1) * 128] * inv * gain[k:k + 1]).astype(bf16)

    loop(batch // nrm, norm)
    eye = lax.broadcasted_iota(jnp.int32, (batch, batch), 0) == lax.broadcasted_iota(jnp.int32, (batch, batch), 1)
    posc = jnp.sum(jnp.where(eye, jnp.broadcast_to(posr_v[...], (batch, batch)).astype(f32), 0.0), axis=1, keepdims=True)
    angles = posc * freq_v[...]
    cos_t = jnp.cos(angles)
    low = lax.broadcasted_iota(jnp.int32, (batch, hd), 1) < hd // 2
    sin_t = jnp.where(low, -jnp.sin(angles), jnp.sin(angles))

    def rope(v):
        r = v.astype(bf16).astype(f32)
        return (r * cos_t + pltpu.roll(r, hd // 2, 1) * sin_t).astype(bf16).astype(f32)

    for cp in weights:
        cp.wait()
    q = fdot(xn[...], wq_v[...])
    for h in range(heads):
        q3[:, h, :] = rope(q[:, h * hd:(h + 1) * hd])
    kv = fdot(xn[...], wkv_v[...])
    kn[...] = rope(kv[:, :hd])
    vn[...] = kv[:, hd:].astype(bf16).astype(f32)

    lane = lax.broadcasted_iota(jnp.int32, (8, 128), 1)
    sub = lax.broadcasted_iota(jnp.int32, (8, 128), 0)
    row16 = lax.broadcasted_iota(jnp.int32, (16, hd), 0)
    zero = jnp.zeros((8, 128), f32)

    def attend(g):
        wait_both(ld_kv(g))
        lps = []
        for i in range(per):
            b = g * per + i
            lp = pos_s[b] - first_slot
            lps.append(lp)
            base = pl.multiple_of(lax.shift_left(lax.shift_right_logical(jnp.clip(lp, 0, slots - 1), 4), 4), 16)
            hit = row16 + base == lp
            for ref, new in ((kc, kn), (vc, vn)):
                old = ref[b, pl.ds(base, 16), :].astype(f32)
                fresh = jnp.broadcast_to(new[pl.ds(b, 1), :], (16, hd))
                ref[b, pl.ds(base, 16), :] = jnp.where(hit, fresh, old).astype(bf16)
        start_both(st_kv(g))
        fours = [pl.ds(g * per + 4 * t, 4) for t in range(per // 4)]

        def scores(ts):
            return [lax.dot_general(q3[fours[t]].reshape(32, hd).astype(bf16), kc[fours[t]].reshape(4 * slots, hd),
                                    (((1,), (1,)), ((), ())), preferred_element_type=f32) * scale for t in ts]

        def soften(ts, sgs):
            out = []
            for t, sg in zip(ts, sgs):
                probs, stats = [], []
                for i in range(4):
                    off = slots * (i % 2)
                    lp = jnp.minimum(lps[4 * t + i], slots - 1)
                    seen = (lane >= off) & (lane <= off + lp)
                    sc = jnp.where(seen, sg[8 * i:8 * i + 8, 128 * (i // 2):128 * (i // 2) + 128], NEG_BIG)
                    mx = jnp.max(sc, axis=1, keepdims=True)
                    pr = jnp.where(seen, jnp.exp(sc - mx), 0.0)
                    ls = jnp.sum(pr, axis=1, keepdims=True)
                    stats.append(jnp.where(lane == sub, mx, jnp.where(lane == sub + 8, ls, 0.0)))
                    probs.append(jnp.concatenate([pr, zero] if i < 2 else [zero, pr], axis=1))
                out.append((jnp.concatenate(probs, axis=0).astype(bf16), stats))
            return out

        def mix(ts, prs):
            return [fdot(pg, vc[fours[t]].reshape(4 * slots, hd)) for t, (pg, _) in zip(ts, prs)]

        sets = [range(t, t + 4) for t in range(0, per // 4, 4)]
        raw, soft, mixed = [scores(sets[0])], [], []
        for k, ts in enumerate(sets):
            if k + 1 < len(sets):
                raw.append(scores(sets[k + 1]))
            soft.append(soften(ts, raw[k]))
            mixed += mix(ts, soft[k])
        flat = [st for sf in soft for _, st in sf]
        for t, (o, stats) in enumerate(zip(mixed, flat)):
            o3[fours[t]] = o.reshape(4, 8, hd)
            for i in range(4):
                st3[g * per + 4 * t + i] = stats[i]

    loop(nch, attend)
    stat = st3[:, 0, :]
    for h in range(1, heads):
        stat = stat + st3[:, h, :]
    for h in range(heads):
        blk_v[:, h * hd:(h + 1) * hd] = o3[:, h, :]
    blk_v[:, heads * hd:] = stat
    loop(nch, lambda g: wait_both(st_kv(g)))


def front(hidden, new_pos, k_self, v_self, gain, wq, wk, wv, heads, hd):
    batch, dim = hidden.shape
    slots = k_self.shape[1]
    f32, bf16 = jnp.float32, jnp.bfloat16
    anyspec = pl.BlockSpec(memory_space=pl.ANY)
    vmem = pl.BlockSpec(memory_space=pltpu.VMEM)
    smem = pl.BlockSpec(memory_space=pltpu.SMEM)
    dma = pltpu.SemaphoreType.DMA
    nch = batch // 64
    cache = jax.ShapeDtypeStruct((batch, slots, hd), bf16)
    ko, vo, blk = pl.pallas_call(
        functools.partial(front_kernel, (heads, hd, dim, batch, slots)),
        out_shape=(cache, cache, jax.ShapeDtypeStruct((batch, heads * hd + hd), f32)),
        in_specs=[anyspec, vmem, smem, vmem, vmem] + [anyspec] * 5,
        out_specs=(anyspec, anyspec, vmem),
        scratch_shapes=[
            pltpu.VMEM((batch, dim), bf16),
            pltpu.VMEM((batch, dim), bf16),
            pltpu.VMEM(wq.shape, bf16),
            pltpu.VMEM((dim, 2 * hd), bf16),
            pltpu.VMEM((batch, slots, hd), bf16),
            pltpu.VMEM((batch, slots, hd), bf16),
            pltpu.VMEM((batch, 8, hd), f32),
            pltpu.VMEM((batch, 8, hd), f32),
            pltpu.VMEM((batch, 8, hd), f32),
            pltpu.VMEM((batch, hd), f32),
            pltpu.VMEM((batch, hd), f32),
            dma((3 + batch // 32,)),
            dma((2, nch)),
            dma((2, nch)),
        ],
        compiler_params=pltpu.CompilerParams(vmem_limit_bytes=60000000),
        name='front',
    )(hidden, new_pos.reshape(1, batch), new_pos, gain.reshape(dim // 128, 128), jnp.asarray(rope_freqs(hd)),
      wq, wk, wv, k_self.reshape(batch, slots, hd), v_self.reshape(batch, slots, hd))
    return ko.reshape(k_self.shape), vo.reshape(v_self.shape), blk


def tail_kernel(cfg, blk_h, hid_h, g2_v, g3_v, g4_v, qn_v, rowm_v, gate_s, xv_h, kc_h, vc_h,
                wo_h, wg_h, wu_h, wd_h, cq_h, cwo_h, cg_h, cu_h, cd_h, out_h,
                bk, yr, yd, yt, yf, ob, hrow, hst,
                wo_v, wg_v, wu_v, wd_v, cq_v, cwo_v, kc_v, vc_v, xv_v,
                pbuf, dbuf, s0, s1, r1, r2, xa, og, acc, act, q3, oc, fac,
                ld_sem, w_sem, kv_sem, ys, yrs, pr_s, pr_r, ar_s, ar_r, lr_s, lr_r, xs_s, xs_r, fg_s, fg_r, out_sem):
    heads, hd, dim, mlp, ntok = cfg
    cw = dim // NC
    hw = heads * hd
    half = 32
    x = lax.axis_index('tp') // 2
    c = lax.axis_index('tp') % 2
    y = lax.axis_index('sp')
    flip = x + 1 - 2 * lax.rem(x, 2)
    cross = 3 - x
    scale = hd ** -0.5

    def ring(v):
        return lax.rem(v + 8, 4)

    def xdev(d):
        return {'tp': 2 * ring(x + d) + c}

    def ydev(d):
        return {'sp': ring(y + d)}

    sib = {'tp': 2 * x + 1 - c}

    def rcopy(src, dst, ss, rs, dev):
        return pltpu.make_async_remote_copy(src_ref=src, dst_ref=dst, send_sem=ss, recv_sem=rs,
                                            device_id=dev, device_id_type=MESH)

    def loop(n, body):
        def step(i, carry):
            body(i)
            return carry
        lax.fori_loop(0, n, step, 0)

    blk_cp = pltpu.make_async_copy(blk_h, bk, ld_sem.at[0])
    hid_cp = pltpu.make_async_copy(hid_h.at[y * 2 + c], hrow, ld_sem.at[1])
    xv_cp = pltpu.make_async_copy(xv_h.at[y], xv_v, ld_sem.at[2])

    def cols(h, v, k, j):
        return pltpu.make_async_copy(h.at[:, pl.ds(pl.multiple_of(j * cw, 128), cw)], v.at[j], w_sem.at[k, j])

    def rows(h, v, k, j):
        return pltpu.make_async_copy(h.at[pl.ds(pl.multiple_of(j * cw, 128), cw)], v.at[j], w_sem.at[k, j])

    def ld_wo(j):
        return cols(wo_h, wo_v, 0, j)

    def ld_wg(j):
        return rows(wg_h, wg_v, 1, j)

    def ld_wu(j):
        return rows(wu_h, wu_v, 2, j)

    def ld_wd(j):
        return cols(wd_h, wd_v, 3, j)

    def ld_cq(j):
        return rows(cq_h, cq_v, 4, j)

    def ld_cwo(j):
        return cols(cwo_h, cwo_v, 5, j)

    def ld_cg(j):
        return rows(cg_h, wg_v, 6, j)

    def ld_cu(j):
        return rows(cu_h, wu_v, 7, j)

    def ld_cd(j):
        return cols(cd_h, wd_v, 8, j)

    def ld_kc(g):
        return pltpu.make_async_copy(kc_h.at[y, pl.ds(g * 8, 8)], kc_v.at[pl.ds(g * 8, 8)], kv_sem.at[0, g])

    def ld_vc(g):
        return pltpu.make_async_copy(vc_h.at[y, pl.ds(g * 8, 8)], vc_v.at[pl.ds(g * 8, 8)], kv_sem.at[1, g])

    blk_cp.start()
    hid_cp.start()
    xv_cp.start()
    loop(NC, lambda j: ld_wo(j).start())

    barrier = pltpu.get_barrier_semaphore()
    for dev in (sib, xdev(1), xdev(2), xdev(-1), ydev(1), ydev(2), ydev(-1)):
        pl.semaphore_signal(barrier, inc=1, device_id=dev, device_id_type=MESH)

    def start_gu(j):
        ld_wg(j).start()
        ld_wu(j).start()

    loop(NC, start_gu)
    loop(NC, lambda j: ld_wd(j).start())
    loop(NC, lambda j: ld_cq(j).start())

    def start_kv(g):
        ld_kc(g).start()
        ld_vc(g).start()

    loop(8, start_kv)
    loop(NC, lambda j: ld_cwo(j).start())
    q3[...] = jnp.zeros_like(q3)
    nrow = rowm_v.shape[1]
    mine = (y * 2 + c) * half + lax.broadcasted_iota(jnp.int32, (half, nrow), 0)
    pick = lax.broadcasted_iota(jnp.int32, (half, nrow), 1) == mine
    rmask = jnp.sum(jnp.where(pick, jnp.broadcast_to(rowm_v[...], (half, nrow)), 0).astype(jnp.float32), axis=1, keepdims=True)
    for k in range(2):
        fac[k] = (jnp.tanh(jnp.full((half, 128), gate_s[k], jnp.float32)) * rmask).reshape(4, 8, 128)
    pl.semaphore_wait(barrier, 7)

    lane = lax.broadcasted_iota(jnp.int32, (half, hd), 1)

    def merge(a, b):
        outs, ms, ls = [], [], []
        for h in range(heads):
            ma, mb = a[:, hw + h:hw + h + 1], b[:, hw + h:hw + h + 1]
            la, lb = a[:, hw + 8 + h:hw + 9 + h], b[:, hw + 8 + h:hw + 9 + h]
            mm = jnp.maximum(ma, mb)
            ea, eb = jnp.exp(ma - mm), jnp.exp(mb - mm)
            outs.append(a[:, h * hd:(h + 1) * hd] * ea + b[:, h * hd:(h + 1) * hd] * eb)
            ms.append(mm)
            ls.append(la * ea + lb * eb)
        stat = jnp.zeros((half, hd), jnp.float32)
        for h in range(heads):
            stat = jnp.where(lane == h, ms[h], stat)
            stat = jnp.where(lane == 8 + h, ls[h], stat)
        return jnp.concatenate(outs + [stat], axis=1), ls

    def y_relay(j, d):
        return rcopy(bk.at[ring(y + 2), j], yr.at[j], ys.at[0, j], yrs.at[0, j], ydev(d))

    def y_direct(j, d):
        return rcopy(bk.at[ring(y - d), j], yd.at[j], ys.at[1, j], yrs.at[1, j], ydev(-d))

    def y_final(j, d):
        return rcopy(yt.at[j], yf.at[j], ys.at[2, j], yrs.at[2, j], ydev(d))

    blk_cp.wait()
    for j, d in ((0, 1), (1, -1)):
        y_relay(j, d).start()
    for j, d in ((0, 1), (1, -1)):
        y_direct(j, d).start()
    for j, d in ((0, 1), (1, -1)):
        y_relay(j, d).wait_recv()
        yt[j] = merge(bk[ring(y + d), j], yr[j])[0]
        y_final(j, d).start()
    for j, d in ((0, 1), (1, -1)):
        y_direct(j, d).wait_recv()
        first = merge(bk[y, j], yd[j])[0]
        y_final(j, d).wait_recv()
        both, sums = merge(first, yf[j])
        for h in range(heads):
            ob[j * half:(j + 1) * half, h * hd:(h + 1) * hd] = (both[:, h * hd:(h + 1) * hd] / sums[h]).astype(jnp.bfloat16)

    def pair_cp(j):
        return rcopy(pbuf.at[j, 1 - c], dbuf.at[j], pr_s.at[j], pr_r.at[j], sib)

    def mate(j, second):
        odd = lax.rem(j + second, 2)
        return {'tp': 2 * (flip + odd * (cross - flip)) + c}

    def one_cp(p, j):
        return rcopy(s0.at[j], r1.at[p % 2, j], ar_s.at[0, j], ar_r.at[p % 2, 0, j], mate(j, 0))

    def two_cp(p, j):
        return rcopy(s1.at[j], r2.at[p % 2, j], ar_s.at[1, j], ar_r.at[p % 2, 1, j], mate(j, 1))

    def pair_sums(p, partial, after):
        def body(j):
            @pl.when(j < NC)
            def _():
                if p > 0:
                    pair_cp(j).wait_send()
                pbuf[j] = partial(j).reshape(2, half, cw)
                pair_cp(j).start()

            @pl.when(j >= 1)
            def _():
                pair_cp(j - 1).wait_recv()
                if p > 0:
                    one_cp(p, j - 1).wait_send()
                s0[j - 1] = (pbuf[j - 1, c] + dbuf[j - 1]).reshape(4, 8, cw)
                after(j - 1)

        loop(NC + 1, body)

    def all_reduce(p, partial):
        pair_sums(p, partial, lambda j: one_cp(p, j).start())

        def step(j):
            one_cp(p, j).wait_recv()
            if p > 0:
                two_cp(p, j).wait_send()
            s1[j] = s0[j] + r1[p % 2, j]
            two_cp(p, j).start()

        loop(NC, step)

    def new_rows(p, k):
        sq = jnp.zeros((4, 8, 1), jnp.float32)
        for j in range(NC):
            two_cp(p, j).wait_recv()
            add = s1[j] + r2[p % 2, j]
            if k is not None:
                add = fac[k][:, :, :1] * add
            old = hrow[:, :, j * cw:(j + 1) * cw].astype(jnp.float32) if p == 0 else hst[j]
            new = (old + add).astype(jnp.bfloat16).astype(jnp.float32)
            hst[j] = new
            sq = sq + jnp.sum(new * new, axis=2, keepdims=True)
        return sq

    def swap_cp(j):
        return rcopy(xa.at[j, c], xa.at[j, c], xs_s.at[j], xs_r.at[j], sib)

    def all_gather(q, sq, gain_row, consume):
        inv = lax.rsqrt(sq / dim + NORM_EPS)
        rows_of = (g2_v, g3_v, g4_v)[gain_row][...].astype(jnp.float32)
        for j in range(NC):
            gain = jnp.concatenate([rows_of[i:i + 1] for i in range(j * cw // 128, (j + 1) * cw // 128)], axis=1)
            if q > 0:
                swap_cp(j).wait_send()
            xa[j, c] = (hst[j] * inv * gain.reshape(1, 1, cw)).astype(jnp.bfloat16).astype(jnp.float32).reshape(half, cw)
            swap_cp(j).start()

        def body(t):
            swap_cp(2 * t).wait_recv()
            swap_cp(2 * t + 1).wait_recv()
            xs = [xa[2 * t + u].reshape(2 * half, cw).astype(jnp.bfloat16) for u in range(2)]
            consume(t, jnp.concatenate(xs, axis=1))

        loop(NC // 2, body)

    def turn(j):
        return 1 - 2 * lax.rem(j, 2)

    def relay_cp(j):
        return rcopy(s0.at[j, ring(x + 2)], r1.at[1, j, 0], lr_s.at[0, j], lr_r.at[0, j], xdev(turn(j)))

    def direct_cp(j):
        return rcopy(s0.at[j, ring(x - turn(j))], r1.at[1, j, 1], lr_s.at[1, j], lr_r.at[1, j], xdev(-turn(j)))

    def last_cp(j):
        return rcopy(s1.at[j, 0], r1.at[1, j, 2], lr_s.at[2, j], lr_r.at[2, j], xdev(turn(j)))

    def last_scatter(partial):
        def send(j):
            relay_cp(j).start()
            direct_cp(j).start()

        pair_sums(3, partial, send)

        def step(j):
            relay_cp(j).wait_recv()
            two_cp(2, j).wait_send()
            s1[j, 0] = s0[j, ring(x + turn(j))] + r1[1, j, 0]
            last_cp(j).start()

        loop(NC, step)

    def last_rows(j):
        direct_cp(j).wait_recv()
        last_cp(j).wait_recv()
        return s0[j, x] + r1[1, j, 1] + r1[1, j, 2]

    def mlp_hidden(q, sq, gain_row, wait_gu):
        acc[...] = jnp.zeros_like(acc)

        def consume(t, xs):
            wait_gu(2 * t)
            wait_gu(2 * t + 1)
            two = pl.ds(2 * t, 2)
            acc[:, :mlp] += fdot(xs, wg_v[two].reshape(2 * cw, mlp))
            acc[:, mlp:] += fdot(xs, wu_v[two].reshape(2 * cw, mlp))

        all_gather(q, sq, gain_row, consume)
        gv = acc[:, :mlp].astype(jnp.bfloat16).astype(jnp.float32)
        uv = acc[:, mlp:].astype(jnp.bfloat16).astype(jnp.float32)
        act[...] = (jax.nn.silu(gv) * uv).astype(jnp.bfloat16)

    def part_wo(j):
        ld_wo(j).wait()
        return fdot(ob[...], wo_v[j])

    all_reduce(0, part_wo)
    hid_cp.wait()
    sq = new_rows(0, None)

    def wait_self(j):
        ld_wg(j).wait()
        ld_wu(j).wait()

    mlp_hidden(0, sq, 0, wait_self)

    def start_cgu(j):
        ld_cg(j).start()
        ld_cu(j).start()

    loop(NC, start_cgu)

    def part_wd(j):
        ld_wd(j).wait()
        return fdot(act[...], wd_v[j])

    all_reduce(1, part_wd)
    loop(NC, lambda j: ld_cd(j).start())
    sq = new_rows(1, None)

    acc[:, :hw] = jnp.zeros((2 * half, hw), jnp.float32)

    def consume_q(t, xs):
        ld_cq(2 * t).wait()
        ld_cq(2 * t + 1).wait()
        acc[:, :hw] += fdot(xs, cq_v[pl.ds(2 * t, 2)].reshape(2 * cw, hw))

    all_gather(1, sq, 1, consume_q)
    qgain = qn_v[...].astype(jnp.float32)
    for h in range(heads):
        qh = acc[:, h * hd:(h + 1) * hd].astype(jnp.bfloat16).astype(jnp.float32)
        qinv = lax.rsqrt(jnp.mean(qh * qh, axis=1, keepdims=True) + NORM_EPS)
        q3[:, h, :] = (qh * qinv * qgain).astype(jnp.bfloat16).astype(jnp.float32)
    xv_cp.wait()

    nat = 16

    def attend(t):
        for u in range(nat // 8):
            ld_kc(t * (nat // 8) + u).wait()
            ld_vc(t * (nat // 8) + u).wait()

        def scores(us):
            return [lax.dot_general(q3[t * nat + u].astype(jnp.bfloat16), kc_v[t * nat + u], (((1,), (1,)), ((), ())),
                                    preferred_element_type=jnp.float32) * scale for u in us]

        def soften(us, scs):
            out = []
            for u, sc in zip(us, scs):
                valid = jnp.broadcast_to(xvs[u // 8][u % 8:u % 8 + 1], (8, ntok)) > 0
                sc = jnp.where(valid, sc, NEG_BIG)
                mx = jnp.max(sc, axis=1, keepdims=True)
                pr = jnp.where(valid, jnp.exp(sc - mx), 0.0)
                out.append((pr.astype(jnp.bfloat16), jnp.sum(pr, axis=1, keepdims=True)))
            return out

        def mix(us, prs):
            return [fdot(pr, vc_v[t * nat + u]) / ls for u, (pr, ls) in zip(us, prs)]

        xvs = [xv_v[pl.ds(pl.multiple_of(t * nat + 8 * u, 8), 8), :] for u in range(nat // 8)]
        one, two = range(nat // 2), range(nat // 2, nat)
        sa = scores(one)
        sb = scores(two)
        oa = mix(one, soften(one, sa))
        o2 = mix(two, soften(two, sb))
        for u, o in enumerate(oa + o2):
            oc[t * nat + u] = o

    loop(2 * half // nat, attend)
    for h in range(heads):
        ob[:, h * hd:(h + 1) * hd] = oc[:, h, :].astype(jnp.bfloat16)

    def part_cwo(j):
        ld_cwo(j).wait()
        return fdot(ob[...], cwo_v[j])

    all_reduce(2, part_cwo)
    sq = new_rows(2, 0)

    def wait_cross(j):
        ld_cg(j).wait()
        ld_cu(j).wait()

    mlp_hidden(2, sq, 2, wait_cross)

    def part_cd(j):
        ld_cd(j).wait()
        return fdot(act[...], wd_v[j])

    last_scatter(part_cd)

    def parts_of(j):
        if j < NC // 2:
            return (lambda k: og.at[j, c, y, ring(x + k)], xdev), (lambda k: og.at[j, c, ring(y + k)], ydev)
        return (lambda k: og.at[j, c, ring(y + k), x], ydev), (lambda k: og.at[j, c, :, ring(x + k)], xdev)

    def fg(j, stage, k, s, what, dev):
        return rcopy(what, what, fg_s.at[j, stage, s], fg_r.at[j, stage, k], dev)

    plans = []
    for j in range(NC):
        d = 1 - 2 * (j % 2)
        stages = []
        for stage, (region, dev) in enumerate(parts_of(j)):
            own = [fg(j, stage, 0, 0, region(0), dev(d)), fg(j, stage, 1, 1, region(0), dev(-d))]
            if stage == 0:
                own.append(fg(j, stage, 2, 2, region(0), dev(2)))
            stages.append(dict(
                own=own,
                relay=[fg(j, stage, 2, 2, region(-d), dev(d))] if stage else [],
                got=[fg(j, stage, 0, 0, region(-d), sib), fg(j, stage, 1, 1, region(d), sib), fg(j, stage, 2, 2, region(2), sib)],
                pair=[fg(j, 2, i, i, region(k), sib) for i, k in enumerate((0, -d, d, 2))] if stage else [],
            ))
        plans.append(stages)
    order = range(NC)
    for j in order:
        og[j, c, y, x] = (hst[j, x] + fac[1, x][:, :1] * last_rows(j)).astype(jnp.bfloat16).astype(jnp.float32)
        for cp in plans[j][0]['own']:
            cp.start()
    for j in order:
        st, nx = plans[j]
        for cp in st['got']:
            cp.wait_recv()
        for cp in nx['own']:
            cp.start()
        nx['pair'][0].start()
    for j in order:
        st = plans[j][1]
        st['got'][0].wait_recv()
        st['relay'][0].start()
        st['pair'][1].start()
        st['got'][1].wait_recv()
        st['pair'][2].start()

    def result_cp(j, cc):
        return pltpu.make_async_copy(og.at[j, cc], out_h.at[:, cc, :, :, j * cw:(j + 1) * cw], out_sem.at[cc, j])

    for j in order:
        st = plans[j][1]
        st['got'][2].wait_recv()
        st['pair'][3].start()
        result_cp(j, c).start()
    for j in order:
        for cp in plans[j][1]['pair']:
            cp.wait_recv()
        result_cp(j, 1 - c).start()

    for j, d in ((0, 1), (1, -1)):
        y_relay(j, d).wait_send()
        y_direct(j, d).wait_send()
        y_final(j, d).wait_send()

    def drain(j):
        pair_cp(j).wait_send()
        swap_cp(j).wait_send()
        relay_cp(j).wait_send()
        direct_cp(j).wait_send()
        last_cp(j).wait_send()

    loop(NC, drain)
    for j in range(NC):
        for st in plans[j]:
            for cp in st['own'] + st['relay'] + st['pair']:
                cp.wait_send()
    for j in order:
        result_cp(j, 0).wait()
        result_cp(j, 1).wait()


def tail(blk, hidden, gains, rowmask, gates, xvalid, k_cross, v_cross, wo, wg, wu, wd, cq, cwo, cg, cu, cd, heads, hd):
    batch, dim = hidden.shape
    mlp = wg.shape[1]
    ntok = xvalid.shape[1]
    cw = dim // NC
    hw = heads * hd
    bl = batch // 4
    half = bl // 2
    f32, bf16 = jnp.float32, jnp.bfloat16
    anyspec = pl.BlockSpec(memory_space=pl.ANY)
    vmem = pl.BlockSpec(memory_space=pltpu.VMEM)
    smem = pl.BlockSpec(memory_space=pltpu.SMEM)
    dma = pltpu.SemaphoreType.DMA
    scratch = [
        pltpu.VMEM((4, 2, half, hw + hd), f32),
        pltpu.VMEM((2, half, hw + hd), f32),
        pltpu.VMEM((2, half, hw + hd), f32),
        pltpu.VMEM((2, half, hw + hd), f32),
        pltpu.VMEM((2, half, hw + hd), f32),
        pltpu.VMEM((bl, hw), bf16),
        pltpu.VMEM((4, 8, dim), bf16),
        pltpu.VMEM((NC, 4, 8, cw), f32),
        pltpu.VMEM((NC, hw, cw), bf16),
        pltpu.VMEM((NC, cw, mlp), bf16),
        pltpu.VMEM((NC, cw, mlp), bf16),
        pltpu.VMEM((NC, mlp, cw), bf16),
        pltpu.VMEM((NC, cw, hw), bf16),
        pltpu.VMEM((NC, hw, cw), bf16),
        pltpu.VMEM((bl, ntok, hd), bf16),
        pltpu.VMEM((bl, ntok, hd), bf16),
        pltpu.VMEM((bl, ntok), jnp.int32),
        pltpu.VMEM((NC, 2, half, cw), f32),
        pltpu.VMEM((NC, half, cw), f32),
        pltpu.VMEM((NC, 4, 8, cw), f32),
        pltpu.VMEM((NC, 4, 8, cw), f32),
        pltpu.VMEM((2, NC, 4, 8, cw), f32),
        pltpu.VMEM((2, NC, 4, 8, cw), f32),
        pltpu.VMEM((NC, 2, half, cw), f32),
        pltpu.VMEM((NC, 2, 4, 4, 8, cw), f32),
        pltpu.VMEM((bl, 2 * mlp), f32),
        pltpu.VMEM((bl, mlp), bf16),
        pltpu.VMEM((bl, 8, hd), f32),
        pltpu.VMEM((bl, 8, hd), f32),
        pltpu.VMEM((2, 4, 8, 128), f32),
        dma((3,)),
        dma((9, NC)),
        dma((2, 8)),
        dma((3, 2)),
        dma((3, 2)),
        dma((NC,)),
        dma((NC,)),
        dma((2, NC)),
        dma((2, 2, NC)),
        dma((3, NC)),
        dma((3, NC)),
        dma((NC,)),
        dma((NC,)),
        dma((NC, 3, 4)),
        dma((NC, 3, 4)),
        dma((2, NC)),
    ]
    out = pl.pallas_call(
        functools.partial(tail_kernel, (heads, hd, dim, mlp, ntok)),
        out_shape=jax.ShapeDtypeStruct((4, 2, 4, 8, dim), f32),
        in_specs=[anyspec, anyspec] + [vmem] * 5 + [smem] + [anyspec] * 12,
        out_specs=anyspec,
        scratch_shapes=scratch,
        compiler_params=pltpu.CompilerParams(collective_id=0, has_side_effects=True, vmem_limit_bytes=67043328),
        name='tail',
    )(blk.reshape(4, 2, half, hw + hd), hidden.reshape(8, 4, 8, dim),
      *[g.reshape(-1, 128) for g in gains], rowmask.reshape(1, batch), gates,
      xvalid.reshape(4, bl, ntok), k_cross.reshape(4, bl, ntok, hd), v_cross.reshape(4, bl, ntok, hd),
      wo, wg, wu, wd, cq, cwo, cg, cu, cd)
    return out.reshape(batch, dim).astype(bf16)


def solution(mesh):
    cache_spec = P('dp', 'sp', 'tp', None)
    cross_spec = P('dp', None, 'tp', None)
    row_spec = P('dp', None)
    vec_spec = P('dp')
    full_spec = P(None)
    col_spec = P(None, 'tp')
    split_rows = P('tp', None)
    in_specs = (row_spec, vec_spec, cache_spec, cache_spec, cross_spec, cross_spec, row_spec, vec_spec,
                full_spec, col_spec, col_spec, col_spec, split_rows, full_spec, col_spec, col_spec, split_rows,
                full_spec, col_spec, full_spec, split_rows, full_spec, full_spec, col_spec, col_spec, split_rows)
    out_specs = (row_spec, cache_spec, cache_spec)

    def local_step(hidden, new_pos, k_self, v_self, k_cross, v_cross, xvalid, rowmask,
                   self_attn_norm, self_wq, self_wk, self_wv, self_wo, self_mlp_norm,
                   self_wgate, self_wup, self_wdown, cross_attn_norm, cross_wq, cross_qnorm,
                   cross_wo, cross_gates, cross_mlp_norm, cross_wgate, cross_wup, cross_wdown):
        head_dim = k_self.shape[3]
        heads_local = self_wq.shape[1] // head_dim
        k_new_cache, v_new_cache, blk = front(hidden, new_pos, k_self, v_self, self_attn_norm, self_wq, self_wk, self_wv,
                                              heads_local, head_dim)
        gains = (self_mlp_norm, cross_attn_norm, cross_mlp_norm, cross_qnorm)
        h4 = tail(blk, hidden, gains, rowmask, cross_gates, xvalid, k_cross, v_cross, self_wo, self_wgate, self_wup, self_wdown,
                  cross_wq, cross_wo, cross_wgate, cross_wup, cross_wdown, heads_local, head_dim)
        return h4, k_new_cache, v_new_cache

    return jax.shard_map(local_step, mesh=mesh, in_specs=in_specs, out_specs=out_specs, check_vma=False)
```

```python
import functools
import math
import jax
import jax.numpy as jnp
import numpy as np
from jax import lax
from jax.experimental import pallas as pl
from jax.experimental.pallas import tpu as pltpu
from jax.sharding import PartitionSpec as P

NORM_EPS = 1e-5
ROPE_THETA = 500000.0
ROPE_FACTOR = 8.0
LOW_FREQ = 1.0
HIGH_FREQ = 4.0
ORIG_CTX = 8192.0
NEG_BIG = -1e30
NC = 6
MESH = pl.DeviceIdType.MESH


def rope_freqs(head_dim):
    inv_freq = (1.0 / (ROPE_THETA ** (np.arange(0, head_dim, 2).astype(np.float32) / np.float32(head_dim)))).astype(np.float32)
    wavelen = 2.0 * math.pi / inv_freq
    smooth = (ORIG_CTX / wavelen - LOW_FREQ) / (HIGH_FREQ - LOW_FREQ)
    mid_freq = (1.0 - smooth) * inv_freq / ROPE_FACTOR + smooth * inv_freq
    scaled = np.where(wavelen > ORIG_CTX / LOW_FREQ, inv_freq / ROPE_FACTOR, mid_freq)
    half = np.where(wavelen < ORIG_CTX / HIGH_FREQ, inv_freq, scaled).astype(np.float32)
    return np.concatenate([half, half])[None, :]


def fdot(a, b):
    return jnp.dot(a, b, preferred_element_type=jnp.float32)


def front_kernel(cfg, hid_h, posr_v, pos_s, gain_v, freq_v, wq_h, wk_h, wv_h, k_h, v_h, ko_h, vo_h, q_h,
                 hid_v, xn, wq_v, wkv_v, kc, vc, q3, kn, vn, in_sem, kv_sem, out_sem):
    heads, hd, dim, batch, slots = cfg
    f32, bf16 = jnp.float32, jnp.bfloat16
    per = 32
    nch = batch // per
    nrm = 32
    first_slot = lax.axis_index('sp') * slots

    def loop(n, body):
        def step(i, carry):
            body(i)
            return carry
        lax.fori_loop(0, n, step, 0)

    def ld_hid(r):
        span = pl.ds(pl.multiple_of(r * nrm, nrm), nrm)
        return pltpu.make_async_copy(hid_h.at[span], hid_v.at[span], in_sem.at[3 + r])

    weights = [pltpu.make_async_copy(h, v, in_sem.at[i])
               for i, (h, v) in enumerate(((wq_h, wq_v), (wk_h, wkv_v.at[:, :hd]), (wv_h, wkv_v.at[:, hd:])))]

    def ld_kv(g):
        span = pl.ds(g * per, per)
        return (pltpu.make_async_copy(k_h.at[span], kc.at[span], kv_sem.at[0, g]),
                pltpu.make_async_copy(v_h.at[span], vc.at[span], kv_sem.at[1, g]))

    def st_kv(g):
        span = pl.ds(g * per, per)
        return (pltpu.make_async_copy(kc.at[span], ko_h.at[span], out_sem.at[0, g]),
                pltpu.make_async_copy(vc.at[span], vo_h.at[span], out_sem.at[1, g]))

    def start_both(pair):
        pair[0].start()
        pair[1].start()

    def wait_both(pair):
        pair[0].wait()
        pair[1].wait()

    loop(batch // nrm, lambda r: ld_hid(r).start())
    for cp in weights:
        cp.start()
    loop(nch, lambda g: start_both(ld_kv(g)))
    q3[...] = jnp.zeros_like(q3)

    gain = gain_v[...].astype(f32)

    def norm(r):
        ld_hid(r).wait()
        span = pl.ds(pl.multiple_of(r * nrm, nrm), nrm)
        xs = hid_v[span, :].astype(f32)
        inv = lax.rsqrt(jnp.sum(xs * xs, axis=1, keepdims=True) / dim + NORM_EPS)
        for k in range(dim // 128):
            xn[span, k * 128:(k + 1) * 128] = (xs[:, k * 128:(k + 1) * 128] * inv * gain[k:k + 1]).astype(bf16)

    loop(batch // nrm, norm)
    eye = lax.broadcasted_iota(jnp.int32, (batch, batch), 0) == lax.broadcasted_iota(jnp.int32, (batch, batch), 1)
    posc = jnp.sum(jnp.where(eye, jnp.broadcast_to(posr_v[...], (batch, batch)).astype(f32), 0.0), axis=1, keepdims=True)
    angles = posc * freq_v[...]
    cos_t = jnp.cos(angles)
    low = lax.broadcasted_iota(jnp.int32, (batch, hd), 1) < hd // 2
    sin_t = jnp.where(low, -jnp.sin(angles), jnp.sin(angles))

    def rope(v):
        r = v.astype(bf16).astype(f32)
        return (r * cos_t + pltpu.roll(r, hd // 2, 1) * sin_t).astype(bf16).astype(f32)

    for cp in weights:
        cp.wait()
    q = fdot(xn[...], wq_v[...])
    for h in range(heads):
        q3[:, h, :] = rope(q[:, h * hd:(h + 1) * hd])
    kv = fdot(xn[...], wkv_v[...])
    kn[...] = rope(kv[:, :hd])
    vn[...] = kv[:, hd:].astype(bf16).astype(f32)
    q_cp = pltpu.make_async_copy(q3, q_h, in_sem.at[3 + batch // nrm])
    q_cp.start()
    row16 = lax.broadcasted_iota(jnp.int32, (16, hd), 0)

    def patch(g):
        wait_both(ld_kv(g))
        for i in range(per):
            b = g * per + i
            lp = pos_s[b] - first_slot
            base = pl.multiple_of(lax.shift_left(lax.shift_right_logical(jnp.clip(lp, 0, slots - 1), 4), 4), 16)
            hit = row16 + base == lp
            for ref, new in ((kc, kn), (vc, vn)):
                old = ref[b, pl.ds(base, 16), :].astype(f32)
                fresh = jnp.broadcast_to(new[pl.ds(b, 1), :], (16, hd))
                ref[b, pl.ds(base, 16), :] = jnp.where(hit, fresh, old).astype(bf16)
        start_both(st_kv(g))

    loop(nch, patch)
    q_cp.wait()
    loop(nch, lambda g: wait_both(st_kv(g)))


def front(hidden, new_pos, k_self, v_self, gain, wq, wk, wv, heads, hd):
    batch, dim = hidden.shape
    slots = k_self.shape[1]
    f32, bf16 = jnp.float32, jnp.bfloat16
    anyspec = pl.BlockSpec(memory_space=pl.ANY)
    vmem = pl.BlockSpec(memory_space=pltpu.VMEM)
    smem = pl.BlockSpec(memory_space=pltpu.SMEM)
    dma = pltpu.SemaphoreType.DMA
    nch = batch // 32
    cache = jax.ShapeDtypeStruct((batch, slots, hd), bf16)
    ko, vo, q = pl.pallas_call(
        functools.partial(front_kernel, (heads, hd, dim, batch, slots)),
        out_shape=(cache, cache, jax.ShapeDtypeStruct((batch, 8, hd), f32)),
        in_specs=[anyspec, vmem, smem, vmem, vmem] + [anyspec] * 5,
        out_specs=(anyspec, anyspec, anyspec),
        scratch_shapes=[
            pltpu.VMEM((batch, dim), bf16),
            pltpu.VMEM((batch, dim), bf16),
            pltpu.VMEM(wq.shape, bf16),
            pltpu.VMEM((dim, 2 * hd), bf16),
            pltpu.VMEM((batch, slots, hd), bf16),
            pltpu.VMEM((batch, slots, hd), bf16),
            pltpu.VMEM((batch, 8, hd), f32),
            pltpu.VMEM((batch, hd), f32),
            pltpu.VMEM((batch, hd), f32),
            dma((4 + batch // 32,)),
            dma((2, nch)),
            dma((2, nch)),
        ],
        compiler_params=pltpu.CompilerParams(vmem_limit_bytes=60000000),
        name='front',
    )(hidden, new_pos.reshape(1, batch), new_pos, gain.reshape(dim // 128, 128), jnp.asarray(rope_freqs(hd)),
      wq, wk, wv, k_self.reshape(batch, slots, hd), v_self.reshape(batch, slots, hd))
    return ko, vo, q


def tail_kernel(cfg, q_h, ks_h, vs_h, pos_s, hid_h, g2_v, g3_v, g4_v, qn_v, rowm_v, gate_s, xv_h, kc_h, vc_h,
                wo_h, wg_h, wu_h, wd_h, cq_h, cwo_h, cg_h, cu_h, cd_h, out_h,
                qs_v, o3, st3, bk, yr, yd, yt, yf, ob, hrow, hst,
                wo_v, wg_v, wu_v, wd_v, cq_v, cwo_v, kc_v, vc_v, xv_v,
                pbuf, dbuf, s0, s1, r1, r2, xa, og, acc, act, q3, oc, fac,
                ld_sem, self_sem, w_sem, kv_sem, ys, yrs, pr_s, pr_r, ar_s, ar_r, lr_s, lr_r, xs_s, xs_r, fg_s, fg_r, out_sem):
    heads, hd, dim, mlp, ntok, slots = cfg
    per = ntok // slots
    free = ks_h.shape[0] * ks_h.shape[1] // per // 8
    cw = dim // NC
    hw = heads * hd
    half = 32
    x = lax.axis_index('tp') // 2
    c = lax.axis_index('tp') % 2
    y = lax.axis_index('sp')
    flip = x + 1 - 2 * lax.rem(x, 2)
    cross = 3 - x
    scale = hd ** -0.5

    def ring(v):
        return lax.rem(v + 8, 4)

    def xdev(d):
        return {'tp': 2 * ring(x + d) + c}

    def ydev(d):
        return {'sp': ring(y + d)}

    sib = {'tp': 2 * x + 1 - c}

    def rcopy(src, dst, ss, rs, dev):
        return pltpu.make_async_remote_copy(src_ref=src, dst_ref=dst, send_sem=ss, recv_sem=rs,
                                            device_id=dev, device_id_type=MESH)

    def loop(n, body):
        def step(i, carry):
            body(i)
            return carry
        lax.fori_loop(0, n, step, 0)

    def ld_self(t):
        dest = ring(y + 2 + t - (t // 2) * (2 * t - 1))
        span = pl.ds(t * 2 * half, 2 * half)
        return (pltpu.make_async_copy(q_h.at[dest], qs_v.at[t], self_sem.at[0, t]),
                pltpu.make_async_copy(ks_h.at[dest], kc_v.at[span], self_sem.at[1, t]),
                pltpu.make_async_copy(vs_h.at[dest], vc_v.at[span], self_sem.at[2, t]))

    hid_cp = pltpu.make_async_copy(hid_h.at[y * 2 + c], hrow, ld_sem.at[1])
    xv_cp = pltpu.make_async_copy(xv_h.at[y], xv_v, ld_sem.at[2])

    def cols(h, v, k, j):
        return pltpu.make_async_copy(h.at[:, pl.ds(pl.multiple_of(j * cw, 128), cw)], v.at[j], w_sem.at[k, j])

    def rows(h, v, k, j):
        return pltpu.make_async_copy(h.at[pl.ds(pl.multiple_of(j * cw, 128), cw)], v.at[j], w_sem.at[k, j])

    def ld_wo(j):
        return cols(wo_h, wo_v, 0, j)

    def ld_wg(j):
        return rows(wg_h, wg_v, 1, j)

    def ld_wu(j):
        return rows(wu_h, wu_v, 2, j)

    def ld_wd(j):
        return cols(wd_h, wd_v, 3, j)

    def ld_cq(j):
        return rows(cq_h, cq_v, 4, j)

    def ld_cwo(j):
        return cols(cwo_h, cwo_v, 5, j)

    def ld_cg(j):
        return rows(cg_h, wg_v, 6, j)

    def ld_cu(j):
        return rows(cu_h, wu_v, 7, j)

    def ld_cd(j):
        return cols(cd_h, wd_v, 8, j)

    def ld_kc(g):
        return pltpu.make_async_copy(kc_h.at[y, pl.ds(g * 8 * per, 8 * per)], kc_v.at[pl.ds(g * 8 * per, 8 * per)], kv_sem.at[0, g])

    def ld_vc(g):
        return pltpu.make_async_copy(vc_h.at[y, pl.ds(g * 8 * per, 8 * per)], vc_v.at[pl.ds(g * 8 * per, 8 * per)], kv_sem.at[1, g])

    def start_self(t):
        for cp in ld_self(t):
            cp.start()

    loop(4, start_self)
    barrier = pltpu.get_barrier_semaphore()
    for dev in (sib, xdev(1), xdev(2), xdev(-1), ydev(1), ydev(2), ydev(-1)):
        pl.semaphore_signal(barrier, inc=1, device_id=dev, device_id_type=MESH)
    hid_cp.start()
    xv_cp.start()
    loop(NC, lambda j: ld_wo(j).start())

    def start_gu(j):
        ld_wg(j).start()
        ld_wu(j).start()

    def start_kv(g):
        ld_kc(g).start()
        ld_vc(g).start()

    def start_bulk():
        loop(NC, start_gu)
        loop(NC, lambda j: ld_wd(j).start())
        loop(NC, lambda j: ld_cq(j).start())
        loop(8 - free, lambda g: start_kv(g + free))
        loop(NC, lambda j: ld_cwo(j).start())

    q3[...] = jnp.zeros_like(q3)
    nrow = rowm_v.shape[1]
    mine = (y * 2 + c) * half + lax.broadcasted_iota(jnp.int32, (half, nrow), 0)
    pick = lax.broadcasted_iota(jnp.int32, (half, nrow), 1) == mine
    rmask = jnp.sum(jnp.where(pick, jnp.broadcast_to(rowm_v[...], (half, nrow)), 0).astype(jnp.float32), axis=1, keepdims=True)
    for k in range(2):
        fac[k] = (jnp.tanh(jnp.full((half, 128), gate_s[k], jnp.float32)) * rmask).reshape(4, 8, 128)
    pl.semaphore_wait(barrier, 7)

    lane = lax.broadcasted_iota(jnp.int32, (half, hd), 1)

    def merge(a, b):
        outs, ms, ls = [], [], []
        for h in range(heads):
            ma, mb = a[:, hw + h:hw + h + 1], b[:, hw + h:hw + h + 1]
            la, lb = a[:, hw + 8 + h:hw + 9 + h], b[:, hw + 8 + h:hw + 9 + h]
            mm = jnp.maximum(ma, mb)
            ea, eb = jnp.exp(ma - mm), jnp.exp(mb - mm)
            outs.append(a[:, h * hd:(h + 1) * hd] * ea + b[:, h * hd:(h + 1) * hd] * eb)
            ms.append(mm)
            ls.append(la * ea + lb * eb)
        stat = jnp.zeros((half, hd), jnp.float32)
        for h in range(heads):
            stat = jnp.where(lane == h, ms[h], stat)
            stat = jnp.where(lane == 8 + h, ls[h], stat)
        return jnp.concatenate(outs + [stat], axis=1), ls

    def y_relay(j, d):
        return rcopy(bk.at[ring(y + 2), j], yr.at[j], ys.at[0, j], yrs.at[0, j], ydev(d))

    def y_direct(j, d):
        return rcopy(bk.at[ring(y - d), j], yd.at[j], ys.at[1, j], yrs.at[1, j], ydev(-d))

    def y_final(j, d):
        return rcopy(yt.at[j], yf.at[j], ys.at[2, j], yrs.at[2, j], ydev(d))

    lane8 = lax.broadcasted_iota(jnp.int32, (8, 128), 1)
    sub8 = lax.broadcasted_iota(jnp.int32, (8, 128), 0)
    zero8 = jnp.zeros((8, 128), jnp.float32)
    nseq = 2 * half

    def attend_self(t):
        for cp in ld_self(t):
            cp.wait()
        dest = ring(y + 2 + t - (t // 2) * (2 * t - 1))
        lps = [jnp.minimum(pos_s[dest * nseq + i] - y * slots, slots - 1) for i in range(nseq)]

        def rows4(ref, u):
            return ref[pl.ds(t * nseq + 4 * u, 4)].reshape(4 * slots, hd)

        def scores(us):
            return [lax.dot_general(qs_v[t, 4 * u:4 * u + 4].reshape(32, hd).astype(jnp.bfloat16), rows4(kc_v, u),
                                    (((1,), (1,)), ((), ())), preferred_element_type=jnp.float32) * scale for u in us]

        def soften(us, sgs):
            out = []
            for u, sg in zip(us, sgs):
                probs, stats = [], []
                for i in range(4):
                    off = slots * (i % 2)
                    seen = (lane8 >= off) & (lane8 <= off + lps[4 * u + i])
                    sc = jnp.where(seen, sg[8 * i:8 * i + 8, 128 * (i // 2):128 * (i // 2) + 128], NEG_BIG)
                    mx = jnp.max(sc, axis=1, keepdims=True)
                    pr = jnp.where(seen, jnp.exp(sc - mx), 0.0)
                    ls = jnp.sum(pr, axis=1, keepdims=True)
                    stats.append(jnp.where(lane8 == sub8, mx, jnp.where(lane8 == sub8 + 8, ls, 0.0)))
                    probs.append(jnp.concatenate([pr, zero8] if i < 2 else [zero8, pr], axis=1))
                out.append((jnp.concatenate(probs, axis=0).astype(jnp.bfloat16), stats))
            return out

        def mix(us, prs):
            return [fdot(pg, rows4(vc_v, u)) for u, (pg, _) in zip(us, prs)]

        sets = [range(u, u + 4) for u in range(0, nseq // 4, 4)]
        raw, soft, mixed = [scores(sets[0])], [], []
        for k, us in enumerate(sets):
            if k + 1 < len(sets):
                raw.append(scores(sets[k + 1]))
            soft.append(soften(us, raw[k]))
            mixed += mix(us, soft[k])
        flat = [st for sf in soft for _, st in sf]
        for u, (o, stats) in enumerate(zip(mixed, flat)):
            o3[4 * u:4 * u + 4] = o.reshape(4, 8, hd)
            for i in range(4):
                st3[4 * u + i] = stats[i]
        stat = st3[:, 0, :]
        for h in range(1, heads):
            stat = stat + st3[:, h, :]
        for h in range(heads):
            bk[dest, :, :, h * hd:(h + 1) * hd] = o3[:, h, :].reshape(2, half, hd)
        bk[dest, :, :, hw:] = stat.reshape(2, half, hd)

        @pl.when(t == 0)
        def _():
            y_relay(0, 1).start()
            y_relay(1, -1).start()
            start_bulk()

        @pl.when(t == 1)
        def _():
            y_direct(0, 1).start()

        @pl.when(t == 2)
        def _():
            y_direct(1, -1).start()

    loop(4, attend_self)
    loop(free, start_kv)
    for j, d in ((0, 1), (1, -1)):
        y_relay(j, d).wait_recv()
        yt[j] = merge(bk[ring(y + d), j], yr[j])[0]
        y_final(j, d).start()
    for j, d in ((0, 1), (1, -1)):
        y_direct(j, d).wait_recv()
        first = merge(bk[y, j], yd[j])[0]
        y_final(j, d).wait_recv()
        both, sums = merge(first, yf[j])
        for h in range(heads):
            ob[j * half:(j + 1) * half, h * hd:(h + 1) * hd] = (both[:, h * hd:(h + 1) * hd] / sums[h]).astype(jnp.bfloat16)

    def pair_cp(j):
        return rcopy(pbuf.at[j, 1 - c], dbuf.at[j], pr_s.at[j], pr_r.at[j], sib)

    def mate(j, second):
        odd = lax.rem(j + second, 2)
        return {'tp': 2 * (flip + odd * (cross - flip)) + c}

    def one_cp(p, j):
        return rcopy(s0.at[j], r1.at[p % 2, j], ar_s.at[0, j], ar_r.at[p % 2, 0, j], mate(j, 0))

    def two_cp(p, j):
        return rcopy(s1.at[j], r2.at[p % 2, j], ar_s.at[1, j], ar_r.at[p % 2, 1, j], mate(j, 1))

    def pair_sums(p, partial, after):
        def body(j):
            @pl.when(j < NC)
            def _():
                if p > 0:
                    pair_cp(j).wait_send()
                pbuf[j] = partial(j).reshape(2, half, cw)
                pair_cp(j).start()

            @pl.when(j >= 1)
            def _():
                pair_cp(j - 1).wait_recv()
                if p > 0:
                    one_cp(p, j - 1).wait_send()
                s0[j - 1] = (pbuf[j - 1, c] + dbuf[j - 1]).reshape(4, 8, cw)
                after(j - 1)

        loop(NC + 1, body)

    def all_reduce(p, partial):
        pair_sums(p, partial, lambda j: one_cp(p, j).start())

        def step(j):
            one_cp(p, j).wait_recv()
            if p > 0:
                two_cp(p, j).wait_send()
            s1[j] = s0[j] + r1[p % 2, j]
            two_cp(p, j).start()

        loop(NC, step)

    def new_rows(p, k):
        sq = jnp.zeros((4, 8, 1), jnp.float32)
        for j in range(NC):
            two_cp(p, j).wait_recv()
            add = s1[j] + r2[p % 2, j]
            if k is not None:
                add = fac[k][:, :, :1] * add
            old = hrow[:, :, j * cw:(j + 1) * cw].astype(jnp.float32) if p == 0 else hst[j]
            new = (old + add).astype(jnp.bfloat16).astype(jnp.float32)
            hst[j] = new
            sq = sq + jnp.sum(new * new, axis=2, keepdims=True)
        return sq

    def swap_cp(j):
        return rcopy(xa.at[j, c], xa.at[j, c], xs_s.at[j], xs_r.at[j], sib)

    def all_gather(q, sq, gain_row, consume):
        inv = lax.rsqrt(sq / dim + NORM_EPS)
        rows_of = (g2_v, g3_v, g4_v)[gain_row][...].astype(jnp.float32)
        for j in range(NC):
            gain = jnp.concatenate([rows_of[i:i + 1] for i in range(j * cw // 128, (j + 1) * cw // 128)], axis=1)
            if q > 0:
                swap_cp(j).wait_send()
            xa[j, c] = (hst[j] * inv * gain.reshape(1, 1, cw)).astype(jnp.bfloat16).astype(jnp.float32).reshape(half, cw)
            swap_cp(j).start()

        def body(t):
            swap_cp(2 * t).wait_recv()
            swap_cp(2 * t + 1).wait_recv()
            xs = [xa[2 * t + u].reshape(2 * half, cw).astype(jnp.bfloat16) for u in range(2)]
            consume(t, jnp.concatenate(xs, axis=1))

        loop(NC // 2, body)

    def turn(j):
        return 1 - 2 * lax.rem(j, 2)

    def relay_cp(j):
        return rcopy(s0.at[j, ring(x + 2)], r1.at[1, j, 0], lr_s.at[0, j], lr_r.at[0, j], xdev(turn(j)))

    def direct_cp(j):
        return rcopy(s0.at[j, ring(x - turn(j))], r1.at[1, j, 1], lr_s.at[1, j], lr_r.at[1, j], xdev(-turn(j)))

    def last_cp(j):
        return rcopy(s1.at[j, 0], r1.at[1, j, 2], lr_s.at[2, j], lr_r.at[2, j], xdev(turn(j)))

    def last_scatter(partial):
        def send(j):
            relay_cp(j).start()
            direct_cp(j).start()

        pair_sums(3, partial, send)

        def step(j):
            relay_cp(j).wait_recv()
            two_cp(2, j).wait_send()
            s1[j, 0] = s0[j, ring(x + turn(j))] + r1[1, j, 0]
            last_cp(j).start()

        loop(NC, step)

    def last_rows(j):
        direct_cp(j).wait_recv()
        last_cp(j).wait_recv()
        return s0[j, x] + r1[1, j, 1] + r1[1, j, 2]

    def mlp_hidden(q, sq, gain_row, wait_gu):
        acc[...] = jnp.zeros_like(acc)

        def consume(t, xs):
            wait_gu(2 * t)
            wait_gu(2 * t + 1)
            two = pl.ds(2 * t, 2)
            acc[:, :mlp] += fdot(xs, wg_v[two].reshape(2 * cw, mlp))
            acc[:, mlp:] += fdot(xs, wu_v[two].reshape(2 * cw, mlp))

        all_gather(q, sq, gain_row, consume)
        gv = acc[:, :mlp].astype(jnp.bfloat16).astype(jnp.float32)
        uv = acc[:, mlp:].astype(jnp.bfloat16).astype(jnp.float32)
        act[...] = (jax.nn.silu(gv) * uv).astype(jnp.bfloat16)

    def part_wo(j):
        ld_wo(j).wait()
        return fdot(ob[...], wo_v[j])

    all_reduce(0, part_wo)
    hid_cp.wait()
    sq = new_rows(0, None)

    def wait_self(j):
        ld_wg(j).wait()
        ld_wu(j).wait()

    mlp_hidden(0, sq, 0, wait_self)

    def start_cgu(j):
        ld_cg(j).start()
        ld_cu(j).start()

    loop(NC, start_cgu)

    def part_wd(j):
        ld_wd(j).wait()
        return fdot(act[...], wd_v[j])

    all_reduce(1, part_wd)
    loop(NC, lambda j: ld_cd(j).start())
    sq = new_rows(1, None)

    acc[:, :hw] = jnp.zeros((2 * half, hw), jnp.float32)

    def consume_q(t, xs):
        ld_cq(2 * t).wait()
        ld_cq(2 * t + 1).wait()
        acc[:, :hw] += fdot(xs, cq_v[pl.ds(2 * t, 2)].reshape(2 * cw, hw))

    all_gather(1, sq, 1, consume_q)
    qgain = qn_v[...].astype(jnp.float32)
    for h in range(heads):
        qh = acc[:, h * hd:(h + 1) * hd].astype(jnp.bfloat16).astype(jnp.float32)
        qinv = lax.rsqrt(jnp.mean(qh * qh, axis=1, keepdims=True) + NORM_EPS)
        q3[:, h, :] = (qh * qinv * qgain).astype(jnp.bfloat16).astype(jnp.float32)
    xv_cp.wait()

    nat = 16

    def whole(ref, b):
        return ref[pl.ds(b * per, per)].reshape(ntok, hd)

    def attend(t):
        for u in range(nat // 8):
            ld_kc(t * (nat // 8) + u).wait()
            ld_vc(t * (nat // 8) + u).wait()

        def scores(us):
            return [lax.dot_general(q3[t * nat + u].astype(jnp.bfloat16), whole(kc_v, t * nat + u), (((1,), (1,)), ((), ())),
                                    preferred_element_type=jnp.float32) * scale for u in us]

        def soften(us, scs):
            out = []
            for u, sc in zip(us, scs):
                valid = jnp.broadcast_to(xvs[u // 8][u % 8:u % 8 + 1], (8, ntok)) > 0
                sc = jnp.where(valid, sc, NEG_BIG)
                mx = jnp.max(sc, axis=1, keepdims=True)
                pr = jnp.where(valid, jnp.exp(sc - mx), 0.0)
                out.append((pr.astype(jnp.bfloat16), jnp.sum(pr, axis=1, keepdims=True)))
            return out

        def mix(us, prs):
            return [fdot(pr, whole(vc_v, t * nat + u)) / ls for u, (pr, ls) in zip(us, prs)]

        xvs = [xv_v[pl.ds(pl.multiple_of(t * nat + 8 * u, 8), 8), :] for u in range(nat // 8)]
        one, two = range(nat // 2), range(nat // 2, nat)
        sa = scores(one)
        sb = scores(two)
        oa = mix(one, soften(one, sa))
        o2 = mix(two, soften(two, sb))
        for u, o in enumerate(oa + o2):
            oc[t * nat + u] = o

    loop(2 * half // nat, attend)
    for h in range(heads):
        ob[:, h * hd:(h + 1) * hd] = oc[:, h, :].astype(jnp.bfloat16)

    def part_cwo(j):
        ld_cwo(j).wait()
        return fdot(ob[...], cwo_v[j])

    all_reduce(2, part_cwo)
    sq = new_rows(2, 0)

    def wait_cross(j):
        ld_cg(j).wait()
        ld_cu(j).wait()

    mlp_hidden(2, sq, 2, wait_cross)

    def part_cd(j):
        ld_cd(j).wait()
        return fdot(act[...], wd_v[j])

    last_scatter(part_cd)

    def parts_of(j):
        if j < NC // 2:
            return (lambda k: og.at[j, c, y, ring(x + k)], xdev), (lambda k: og.at[j, c, ring(y + k)], ydev)
        return (lambda k: og.at[j, c, ring(y + k), x], ydev), (lambda k: og.at[j, c, :, ring(x + k)], xdev)

    def fg(j, stage, k, s, what, dev):
        return rcopy(what, what, fg_s.at[j, stage, s], fg_r.at[j, stage, k], dev)

    plans = []
    for j in range(NC):
        d = 1 - 2 * (j % 2)
        stages = []
        for stage, (region, dev) in enumerate(parts_of(j)):
            own = [fg(j, stage, 0, 0, region(0), dev(d)), fg(j, stage, 1, 1, region(0), dev(-d))]
            if stage == 0:
                own.append(fg(j, stage, 2, 2, region(0), dev(2)))
            stages.append(dict(
                own=own,
                relay=[fg(j, stage, 2, 2, region(-d), dev(d))] if stage else [],
                got=[fg(j, stage, 0, 0, region(-d), sib), fg(j, stage, 1, 1, region(d), sib), fg(j, stage, 2, 2, region(2), sib)],
                pair=[fg(j, 2, i, i, region(k), sib) for i, k in enumerate((0, -d, d, 2))] if stage else [],
            ))
        plans.append(stages)
    order = range(NC)
    for j in order:
        og[j, c, y, x] = (hst[j, x] + fac[1, x][:, :1] * last_rows(j)).astype(jnp.bfloat16).astype(jnp.float32)
        for cp in plans[j][0]['own']:
            cp.start()
    for j in order:
        st, nx = plans[j]
        for cp in st['got']:
            cp.wait_recv()
        for cp in nx['own']:
            cp.start()
        nx['pair'][0].start()
    for j in order:
        st = plans[j][1]
        st['got'][0].wait_recv()
        st['relay'][0].start()
        st['pair'][1].start()
        st['got'][1].wait_recv()
        st['pair'][2].start()

    def result_cp(j, cc):
        return pltpu.make_async_copy(og.at[j, cc], out_h.at[:, cc, :, :, j * cw:(j + 1) * cw], out_sem.at[cc, j])

    for j in order:
        st = plans[j][1]
        st['got'][2].wait_recv()
        st['pair'][3].start()
        result_cp(j, c).start()
    for j in order:
        for cp in plans[j][1]['pair']:
            cp.wait_recv()
        result_cp(j, 1 - c).start()

    for j, d in ((0, 1), (1, -1)):
        y_relay(j, d).wait_send()
        y_direct(j, d).wait_send()
        y_final(j, d).wait_send()

    def drain(j):
        pair_cp(j).wait_send()
        swap_cp(j).wait_send()
        relay_cp(j).wait_send()
        direct_cp(j).wait_send()
        last_cp(j).wait_send()

    loop(NC, drain)
    for j in range(NC):
        for st in plans[j]:
            for cp in st['own'] + st['relay'] + st['pair']:
                cp.wait_send()
    for j in order:
        result_cp(j, 0).wait()
        result_cp(j, 1).wait()


def tail(q, ko, vo, new_pos, hidden, gains, rowmask, gates, xvalid, k_cross, v_cross, wo, wg, wu, wd, cq, cwo, cg, cu, cd, heads, hd):
    batch, dim = hidden.shape
    mlp = wg.shape[1]
    ntok = xvalid.shape[1]
    slots = ko.shape[1]
    cw = dim // NC
    hw = heads * hd
    bl = batch // 4
    half = bl // 2
    f32, bf16 = jnp.float32, jnp.bfloat16
    anyspec = pl.BlockSpec(memory_space=pl.ANY)
    vmem = pl.BlockSpec(memory_space=pltpu.VMEM)
    smem = pl.BlockSpec(memory_space=pltpu.SMEM)
    dma = pltpu.SemaphoreType.DMA
    scratch = [
        pltpu.VMEM((4, bl, 8, hd), f32),
        pltpu.VMEM((bl, 8, hd), f32),
        pltpu.VMEM((bl, 8, hd), f32),
        pltpu.VMEM((4, 2, half, hw + hd), f32),
        pltpu.VMEM((2, half, hw + hd), f32),
        pltpu.VMEM((2, half, hw + hd), f32),
        pltpu.VMEM((2, half, hw + hd), f32),
        pltpu.VMEM((2, half, hw + hd), f32),
        pltpu.VMEM((bl, hw), bf16),
        pltpu.VMEM((4, 8, dim), bf16),
        pltpu.VMEM((NC, 4, 8, cw), f32),
        pltpu.VMEM((NC, hw, cw), bf16),
        pltpu.VMEM((NC, cw, mlp), bf16),
        pltpu.VMEM((NC, cw, mlp), bf16),
        pltpu.VMEM((NC, mlp, cw), bf16),
        pltpu.VMEM((NC, cw, hw), bf16),
        pltpu.VMEM((NC, hw, cw), bf16),
        pltpu.VMEM((bl * ntok // slots, slots, hd), bf16),
        pltpu.VMEM((bl * ntok // slots, slots, hd), bf16),
        pltpu.VMEM((bl, ntok), jnp.int32),
        pltpu.VMEM((NC, 2, half, cw), f32),
        pltpu.VMEM((NC, half, cw), f32),
        pltpu.VMEM((NC, 4, 8, cw), f32),
        pltpu.VMEM((NC, 4, 8, cw), f32),
        pltpu.VMEM((2, NC, 4, 8, cw), f32),
        pltpu.VMEM((2, NC, 4, 8, cw), f32),
        pltpu.VMEM((NC, 2, half, cw), f32),
        pltpu.VMEM((NC, 2, 4, 4, 8, cw), f32),
        pltpu.VMEM((bl, 2 * mlp), f32),
        pltpu.VMEM((bl, mlp), bf16),
        pltpu.VMEM((bl, 8, hd), f32),
        pltpu.VMEM((bl, 8, hd), f32),
        pltpu.VMEM((2, 4, 8, 128), f32),
        dma((3,)),
        dma((3, 4)),
        dma((9, NC)),
        dma((2, 8)),
        dma((3, 2)),
        dma((3, 2)),
        dma((NC,)),
        dma((NC,)),
        dma((2, NC)),
        dma((2, 2, NC)),
        dma((3, NC)),
        dma((3, NC)),
        dma((NC,)),
        dma((NC,)),
        dma((NC, 3, 4)),
        dma((NC, 3, 4)),
        dma((2, NC)),
    ]
    out = pl.pallas_call(
        functools.partial(tail_kernel, (heads, hd, dim, mlp, ntok, slots)),
        out_shape=jax.ShapeDtypeStruct((4, 2, 4, 8, dim), f32),
        in_specs=[anyspec] * 3 + [smem, anyspec] + [vmem] * 5 + [smem] + [anyspec] * 12,
        out_specs=anyspec,
        scratch_shapes=scratch,
        compiler_params=pltpu.CompilerParams(collective_id=0, has_side_effects=True, vmem_limit_bytes=67043328),
        name='tail',
    )(q.reshape(4, bl, 8, hd), ko.reshape(4, bl, slots, hd), vo.reshape(4, bl, slots, hd), new_pos, hidden.reshape(8, 4, 8, dim),
      *[g.reshape(-1, 128) for g in gains], rowmask.reshape(1, batch), gates,
      xvalid.reshape(4, bl, ntok), k_cross.reshape(4, bl * ntok // slots, slots, hd), v_cross.reshape(4, bl * ntok // slots, slots, hd),
      wo, wg, wu, wd, cq, cwo, cg, cu, cd)
    return out.reshape(batch, dim).astype(bf16)


def solution(mesh):
    cache_spec = P('dp', 'sp', 'tp', None)
    cross_spec = P('dp', None, 'tp', None)
    row_spec = P('dp', None)
    vec_spec = P('dp')
    full_spec = P(None)
    col_spec = P(None, 'tp')
    split_rows = P('tp', None)
    in_specs = (row_spec, vec_spec, cache_spec, cache_spec, cross_spec, cross_spec, row_spec, vec_spec,
                full_spec, col_spec, col_spec, col_spec, split_rows, full_spec, col_spec, col_spec, split_rows,
                full_spec, col_spec, full_spec, split_rows, full_spec, full_spec, col_spec, col_spec, split_rows)
    out_specs = (row_spec, cache_spec, cache_spec)

    def local_step(hidden, new_pos, k_self, v_self, k_cross, v_cross, xvalid, rowmask,
                   self_attn_norm, self_wq, self_wk, self_wv, self_wo, self_mlp_norm,
                   self_wgate, self_wup, self_wdown, cross_attn_norm, cross_wq, cross_qnorm,
                   cross_wo, cross_gates, cross_mlp_norm, cross_wgate, cross_wup, cross_wdown):
        head_dim = k_self.shape[3]
        heads_local = self_wq.shape[1] // head_dim
        ko, vo, q = front(hidden, new_pos, k_self, v_self, self_attn_norm, self_wq, self_wk, self_wv,
                          heads_local, head_dim)
        gains = (self_mlp_norm, cross_attn_norm, cross_mlp_norm, cross_qnorm)
        h4 = tail(q, ko, vo, new_pos, hidden, gains, rowmask, cross_gates, xvalid, k_cross, v_cross, self_wo, self_wgate, self_wup, self_wdown,
                  cross_wq, cross_wo, cross_wgate, cross_wup, cross_wdown, heads_local, head_dim)
        return h4, ko.reshape(k_self.shape), vo.reshape(v_self.shape)

    return jax.shard_map(local_step, mesh=mesh, in_specs=in_specs, out_specs=out_specs, check_vma=False)
```

```python
import functools
import math
import jax
import jax.numpy as jnp
import numpy as np
from jax import lax
from jax.experimental import pallas as pl
from jax.experimental.pallas import tpu as pltpu
from jax.sharding import PartitionSpec as P

NORM_EPS = 1e-5
ROPE_THETA = 500000.0
ROPE_FACTOR = 8.0
LOW_FREQ = 1.0
HIGH_FREQ = 4.0
ORIG_CTX = 8192.0
NEG_BIG = -1e30
NC = 6
MESH = pl.DeviceIdType.MESH


def rope_freqs(head_dim):
    inv_freq = (1.0 / (ROPE_THETA ** (np.arange(0, head_dim, 2).astype(np.float32) / np.float32(head_dim)))).astype(np.float32)
    wavelen = 2.0 * math.pi / inv_freq
    smooth = (ORIG_CTX / wavelen - LOW_FREQ) / (HIGH_FREQ - LOW_FREQ)
    mid_freq = (1.0 - smooth) * inv_freq / ROPE_FACTOR + smooth * inv_freq
    scaled = np.where(wavelen > ORIG_CTX / LOW_FREQ, inv_freq / ROPE_FACTOR, mid_freq)
    half = np.where(wavelen < ORIG_CTX / HIGH_FREQ, inv_freq, scaled).astype(np.float32)
    return np.concatenate([half, half])[None, :]


def fdot(a, b):
    return jnp.dot(a, b, preferred_element_type=jnp.float32)


def front_kernel(cfg, hid_h, posr_v, pos_s, gain_v, freq_v, wq_h, wk_h, wv_h, k_h, v_h, ko_h, vo_h, q_h,
                 hid_v, xn, wq_v, wkv_v, kc, vc, q3, kn, vn, in_sem, kv_sem, out_sem):
    heads, hd, dim, batch, slots = cfg
    f32, bf16 = jnp.float32, jnp.bfloat16
    per = 32
    nch = batch // per
    nrm = 32
    first_slot = lax.axis_index('sp') * slots

    def loop(n, body):
        def step(i, carry):
            body(i)
            return carry
        lax.fori_loop(0, n, step, 0)

    def ld_hid(r):
        span = pl.ds(pl.multiple_of(r * nrm, nrm), nrm)
        return pltpu.make_async_copy(hid_h.at[span], hid_v.at[span], in_sem.at[3 + r])

    weights = [pltpu.make_async_copy(h, v, in_sem.at[i])
               for i, (h, v) in enumerate(((wq_h, wq_v), (wk_h, wkv_v.at[:, :hd]), (wv_h, wkv_v.at[:, hd:])))]

    def ld_kv(g):
        span = pl.ds(g * per, per)
        return (pltpu.make_async_copy(k_h.at[span], kc.at[span], kv_sem.at[0, g]),
                pltpu.make_async_copy(v_h.at[span], vc.at[span], kv_sem.at[1, g]))

    def st_kv(g):
        span = pl.ds(g * per, per)
        return (pltpu.make_async_copy(kc.at[span], ko_h.at[span], out_sem.at[0, g]),
                pltpu.make_async_copy(vc.at[span], vo_h.at[span], out_sem.at[1, g]))

    def start_both(pair):
        pair[0].start()
        pair[1].start()

    def wait_both(pair):
        pair[0].wait()
        pair[1].wait()

    loop(batch // nrm, lambda r: ld_hid(r).start())
    for cp in weights:
        cp.start()
    loop(nch, lambda g: start_both(ld_kv(g)))
    q3[...] = jnp.zeros_like(q3)

    gain = gain_v[...].astype(f32)

    def norm(r):
        ld_hid(r).wait()
        span = pl.ds(pl.multiple_of(r * nrm, nrm), nrm)
        xs = hid_v[span, :].astype(f32)
        inv = lax.rsqrt(jnp.sum(xs * xs, axis=1, keepdims=True) / dim + NORM_EPS)
        for k in range(dim // 128):
            xn[span, k * 128:(k + 1) * 128] = (xs[:, k * 128:(k + 1) * 128] * inv * gain[k:k + 1]).astype(bf16)

    loop(batch // nrm, norm)
    eye = lax.broadcasted_iota(jnp.int32, (batch, batch), 0) == lax.broadcasted_iota(jnp.int32, (batch, batch), 1)
    posc = jnp.sum(jnp.where(eye, jnp.broadcast_to(posr_v[...], (batch, batch)).astype(f32), 0.0), axis=1, keepdims=True)
    angles = posc * freq_v[...]
    cos_t = jnp.cos(angles)
    low = lax.broadcasted_iota(jnp.int32, (batch, hd), 1) < hd // 2
    sin_t = jnp.where(low, -jnp.sin(angles), jnp.sin(angles))

    def rope(v):
        r = v.astype(bf16).astype(f32)
        return (r * cos_t + pltpu.roll(r, hd // 2, 1) * sin_t).astype(bf16).astype(f32)

    for cp in weights:
        cp.wait()
    q = fdot(xn[...], wq_v[...])
    for h in range(heads):
        q3[:, h, :] = rope(q[:, h * hd:(h + 1) * hd])
    kv = fdot(xn[...], wkv_v[...])
    kn[...] = rope(kv[:, :hd])
    vn[...] = kv[:, hd:].astype(bf16).astype(f32)
    q_cp = pltpu.make_async_copy(q3, q_h, in_sem.at[3 + batch // nrm])
    q_cp.start()
    row16 = lax.broadcasted_iota(jnp.int32, (16, hd), 0)

    def patch(g):
        wait_both(ld_kv(g))
        for i in range(per):
            b = g * per + i
            lp = pos_s[b] - first_slot
            base = pl.multiple_of(lax.shift_left(lax.shift_right_logical(jnp.clip(lp, 0, slots - 1), 4), 4), 16)
            hit = row16 + base == lp
            for ref, new in ((kc, kn), (vc, vn)):
                old = ref[b, pl.ds(base, 16), :].astype(f32)
                fresh = jnp.broadcast_to(new[pl.ds(b, 1), :], (16, hd))
                ref[b, pl.ds(base, 16), :] = jnp.where(hit, fresh, old).astype(bf16)
        start_both(st_kv(g))

    loop(nch, patch)
    q_cp.wait()
    loop(nch, lambda g: wait_both(st_kv(g)))


def front(hidden, new_pos, k_self, v_self, gain, wq, wk, wv, heads, hd):
    batch, dim = hidden.shape
    slots = k_self.shape[1]
    f32, bf16 = jnp.float32, jnp.bfloat16
    anyspec = pl.BlockSpec(memory_space=pl.ANY)
    vmem = pl.BlockSpec(memory_space=pltpu.VMEM)
    smem = pl.BlockSpec(memory_space=pltpu.SMEM)
    dma = pltpu.SemaphoreType.DMA
    nch = batch // 32
    cache = jax.ShapeDtypeStruct((batch, slots, hd), bf16)
    ko, vo, q = pl.pallas_call(
        functools.partial(front_kernel, (heads, hd, dim, batch, slots)),
        out_shape=(cache, cache, jax.ShapeDtypeStruct((batch, 8, hd), f32)),
        in_specs=[anyspec, vmem, smem, vmem, vmem] + [anyspec] * 5,
        out_specs=(anyspec, anyspec, anyspec),
        scratch_shapes=[
            pltpu.VMEM((batch, dim), bf16),
            pltpu.VMEM((batch, dim), bf16),
            pltpu.VMEM(wq.shape, bf16),
            pltpu.VMEM((dim, 2 * hd), bf16),
            pltpu.VMEM((batch, slots, hd), bf16),
            pltpu.VMEM((batch, slots, hd), bf16),
            pltpu.VMEM((batch, 8, hd), f32),
            pltpu.VMEM((batch, hd), f32),
            pltpu.VMEM((batch, hd), f32),
            dma((4 + batch // 32,)),
            dma((2, nch)),
            dma((2, nch)),
        ],
        compiler_params=pltpu.CompilerParams(vmem_limit_bytes=60000000),
        name='front',
    )(hidden, new_pos.reshape(1, batch), new_pos, gain.reshape(dim // 128, 128), jnp.asarray(rope_freqs(hd)),
      wq, wk, wv, k_self.reshape(batch, slots, hd), v_self.reshape(batch, slots, hd))
    return ko, vo, q


def tail_kernel(cfg, q_h, ks_h, vs_h, pos_s, hid_h, g2_v, g3_v, g4_v, qn_v, rowm_v, gate_s, xv_h, kc_h, vc_h,
                wo_h, wg_h, wu_h, wd_h, cq_h, cwo_h, cg_h, cu_h, cd_h, out_v,
                qs_v, o3, st3, bk, yr, yd, yt, yf, ob, hrow, hst,
                wo_v, wg_v, wu_v, wd_v, cq_v, cwo_v, kc_v, vc_v, xv_v,
                pbuf, dbuf, s0, s1, r1, r2, xa, og, acc, act, q3, oc, fac,
                ld_sem, self_sem, w_sem, kv_sem, ys, yrs, pr_s, pr_r, ar_s, ar_r, lr_s, lr_r, xs_s, xs_r, fg_s, fg_r):
    heads, hd, dim, mlp, ntok, slots = cfg
    per = ntok // slots
    free = ks_h.shape[0] * ks_h.shape[1] // per // 8
    cw = dim // NC
    hw = heads * hd
    half = 32
    x = lax.axis_index('tp') // 2
    c = lax.axis_index('tp') % 2
    y = lax.axis_index('sp')
    flip = x + 1 - 2 * lax.rem(x, 2)
    cross = 3 - x
    scale = hd ** -0.5

    def ring(v):
        return lax.rem(v + 8, 4)

    def xdev(d):
        return {'tp': 2 * ring(x + d) + c}

    def ydev(d):
        return {'sp': ring(y + d)}

    sib = {'tp': 2 * x + 1 - c}

    def rcopy(src, dst, ss, rs, dev):
        return pltpu.make_async_remote_copy(src_ref=src, dst_ref=dst, send_sem=ss, recv_sem=rs,
                                            device_id=dev, device_id_type=MESH)

    def loop(n, body):
        def step(i, carry):
            body(i)
            return carry
        lax.fori_loop(0, n, step, 0)

    def ld_self(t):
        dest = ring(y + 2 + t - (t // 2) * (2 * t - 1))
        span = pl.ds(t * 2 * half, 2 * half)
        return (pltpu.make_async_copy(q_h.at[dest], qs_v.at[t], self_sem.at[0, t]),
                pltpu.make_async_copy(ks_h.at[dest], kc_v.at[span], self_sem.at[1, t]),
                pltpu.make_async_copy(vs_h.at[dest], vc_v.at[span], self_sem.at[2, t]))

    hid_cp = pltpu.make_async_copy(hid_h.at[y * 2 + c], hrow, ld_sem.at[1])
    xv_cp = pltpu.make_async_copy(xv_h.at[y], xv_v, ld_sem.at[2])

    def cols(h, v, k, j):
        return pltpu.make_async_copy(h.at[:, pl.ds(pl.multiple_of(j * cw, 128), cw)], v.at[j], w_sem.at[k, j])

    def rows(h, v, k, j):
        return pltpu.make_async_copy(h.at[pl.ds(pl.multiple_of(j * cw, 128), cw)], v.at[j], w_sem.at[k, j])

    def ld_wo(j):
        return cols(wo_h, wo_v, 0, j)

    def ld_wg(j):
        return rows(wg_h, wg_v, 1, j)

    def ld_wu(j):
        return rows(wu_h, wu_v, 2, j)

    def ld_wd(j):
        return cols(wd_h, wd_v, 3, j)

    def ld_cq(j):
        return rows(cq_h, cq_v, 4, j)

    def ld_cwo(j):
        return cols(cwo_h, cwo_v, 5, j)

    def ld_cg(j):
        return rows(cg_h, wg_v, 6, j)

    def ld_cu(j):
        return rows(cu_h, wu_v, 7, j)

    def ld_cd(j):
        return cols(cd_h, wd_v, 8, j)

    def ld_kc(g):
        return pltpu.make_async_copy(kc_h.at[y, pl.ds(g * 8 * per, 8 * per)], kc_v.at[pl.ds(g * 8 * per, 8 * per)], kv_sem.at[0, g])

    def ld_vc(g):
        return pltpu.make_async_copy(vc_h.at[y, pl.ds(g * 8 * per, 8 * per)], vc_v.at[pl.ds(g * 8 * per, 8 * per)], kv_sem.at[1, g])

    def start_self(t):
        for cp in ld_self(t):
            cp.start()

    loop(4, start_self)
    barrier = pltpu.get_barrier_semaphore()
    for dev in (sib, xdev(1), xdev(2), xdev(-1), ydev(1), ydev(2), ydev(-1)):
        pl.semaphore_signal(barrier, inc=1, device_id=dev, device_id_type=MESH)
    hid_cp.start()
    xv_cp.start()
    loop(NC, lambda j: ld_wo(j).start())

    def start_gu(j):
        ld_wg(j).start()
        ld_wu(j).start()

    def start_kv(g):
        ld_kc(g).start()
        ld_vc(g).start()

    def start_bulk():
        loop(NC, start_gu)
        loop(NC, lambda j: ld_wd(j).start())
        loop(NC, lambda j: ld_cq(j).start())
        loop(8 - free, lambda g: start_kv(g + free))
        loop(NC, lambda j: ld_cwo(j).start())

    q3[...] = jnp.zeros_like(q3)
    nrow = rowm_v.shape[1]
    mine = (y * 2 + c) * half + lax.broadcasted_iota(jnp.int32, (half, nrow), 0)
    pick = lax.broadcasted_iota(jnp.int32, (half, nrow), 1) == mine
    rmask = jnp.sum(jnp.where(pick, jnp.broadcast_to(rowm_v[...], (half, nrow)), 0).astype(jnp.float32), axis=1, keepdims=True)
    for k in range(2):
        fac[k] = (jnp.tanh(jnp.full((half, 128), gate_s[k], jnp.float32)) * rmask).reshape(4, 8, 128)
    pl.semaphore_wait(barrier, 7)

    lane = lax.broadcasted_iota(jnp.int32, (half, hd), 1)

    def merge(a, b):
        sa, sb = a[:, hw:], b[:, hw:]
        mm = jnp.maximum(sa, sb)
        ea, eb = jnp.exp(sa - mm), jnp.exp(sb - mm)
        stat = jnp.where(lane < 8, mm, sa * pltpu.roll(ea, 8, 1) + sb * pltpu.roll(eb, 8, 1))
        outs = [a[:, h * hd:(h + 1) * hd] * ea[:, h:h + 1] + b[:, h * hd:(h + 1) * hd] * eb[:, h:h + 1] for h in range(heads)]
        return jnp.concatenate(outs + [stat], axis=1), [stat[:, 8 + h:9 + h] for h in range(heads)]

    def y_relay(j, d):
        return rcopy(bk.at[ring(y + 2), j], yr.at[j], ys.at[0, j], yrs.at[0, j], ydev(d))

    def y_direct(j, d):
        return rcopy(bk.at[ring(y - d), j], yd.at[j], ys.at[1, j], yrs.at[1, j], ydev(-d))

    def y_final(j, d):
        return rcopy(yt.at[j], yf.at[j], ys.at[2, j], yrs.at[2, j], ydev(d))

    lane8 = lax.broadcasted_iota(jnp.int32, (8, 128), 1)
    sub8 = lax.broadcasted_iota(jnp.int32, (8, 128), 0)
    zero8 = jnp.zeros((8, 128), jnp.float32)
    nseq = 2 * half

    def attend_self(t):
        for cp in ld_self(t):
            cp.wait()
        dest = ring(y + 2 + t - (t // 2) * (2 * t - 1))
        lps = [jnp.minimum(pos_s[dest * nseq + i] - y * slots, slots - 1) for i in range(nseq)]

        def rows4(ref, u):
            return ref[pl.ds(t * nseq + 4 * u, 4)].reshape(4 * slots, hd)

        def scores(us):
            return [lax.dot_general(qs_v[t, 4 * u:4 * u + 4].reshape(32, hd).astype(jnp.bfloat16), rows4(kc_v, u),
                                    (((1,), (1,)), ((), ())), preferred_element_type=jnp.float32) * scale for u in us]

        def soften(us, sgs):
            out = []
            for u, sg in zip(us, sgs):
                probs, stats = [], []
                for i in range(4):
                    off = slots * (i % 2)
                    seen = (lane8 >= off) & (lane8 <= off + lps[4 * u + i])
                    sc = jnp.where(seen, sg[8 * i:8 * i + 8, 128 * (i // 2):128 * (i // 2) + 128], NEG_BIG)
                    mx = jnp.max(sc, axis=1, keepdims=True)
                    pr = jnp.where(seen, jnp.exp(sc - mx), 0.0)
                    ls = jnp.sum(pr, axis=1, keepdims=True)
                    stats.append(jnp.where(lane8 == sub8, mx, jnp.where(lane8 == sub8 + 8, ls, 0.0)))
                    probs.append(jnp.concatenate([pr, zero8] if i < 2 else [zero8, pr], axis=1))
                out.append((jnp.concatenate(probs, axis=0).astype(jnp.bfloat16), stats))
            return out

        def mix(us, prs):
            return [fdot(pg, rows4(vc_v, u)) for u, (pg, _) in zip(us, prs)]

        sets = [range(u, u + 4) for u in range(0, nseq // 4, 4)]
        raw, soft, mixed = [scores(sets[0])], [], []
        for k, us in enumerate(sets):
            if k + 1 < len(sets):
                raw.append(scores(sets[k + 1]))
            soft.append(soften(us, raw[k]))
            mixed += mix(us, soft[k])
        flat = [st for sf in soft for _, st in sf]
        for u, (o, stats) in enumerate(zip(mixed, flat)):
            o3[4 * u:4 * u + 4] = o.reshape(4, 8, hd)
            for i in range(4):
                st3[4 * u + i] = stats[i]
        stat = st3[:, 0, :]
        for h in range(1, heads):
            stat = stat + st3[:, h, :]
        for h in range(heads):
            bk[dest, :, :, h * hd:(h + 1) * hd] = o3[:, h, :].reshape(2, half, hd)
        bk[dest, :, :, hw:] = stat.reshape(2, half, hd)

        @pl.when(t == 0)
        def _():
            y_relay(0, 1).start()
            y_relay(1, -1).start()
            start_bulk()

        @pl.when(t == 1)
        def _():
            y_direct(0, 1).start()

        @pl.when(t == 2)
        def _():
            y_direct(1, -1).start()

    loop(4, attend_self)
    loop(free, start_kv)
    for j, d in ((0, 1), (1, -1)):
        y_relay(j, d).wait_recv()
        yt[j] = merge(bk[ring(y + d), j], yr[j])[0]
        y_final(j, d).start()
    for j, d in ((0, 1), (1, -1)):
        y_direct(j, d).wait_recv()
        first = merge(bk[y, j], yd[j])[0]
        y_final(j, d).wait_recv()
        both, sums = merge(first, yf[j])
        for h in range(heads):
            ob[j * half:(j + 1) * half, h * hd:(h + 1) * hd] = (both[:, h * hd:(h + 1) * hd] / sums[h]).astype(jnp.bfloat16)

    def pair_cp(j):
        return rcopy(pbuf.at[j, 1 - c], dbuf.at[j], pr_s.at[j], pr_r.at[j], sib)

    def mate(j, second):
        odd = lax.rem(j + second, 2)
        return {'tp': 2 * (flip + odd * (cross - flip)) + c}

    def one_cp(p, j):
        return rcopy(s0.at[j], r1.at[p % 2, j], ar_s.at[0, j], ar_r.at[p % 2, 0, j], mate(j, 0))

    def two_cp(p, j):
        return rcopy(s1.at[j], r2.at[p % 2, j], ar_s.at[1, j], ar_r.at[p % 2, 1, j], mate(j, 1))

    def pair_sums(p, partial, after):
        def body(j):
            @pl.when(j < NC)
            def _():
                if p > 0:
                    pair_cp(j).wait_send()
                pbuf[j] = partial(j).reshape(2, half, cw)
                pair_cp(j).start()

            @pl.when(j >= 1)
            def _():
                pair_cp(j - 1).wait_recv()
                if p > 0:
                    one_cp(p, j - 1).wait_send()
                s0[j - 1] = (pbuf[j - 1, c] + dbuf[j - 1]).reshape(4, 8, cw)
                after(j - 1)

        loop(NC + 1, body)

    def all_reduce(p, partial):
        pair_sums(p, partial, lambda j: one_cp(p, j).start())

        def step(j):
            one_cp(p, j).wait_recv()
            if p > 0:
                two_cp(p, j).wait_send()
            s1[j] = s0[j] + r1[p % 2, j]
            two_cp(p, j).start()

        loop(NC, step)

    def new_rows(p, k):
        sq = jnp.zeros((4, 8, 1), jnp.float32)
        for j in range(NC):
            two_cp(p, j).wait_recv()
            add = s1[j] + r2[p % 2, j]
            if k is not None:
                add = fac[k][:, :, :1] * add
            old = hrow[:, :, j * cw:(j + 1) * cw].astype(jnp.float32) if p == 0 else hst[j]
            new = (old + add).astype(jnp.bfloat16).astype(jnp.float32)
            hst[j] = new
            sq = sq + jnp.sum(new * new, axis=2, keepdims=True)
        return sq

    def swap_cp(j):
        return rcopy(xa.at[j, c], xa.at[j, c], xs_s.at[j], xs_r.at[j], sib)

    def all_gather(q, sq, gain_row, consume):
        inv = lax.rsqrt(sq / dim + NORM_EPS)
        rows_of = (g2_v, g3_v, g4_v)[gain_row][...].astype(jnp.float32)
        for j in range(NC):
            gain = jnp.concatenate([rows_of[i:i + 1] for i in range(j * cw // 128, (j + 1) * cw // 128)], axis=1)
            if q > 0:
                swap_cp(j).wait_send()
            xa[j, c] = (hst[j] * inv * gain.reshape(1, 1, cw)).astype(jnp.bfloat16).astype(jnp.float32).reshape(half, cw)
            swap_cp(j).start()

        def body(t):
            swap_cp(2 * t).wait_recv()
            swap_cp(2 * t + 1).wait_recv()
            xs = [xa[2 * t + u].reshape(2 * half, cw).astype(jnp.bfloat16) for u in range(2)]
            consume(t, jnp.concatenate(xs, axis=1))

        loop(NC // 2, body)

    def turn(j):
        return 1 - 2 * lax.rem(j, 2)

    def relay_cp(j):
        return rcopy(s0.at[j, ring(x + 2)], r1.at[1, j, 0], lr_s.at[0, j], lr_r.at[0, j], xdev(turn(j)))

    def direct_cp(j):
        return rcopy(s0.at[j, ring(x - turn(j))], r1.at[1, j, 1], lr_s.at[1, j], lr_r.at[1, j], xdev(-turn(j)))

    def last_cp(j):
        return rcopy(s1.at[j, 0], r1.at[1, j, 2], lr_s.at[2, j], lr_r.at[2, j], xdev(turn(j)))

    def last_scatter(partial):
        def send(j):
            relay_cp(j).start()
            direct_cp(j).start()

        pair_sums(3, partial, send)

        def step(j):
            relay_cp(j).wait_recv()
            two_cp(2, j).wait_send()
            s1[j, 0] = s0[j, ring(x + turn(j))] + r1[1, j, 0]
            last_cp(j).start()

        loop(NC, step)

    def last_rows(j):
        direct_cp(j).wait_recv()
        last_cp(j).wait_recv()
        return s0[j, x] + r1[1, j, 1] + r1[1, j, 2]

    def mlp_hidden(q, sq, gain_row, wait_gu):
        acc[...] = jnp.zeros_like(acc)

        def consume(t, xs):
            wait_gu(2 * t)
            wait_gu(2 * t + 1)
            two = pl.ds(2 * t, 2)
            acc[:, :mlp] += fdot(xs, wg_v[two].reshape(2 * cw, mlp))
            acc[:, mlp:] += fdot(xs, wu_v[two].reshape(2 * cw, mlp))

        all_gather(q, sq, gain_row, consume)
        gv = acc[:, :mlp].astype(jnp.bfloat16).astype(jnp.float32)
        uv = acc[:, mlp:].astype(jnp.bfloat16).astype(jnp.float32)
        act[...] = (jax.nn.silu(gv) * uv).astype(jnp.bfloat16)

    def part_wo(j):
        ld_wo(j).wait()
        return fdot(ob[...], wo_v[j])

    all_reduce(0, part_wo)
    hid_cp.wait()
    sq = new_rows(0, None)

    def wait_self(j):
        ld_wg(j).wait()
        ld_wu(j).wait()

    mlp_hidden(0, sq, 0, wait_self)

    def start_cgu(j):
        ld_cg(j).start()
        ld_cu(j).start()

    loop(NC, start_cgu)

    def part_wd(j):
        ld_wd(j).wait()
        return fdot(act[...], wd_v[j])

    all_reduce(1, part_wd)
    loop(NC, lambda j: ld_cd(j).start())
    sq = new_rows(1, None)

    acc[:, :hw] = jnp.zeros((2 * half, hw), jnp.float32)

    def consume_q(t, xs):
        ld_cq(2 * t).wait()
        ld_cq(2 * t + 1).wait()
        acc[:, :hw] += fdot(xs, cq_v[pl.ds(2 * t, 2)].reshape(2 * cw, hw))

    all_gather(1, sq, 1, consume_q)
    qgain = qn_v[...].astype(jnp.float32)
    for h in range(heads):
        qh = acc[:, h * hd:(h + 1) * hd].astype(jnp.bfloat16).astype(jnp.float32)
        qinv = lax.rsqrt(jnp.mean(qh * qh, axis=1, keepdims=True) + NORM_EPS)
        q3[:, h, :] = (qh * qinv * qgain).astype(jnp.bfloat16).astype(jnp.float32)
    xv_cp.wait()

    nat = 16

    def whole(ref, b):
        return ref[pl.ds(b * per, per)].reshape(ntok, hd)

    def attend(t):
        for u in range(nat // 8):
            ld_kc(t * (nat // 8) + u).wait()
            ld_vc(t * (nat // 8) + u).wait()

        def scores(us):
            return [lax.dot_general(q3[t * nat + u].astype(jnp.bfloat16), whole(kc_v, t * nat + u), (((1,), (1,)), ((), ())),
                                    preferred_element_type=jnp.float32) * scale for u in us]

        def soften(us, scs):
            out = []
            for u, sc in zip(us, scs):
                valid = jnp.broadcast_to(xvs[u // 8][u % 8:u % 8 + 1], (8, ntok)) > 0
                sc = jnp.where(valid, sc, NEG_BIG)
                mx = jnp.max(sc, axis=1, keepdims=True)
                pr = jnp.where(valid, jnp.exp(sc - mx), 0.0)
                out.append((pr.astype(jnp.bfloat16), jnp.sum(pr, axis=1, keepdims=True)))
            return out

        def mix(us, prs):
            return [fdot(pr, whole(vc_v, t * nat + u)) / ls for u, (pr, ls) in zip(us, prs)]

        xvs = [xv_v[pl.ds(pl.multiple_of(t * nat + 8 * u, 8), 8), :] for u in range(nat // 8)]
        one, two = range(nat // 2), range(nat // 2, nat)
        sa = scores(one)
        sb = scores(two)
        oa = mix(one, soften(one, sa))
        o2 = mix(two, soften(two, sb))
        for u, o in enumerate(oa + o2):
            oc[t * nat + u] = o

    loop(2 * half // nat, attend)
    for h in range(heads):
        ob[:, h * hd:(h + 1) * hd] = oc[:, h, :].astype(jnp.bfloat16)

    def part_cwo(j):
        ld_cwo(j).wait()
        return fdot(ob[...], cwo_v[j])

    all_reduce(2, part_cwo)
    sq = new_rows(2, 0)

    def wait_cross(j):
        ld_cg(j).wait()
        ld_cu(j).wait()

    mlp_hidden(2, sq, 2, wait_cross)

    def part_cd(j):
        ld_cd(j).wait()
        return fdot(act[...], wd_v[j])

    last_scatter(part_cd)

    def parts_of(j):
        if j < NC // 2:
            return (lambda k: og.at[j, c, y, ring(x + k)], xdev), (lambda k: og.at[j, c, ring(y + k)], ydev)
        return (lambda k: og.at[j, c, ring(y + k), x], ydev), (lambda k: og.at[j, c, :, ring(x + k)], xdev)

    def fg(j, stage, k, s, what, dev):
        return rcopy(what, what, fg_s.at[j, stage, s], fg_r.at[j, stage, k], dev)

    plans = []
    for j in range(NC):
        d = 1 - 2 * (j % 2)
        stages = []
        for stage, (region, dev) in enumerate(parts_of(j)):
            own = [fg(j, stage, 0, 0, region(0), dev(d)), fg(j, stage, 1, 1, region(0), dev(-d))]
            if stage == 0:
                own.append(fg(j, stage, 2, 2, region(0), dev(2)))
            stages.append(dict(
                own=own,
                relay=[fg(j, stage, 2, 2, region(-d), dev(d))] if stage else [],
                got=[fg(j, stage, 0, 0, region(-d), sib), fg(j, stage, 1, 1, region(d), sib), fg(j, stage, 2, 2, region(2), sib)],
                pair=[fg(j, 2, i, i, region(k), sib) for i, k in enumerate((0, -d, d, 2))] if stage else [],
            ))
        plans.append(stages)
    order = range(NC)
    for j in order:
        og[j, c, y, x] = (hst[j, x] + fac[1, x][:, :1] * last_rows(j)).astype(jnp.bfloat16).astype(jnp.float32)
        for cp in plans[j][0]['own']:
            cp.start()
    for j in order:
        st, nx = plans[j]
        for cp in st['got']:
            cp.wait_recv()
        for cp in nx['own']:
            cp.start()
        nx['pair'][0].start()
    for j in order:
        st = plans[j][1]
        st['got'][0].wait_recv()
        st['relay'][0].start()
        st['pair'][1].start()
        st['got'][1].wait_recv()
        st['pair'][2].start()

    def result(j, cc):
        for yy in range(4):
            out_v[yy * 8 + cc * 4:yy * 8 + cc * 4 + 4, :, j * cw:(j + 1) * cw] = og[j, cc, yy].astype(jnp.bfloat16)

    for j in order:
        st = plans[j][1]
        st['got'][2].wait_recv()
        st['pair'][3].start()
    for j in order:
        for cp in plans[j][1]['pair']:
            cp.wait_recv()
        result(j, 0)
        result(j, 1)

    for j, d in ((0, 1), (1, -1)):
        y_relay(j, d).wait_send()
        y_direct(j, d).wait_send()
        y_final(j, d).wait_send()

    def drain(j):
        pair_cp(j).wait_send()
        swap_cp(j).wait_send()
        relay_cp(j).wait_send()
        direct_cp(j).wait_send()
        last_cp(j).wait_send()

    loop(NC, drain)
    for j in range(NC):
        for st in plans[j]:
            for cp in st['own'] + st['relay'] + st['pair']:
                cp.wait_send()


def tail(q, ko, vo, new_pos, hidden, gains, rowmask, gates, xvalid, k_cross, v_cross, wo, wg, wu, wd, cq, cwo, cg, cu, cd, heads, hd):
    batch, dim = hidden.shape
    mlp = wg.shape[1]
    ntok = xvalid.shape[1]
    slots = ko.shape[1]
    cw = dim // NC
    hw = heads * hd
    bl = batch // 4
    half = bl // 2
    f32, bf16 = jnp.float32, jnp.bfloat16
    anyspec = pl.BlockSpec(memory_space=pl.ANY)
    vmem = pl.BlockSpec(memory_space=pltpu.VMEM)
    smem = pl.BlockSpec(memory_space=pltpu.SMEM)
    dma = pltpu.SemaphoreType.DMA
    scratch = [
        pltpu.VMEM((4, bl, 8, hd), f32),
        pltpu.VMEM((bl, 8, hd), f32),
        pltpu.VMEM((bl, 8, hd), f32),
        pltpu.VMEM((4, 2, half, hw + hd), f32),
        pltpu.VMEM((2, half, hw + hd), f32),
        pltpu.VMEM((2, half, hw + hd), f32),
        pltpu.VMEM((2, half, hw + hd), f32),
        pltpu.VMEM((2, half, hw + hd), f32),
        pltpu.VMEM((bl, hw), bf16),
        pltpu.VMEM((4, 8, dim), bf16),
        pltpu.VMEM((NC, 4, 8, cw), f32),
        pltpu.VMEM((NC, hw, cw), bf16),
        pltpu.VMEM((NC, cw, mlp), bf16),
        pltpu.VMEM((NC, cw, mlp), bf16),
        pltpu.VMEM((NC, mlp, cw), bf16),
        pltpu.VMEM((NC, cw, hw), bf16),
        pltpu.VMEM((NC, hw, cw), bf16),
        pltpu.VMEM((bl * ntok // slots, slots, hd), bf16),
        pltpu.VMEM((bl * ntok // slots, slots, hd), bf16),
        pltpu.VMEM((bl, ntok), jnp.int32),
        pltpu.VMEM((NC, 2, half, cw), f32),
        pltpu.VMEM((NC, half, cw), f32),
        pltpu.VMEM((NC, 4, 8, cw), f32),
        pltpu.VMEM((NC, 4, 8, cw), f32),
        pltpu.VMEM((2, NC, 4, 8, cw), f32),
        pltpu.VMEM((2, NC, 4, 8, cw), f32),
        pltpu.VMEM((NC, 2, half, cw), f32),
        pltpu.VMEM((NC, 2, 4, 4, 8, cw), f32),
        pltpu.VMEM((bl, 2 * mlp), f32),
        pltpu.VMEM((bl, mlp), bf16),
        pltpu.VMEM((bl, 8, hd), f32),
        pltpu.VMEM((bl, 8, hd), f32),
        pltpu.VMEM((2, 4, 8, 128), f32),
        dma((3,)),
        dma((3, 4)),
        dma((9, NC)),
        dma((2, 8)),
        dma((3, 2)),
        dma((3, 2)),
        dma((NC,)),
        dma((NC,)),
        dma((2, NC)),
        dma((2, 2, NC)),
        dma((3, NC)),
        dma((3, NC)),
        dma((NC,)),
        dma((NC,)),
        dma((NC, 3, 4)),
        dma((NC, 3, 4)),
    ]
    out = pl.pallas_call(
        functools.partial(tail_kernel, (heads, hd, dim, mlp, ntok, slots)),
        out_shape=pltpu.VMEM((batch // 8, 8, dim), bf16),
        in_specs=[anyspec] * 3 + [smem, anyspec] + [vmem] * 5 + [smem] + [anyspec] * 12,
        out_specs=vmem,
        scratch_shapes=scratch,
        compiler_params=pltpu.CompilerParams(collective_id=0, has_side_effects=True, vmem_limit_bytes=61000000),
        name='tail',
    )(q.reshape(4, bl, 8, hd), ko.reshape(4, bl, slots, hd), vo.reshape(4, bl, slots, hd), new_pos, hidden.reshape(8, 4, 8, dim),
      *[g.reshape(-1, 128) for g in gains], rowmask.reshape(1, batch), gates,
      xvalid.reshape(4, bl, ntok), k_cross.reshape(4, bl * ntok // slots, slots, hd), v_cross.reshape(4, bl * ntok // slots, slots, hd),
      wo, wg, wu, wd, cq, cwo, cg, cu, cd)
    return out.reshape(batch, dim)


def solution(mesh):
    cache_spec = P('dp', 'sp', 'tp', None)
    cross_spec = P('dp', None, 'tp', None)
    row_spec = P('dp', None)
    vec_spec = P('dp')
    full_spec = P(None)
    col_spec = P(None, 'tp')
    split_rows = P('tp', None)
    in_specs = (row_spec, vec_spec, cache_spec, cache_spec, cross_spec, cross_spec, row_spec, vec_spec,
                full_spec, col_spec, col_spec, col_spec, split_rows, full_spec, col_spec, col_spec, split_rows,
                full_spec, col_spec, full_spec, split_rows, full_spec, full_spec, col_spec, col_spec, split_rows)
    out_specs = (row_spec, cache_spec, cache_spec)

    def local_step(hidden, new_pos, k_self, v_self, k_cross, v_cross, xvalid, rowmask,
                   self_attn_norm, self_wq, self_wk, self_wv, self_wo, self_mlp_norm,
                   self_wgate, self_wup, self_wdown, cross_attn_norm, cross_wq, cross_qnorm,
                   cross_wo, cross_gates, cross_mlp_norm, cross_wgate, cross_wup, cross_wdown):
        head_dim = k_self.shape[3]
        heads_local = self_wq.shape[1] // head_dim
        ko, vo, q = front(hidden, new_pos, k_self, v_self, self_attn_norm, self_wq, self_wk, self_wv,
                          heads_local, head_dim)
        gains = (self_mlp_norm, cross_attn_norm, cross_mlp_norm, cross_qnorm)
        h4 = tail(q, ko, vo, new_pos, hidden, gains, rowmask, cross_gates, xvalid, k_cross, v_cross, self_wo, self_wgate, self_wup, self_wdown,
                  cross_wq, cross_wo, cross_wgate, cross_wup, cross_wdown, heads_local, head_dim)
        return h4, ko.reshape(k_self.shape), vo.reshape(v_self.shape)

    return jax.shard_map(local_step, mesh=mesh, in_specs=in_specs, out_specs=out_specs, check_vma=False)
```

```python
import functools
import math
import jax
import jax.numpy as jnp
import numpy as np
from jax import lax
from jax.experimental import pallas as pl
from jax.experimental.pallas import tpu as pltpu
from jax.sharding import PartitionSpec as P

NORM_EPS = 1e-5
ROPE_THETA = 500000.0
ROPE_FACTOR = 8.0
LOW_FREQ = 1.0
HIGH_FREQ = 4.0
ORIG_CTX = 8192.0
NEG_BIG = -1e30
NC = 4
MESH = pl.DeviceIdType.MESH


def rope_freqs(head_dim):
    inv_freq = (1.0 / (ROPE_THETA ** (np.arange(0, head_dim, 2).astype(np.float32) / np.float32(head_dim)))).astype(np.float32)
    wavelen = 2.0 * math.pi / inv_freq
    smooth = (ORIG_CTX / wavelen - LOW_FREQ) / (HIGH_FREQ - LOW_FREQ)
    mid_freq = (1.0 - smooth) * inv_freq / ROPE_FACTOR + smooth * inv_freq
    scaled = np.where(wavelen > ORIG_CTX / LOW_FREQ, inv_freq / ROPE_FACTOR, mid_freq)
    half = np.where(wavelen < ORIG_CTX / HIGH_FREQ, inv_freq, scaled).astype(np.float32)
    return np.concatenate([half, half])[None, :]


def fdot(a, b):
    return jnp.dot(a, b, preferred_element_type=jnp.float32)


def front_kernel(cfg, hid_h, posr_v, pos_s, gain_v, freq_v, wq_h, wk_h, wv_h, k_h, v_h, ko_h, vo_h, q_h,
                 hid_v, xn, wq_v, wkv_v, kc, vc, q3, kn, vn, in_sem, kv_sem, out_sem):
    heads, hd, dim, batch, slots = cfg
    f32, bf16 = jnp.float32, jnp.bfloat16
    per = 32
    nch = batch // per
    nrm = 32
    first_slot = lax.axis_index('sp') * slots

    def loop(n, body):
        def step(i, carry):
            body(i)
            return carry
        lax.fori_loop(0, n, step, 0)

    def ld_hid(r):
        span = pl.ds(pl.multiple_of(r * nrm, nrm), nrm)
        return pltpu.make_async_copy(hid_h.at[span], hid_v.at[span], in_sem.at[3 + r])

    weights = [pltpu.make_async_copy(h, v, in_sem.at[i])
               for i, (h, v) in enumerate(((wq_h, wq_v), (wk_h, wkv_v.at[:, :hd]), (wv_h, wkv_v.at[:, hd:])))]

    def ld_kv(g):
        span = pl.ds(g * per, per)
        return (pltpu.make_async_copy(k_h.at[span], kc.at[span], kv_sem.at[0, g]),
                pltpu.make_async_copy(v_h.at[span], vc.at[span], kv_sem.at[1, g]))

    def st_kv(g):
        span = pl.ds(g * per, per)
        return (pltpu.make_async_copy(kc.at[span], ko_h.at[span], out_sem.at[0, g]),
                pltpu.make_async_copy(vc.at[span], vo_h.at[span], out_sem.at[1, g]))

    def start_both(pair):
        pair[0].start()
        pair[1].start()

    def wait_both(pair):
        pair[0].wait()
        pair[1].wait()

    loop(batch // nrm, lambda r: ld_hid(r).start())
    for cp in weights:
        cp.start()
    loop(nch, lambda g: start_both(ld_kv(g)))
    q3[...] = jnp.zeros_like(q3)

    gain = gain_v[...].astype(f32)

    def norm(r):
        ld_hid(r).wait()
        span = pl.ds(pl.multiple_of(r * nrm, nrm), nrm)
        xs = hid_v[span, :].astype(f32)
        inv = lax.rsqrt(jnp.sum(xs * xs, axis=1, keepdims=True) / dim + NORM_EPS)
        for k in range(dim // 128):
            xn[span, k * 128:(k + 1) * 128] = (xs[:, k * 128:(k + 1) * 128] * inv * gain[k:k + 1]).astype(bf16)

    loop(batch // nrm, norm)
    eye = lax.broadcasted_iota(jnp.int32, (batch, batch), 0) == lax.broadcasted_iota(jnp.int32, (batch, batch), 1)
    posc = jnp.sum(jnp.where(eye, jnp.broadcast_to(posr_v[...], (batch, batch)).astype(f32), 0.0), axis=1, keepdims=True)
    angles = posc * freq_v[...]
    cos_t = jnp.cos(angles)
    low = lax.broadcasted_iota(jnp.int32, (batch, hd), 1) < hd // 2
    sin_t = jnp.where(low, -jnp.sin(angles), jnp.sin(angles))

    def rope(v):
        r = v.astype(bf16).astype(f32)
        return (r * cos_t + pltpu.roll(r, hd // 2, 1) * sin_t).astype(bf16).astype(f32)

    for cp in weights:
        cp.wait()
    q = fdot(xn[...], wq_v[...])
    for h in range(heads):
        q3[:, h, :] = rope(q[:, h * hd:(h + 1) * hd])
    kv = fdot(xn[...], wkv_v[...])
    kn[...] = rope(kv[:, :hd])
    vn[...] = kv[:, hd:].astype(bf16).astype(f32)
    q_cp = pltpu.make_async_copy(q3, q_h, in_sem.at[3 + batch // nrm])
    q_cp.start()
    row16 = lax.broadcasted_iota(jnp.int32, (16, hd), 0)

    def patch(g):
        wait_both(ld_kv(g))
        for i in range(per):
            b = g * per + i
            lp = pos_s[b] - first_slot
            base = pl.multiple_of(lax.shift_left(lax.shift_right_logical(jnp.clip(lp, 0, slots - 1), 4), 4), 16)
            hit = row16 + base == lp
            for ref, new in ((kc, kn), (vc, vn)):
                old = ref[b, pl.ds(base, 16), :].astype(f32)
                fresh = jnp.broadcast_to(new[pl.ds(b, 1), :], (16, hd))
                ref[b, pl.ds(base, 16), :] = jnp.where(hit, fresh, old).astype(bf16)
        start_both(st_kv(g))

    loop(nch, patch)
    q_cp.wait()
    loop(nch, lambda g: wait_both(st_kv(g)))


def front(hidden, new_pos, k_self, v_self, gain, wq, wk, wv, heads, hd):
    batch, dim = hidden.shape
    slots = k_self.shape[1]
    f32, bf16 = jnp.float32, jnp.bfloat16
    anyspec = pl.BlockSpec(memory_space=pl.ANY)
    vmem = pl.BlockSpec(memory_space=pltpu.VMEM)
    smem = pl.BlockSpec(memory_space=pltpu.SMEM)
    dma = pltpu.SemaphoreType.DMA
    nch = batch // 32
    cache = jax.ShapeDtypeStruct((batch, slots, hd), bf16)
    ko, vo, q = pl.pallas_call(
        functools.partial(front_kernel, (heads, hd, dim, batch, slots)),
        out_shape=(cache, cache, jax.ShapeDtypeStruct((batch, 8, hd), f32)),
        in_specs=[anyspec, vmem, smem, vmem, vmem] + [anyspec] * 5,
        out_specs=(anyspec, anyspec, anyspec),
        scratch_shapes=[
            pltpu.VMEM((batch, dim), bf16),
            pltpu.VMEM((batch, dim), bf16),
            pltpu.VMEM(wq.shape, bf16),
            pltpu.VMEM((dim, 2 * hd), bf16),
            pltpu.VMEM((batch, slots, hd), bf16),
            pltpu.VMEM((batch, slots, hd), bf16),
            pltpu.VMEM((batch, 8, hd), f32),
            pltpu.VMEM((batch, hd), f32),
            pltpu.VMEM((batch, hd), f32),
            dma((4 + batch // 32,)),
            dma((2, nch)),
            dma((2, nch)),
        ],
        compiler_params=pltpu.CompilerParams(vmem_limit_bytes=60000000),
        name='front',
    )(hidden, new_pos.reshape(1, batch), new_pos, gain.reshape(dim // 128, 128), jnp.asarray(rope_freqs(hd)),
      wq, wk, wv, k_self.reshape(batch, slots, hd), v_self.reshape(batch, slots, hd))
    return ko, vo, q


def tail_kernel(cfg, q_h, ks_h, vs_h, pos_s, hid_h, g2_v, g3_v, g4_v, qn_v, rowm_v, gate_s, xv_h, kc_h, vc_h,
                wo_h, wg_h, wu_h, wd_h, cq_h, cwo_h, cg_h, cu_h, cd_h, out_v,
                qs_v, o3, st3, bk, yr, yd, yt, yf, ob, hrow, hst,
                wo_v, wg_v, wu_v, wd_v, cq_v, cwo_v, kc_v, vc_v, xv_v,
                pbuf, dbuf, s0, s1, r1, r2, xa, og, acc, act, q3, oc, fac,
                ld_sem, self_sem, w_sem, kv_sem, ys, yrs, pr_s, pr_r, ar_s, ar_r, lr_s, lr_r, xs_s, xs_r, fg_s, fg_r):
    heads, hd, dim, mlp, ntok, slots = cfg
    per = ntok // slots
    free = ks_h.shape[0] * ks_h.shape[1] // per // 8
    cw = dim // NC
    hw = heads * hd
    half = 32
    x = lax.axis_index('tp') // 2
    c = lax.axis_index('tp') % 2
    y = lax.axis_index('sp')
    flip = x + 1 - 2 * lax.rem(x, 2)
    cross = 3 - x
    scale = hd ** -0.5

    def ring(v):
        return lax.rem(v + 8, 4)

    def xdev(d):
        return {'tp': 2 * ring(x + d) + c}

    def ydev(d):
        return {'sp': ring(y + d)}

    sib = {'tp': 2 * x + 1 - c}

    def rcopy(src, dst, ss, rs, dev):
        return pltpu.make_async_remote_copy(src_ref=src, dst_ref=dst, send_sem=ss, recv_sem=rs,
                                            device_id=dev, device_id_type=MESH)

    def loop(n, body):
        def step(i, carry):
            body(i)
            return carry
        lax.fori_loop(0, n, step, 0)

    def ld_self(t):
        dest = ring(y + 2 + t - (t // 2) * (2 * t - 1))
        span = pl.ds(t * 2 * half, 2 * half)
        return (pltpu.make_async_copy(q_h.at[dest], qs_v.at[t], self_sem.at[0, t]),
                pltpu.make_async_copy(ks_h.at[dest], kc_v.at[span], self_sem.at[1, t]),
                pltpu.make_async_copy(vs_h.at[dest], vc_v.at[span], self_sem.at[2, t]))

    hid_cp = pltpu.make_async_copy(hid_h.at[y * 2 + c], hrow, ld_sem.at[1])
    xv_cp = pltpu.make_async_copy(xv_h.at[y], xv_v, ld_sem.at[2])

    def cols(h, v, k, j):
        return pltpu.make_async_copy(h.at[:, pl.ds(pl.multiple_of(j * cw, 128), cw)], v.at[j], w_sem.at[k, j])

    def rows(h, v, k, j):
        return pltpu.make_async_copy(h.at[pl.ds(pl.multiple_of(j * cw, 128), cw)], v.at[j], w_sem.at[k, j])

    def ld_wo(j):
        return cols(wo_h, wo_v, 0, j)

    def ld_wg(j):
        return rows(wg_h, wg_v, 1, j)

    def ld_wu(j):
        return rows(wu_h, wu_v, 2, j)

    def ld_wd(j):
        return cols(wd_h, wd_v, 3, j)

    def ld_cq(j):
        return rows(cq_h, cq_v, 4, j)

    def ld_cwo(j):
        return cols(cwo_h, cwo_v, 5, j)

    def ld_cg(j):
        return rows(cg_h, wg_v, 1, j)

    def ld_cu(j):
        return rows(cu_h, wu_v, 2, j)

    def ld_cd(j):
        return cols(cd_h, wd_v, 3, j)

    def ld_kc(g):
        return pltpu.make_async_copy(kc_h.at[y, pl.ds(g * 8 * per, 8 * per)], kc_v.at[pl.ds(g * 8 * per, 8 * per)], kv_sem.at[0, g])

    def ld_vc(g):
        return pltpu.make_async_copy(vc_h.at[y, pl.ds(g * 8 * per, 8 * per)], vc_v.at[pl.ds(g * 8 * per, 8 * per)], kv_sem.at[1, g])

    def start_self(t):
        for cp in ld_self(t):
            cp.start()

    loop(4, start_self)
    barrier = pltpu.get_barrier_semaphore()
    for dev in (sib, xdev(1), xdev(2), xdev(-1), ydev(1), ydev(2), ydev(-1)):
        pl.semaphore_signal(barrier, inc=1, device_id=dev, device_id_type=MESH)
    hid_cp.start()
    xv_cp.start()
    loop(NC, lambda j: ld_wo(j).start())

    def start_gu(j):
        ld_wg(j).start()
        ld_wu(j).start()

    def start_kv(g):
        ld_kc(g).start()
        ld_vc(g).start()

    def start_bulk():
        loop(NC, start_gu)
        loop(NC, lambda j: ld_wd(j).start())
        loop(NC, lambda j: ld_cq(j).start())
        loop(8 - free, lambda g: start_kv(g + free))
        loop(NC, lambda j: ld_cwo(j).start())

    q3[...] = jnp.zeros_like(q3)
    nrow = rowm_v.shape[1]
    mine = (y * 2 + c) * half + lax.broadcasted_iota(jnp.int32, (half, nrow), 0)
    pick = lax.broadcasted_iota(jnp.int32, (half, nrow), 1) == mine
    rmask = jnp.sum(jnp.where(pick, jnp.broadcast_to(rowm_v[...], (half, nrow)), 0).astype(jnp.float32), axis=1, keepdims=True)
    for k in range(2):
        fac[k] = (jnp.tanh(jnp.full((half, 128), gate_s[k], jnp.float32)) * rmask).reshape(4, 8, 128)
    pl.semaphore_wait(barrier, 7)

    lane = lax.broadcasted_iota(jnp.int32, (half, hd), 1)

    def merge(a, b):
        sa, sb = a[:, hw:], b[:, hw:]
        mm = jnp.maximum(sa, sb)
        ea, eb = jnp.exp(sa - mm), jnp.exp(sb - mm)
        stat = jnp.where(lane < 8, mm, sa * pltpu.roll(ea, 8, 1) + sb * pltpu.roll(eb, 8, 1))
        outs = [a[:, h * hd:(h + 1) * hd] * ea[:, h:h + 1] + b[:, h * hd:(h + 1) * hd] * eb[:, h:h + 1] for h in range(heads)]
        return jnp.concatenate(outs + [stat], axis=1), [stat[:, 8 + h:9 + h] for h in range(heads)]

    def y_relay(j, d):
        return rcopy(bk.at[ring(y + 2), j], yr.at[j], ys.at[0, j], yrs.at[0, j], ydev(d))

    def y_direct(j, d):
        return rcopy(bk.at[ring(y - d), j], yd.at[j], ys.at[1, j], yrs.at[1, j], ydev(-d))

    def y_final(j, d):
        return rcopy(yt.at[j], yf.at[j], ys.at[2, j], yrs.at[2, j], ydev(d))

    lane8 = lax.broadcasted_iota(jnp.int32, (8, 128), 1)
    sub8 = lax.broadcasted_iota(jnp.int32, (8, 128), 0)
    zero8 = jnp.zeros((8, 128), jnp.float32)
    nseq = 2 * half

    def attend_self(t):
        for cp in ld_self(t):
            cp.wait()
        dest = ring(y + 2 + t - (t // 2) * (2 * t - 1))
        lps = [jnp.minimum(pos_s[dest * nseq + i] - y * slots, slots - 1) for i in range(nseq)]

        def rows4(ref, u):
            return ref[pl.ds(t * nseq + 4 * u, 4)].reshape(4 * slots, hd)

        def scores(us):
            return [lax.dot_general(qs_v[t, 4 * u:4 * u + 4].reshape(32, hd).astype(jnp.bfloat16), rows4(kc_v, u),
                                    (((1,), (1,)), ((), ())), preferred_element_type=jnp.float32) * scale for u in us]

        def soften(us, sgs):
            out = []
            for u, sg in zip(us, sgs):
                probs, stats = [], []
                for i in range(4):
                    off = slots * (i % 2)
                    seen = (lane8 >= off) & (lane8 <= off + lps[4 * u + i])
                    sc = jnp.where(seen, sg[8 * i:8 * i + 8, 128 * (i // 2):128 * (i // 2) + 128], NEG_BIG)
                    mx = jnp.max(sc, axis=1, keepdims=True)
                    pr = jnp.where(seen, jnp.exp(sc - mx), 0.0)
                    ls = jnp.sum(pr, axis=1, keepdims=True)
                    stats.append(jnp.where(lane8 == sub8, mx, jnp.where(lane8 == sub8 + 8, ls, 0.0)))
                    probs.append(jnp.concatenate([pr, zero8] if i < 2 else [zero8, pr], axis=1))
                out.append((jnp.concatenate(probs, axis=0).astype(jnp.bfloat16), stats))
            return out

        def mix(us, prs):
            return [fdot(pg, rows4(vc_v, u)) for u, (pg, _) in zip(us, prs)]

        sets = [range(u, u + 4) for u in range(0, nseq // 4, 4)]
        raw, soft, mixed = [scores(sets[0])], [], []
        for k, us in enumerate(sets):
            if k + 1 < len(sets):
                raw.append(scores(sets[k + 1]))
            soft.append(soften(us, raw[k]))
            mixed += mix(us, soft[k])
        flat = [st for sf in soft for _, st in sf]
        for u, (o, stats) in enumerate(zip(mixed, flat)):
            o3[4 * u:4 * u + 4] = o.reshape(4, 8, hd)
            for i in range(4):
                st3[4 * u + i] = stats[i]
        stat = st3[:, 0, :]
        for h in range(1, heads):
            stat = stat + st3[:, h, :]
        for h in range(heads):
            bk[dest, :, :, h * hd:(h + 1) * hd] = o3[:, h, :].reshape(2, half, hd)
        bk[dest, :, :, hw:] = stat.reshape(2, half, hd)

        @pl.when(t == 0)
        def _():
            y_relay(0, 1).start()
            y_relay(1, -1).start()
            start_bulk()

        @pl.when(t == 1)
        def _():
            y_direct(0, 1).start()

        @pl.when(t == 2)
        def _():
            y_direct(1, -1).start()

    loop(4, attend_self)
    loop(free, start_kv)
    for j, d in ((0, 1), (1, -1)):
        y_relay(j, d).wait_recv()
        yt[j] = merge(bk[ring(y + d), j], yr[j])[0]
        y_final(j, d).start()
    for j, d in ((0, 1), (1, -1)):
        y_direct(j, d).wait_recv()
        first = merge(bk[y, j], yd[j])[0]
        y_final(j, d).wait_recv()
        both, sums = merge(first, yf[j])
        for h in range(heads):
            ob[j * half:(j + 1) * half, h * hd:(h + 1) * hd] = (both[:, h * hd:(h + 1) * hd] / sums[h]).astype(jnp.bfloat16)

    def pair_cp(j):
        return rcopy(pbuf.at[j, 1 - c], dbuf.at[j], pr_s.at[j], pr_r.at[j], sib)

    def mate(j, second):
        odd = lax.rem(j + second, 2)
        return {'tp': 2 * (flip + odd * (cross - flip)) + c}

    def one_cp(p, j):
        return rcopy(s0.at[j], r1.at[p % 2, j], ar_s.at[0, j], ar_r.at[p % 2, 0, j], mate(j, 0))

    def two_cp(p, j):
        return rcopy(s1.at[j], r2.at[p % 2, j], ar_s.at[1, j], ar_r.at[p % 2, 1, j], mate(j, 1))

    def pair_sums(p, partial, after):
        def body(j):
            @pl.when(j < NC)
            def _():
                if p > 0:
                    pair_cp(j).wait_send()
                pbuf[j] = partial(j).reshape(2, half, cw)
                pair_cp(j).start()

            @pl.when(j >= 1)
            def _():
                pair_cp(j - 1).wait_recv()
                if p > 0:
                    one_cp(p, j - 1).wait_send()
                s0[j - 1] = (pbuf[j - 1, c] + dbuf[j - 1]).reshape(4, 8, cw)
                after(j - 1)

        loop(NC + 1, body)

    def all_reduce(p, partial):
        pair_sums(p, partial, lambda j: one_cp(p, j).start())

        def step(j):
            one_cp(p, j).wait_recv()
            if p > 0:
                two_cp(p, j).wait_send()
            s1[j] = s0[j] + r1[p % 2, j]
            two_cp(p, j).start()

        loop(NC, step)

    def new_rows(p, k):
        sq = jnp.zeros((4, 8, 1), jnp.float32)
        for j in range(NC):
            two_cp(p, j).wait_recv()
            add = s1[j] + r2[p % 2, j]
            if k is not None:
                add = fac[k][:, :, :1] * add
            old = hrow[:, :, j * cw:(j + 1) * cw].astype(jnp.float32) if p == 0 else hst[j]
            new = (old + add).astype(jnp.bfloat16).astype(jnp.float32)
            hst[j] = new
            sq = sq + jnp.sum(new * new, axis=2, keepdims=True)
        return sq

    def swap_cp(j):
        return rcopy(xa.at[j, c], xa.at[j, c], xs_s.at[j], xs_r.at[j], sib)

    def all_gather(q, sq, gain_row, consume):
        inv = lax.rsqrt(sq / dim + NORM_EPS)
        rows_of = (g2_v, g3_v, g4_v)[gain_row][...].astype(jnp.float32)
        for j in range(NC):
            gain = jnp.concatenate([rows_of[i:i + 1] for i in range(j * cw // 128, (j + 1) * cw // 128)], axis=1)
            if q > 0:
                swap_cp(j).wait_send()
            xa[j, c] = (hst[j] * inv * gain.reshape(1, 1, cw)).astype(jnp.bfloat16).astype(jnp.float32).reshape(half, cw)
            swap_cp(j).start()

        def body(t):
            swap_cp(2 * t).wait_recv()
            swap_cp(2 * t + 1).wait_recv()
            xs = [xa[2 * t + u].reshape(2 * half, cw).astype(jnp.bfloat16) for u in range(2)]
            consume(t, jnp.concatenate(xs, axis=1))

        loop(NC // 2, body)

    def turn(j):
        return 1 - 2 * lax.rem(j, 2)

    def relay_cp(j):
        return rcopy(s0.at[j, ring(x + 2)], r1.at[1, j, 0], lr_s.at[0, j], lr_r.at[0, j], xdev(turn(j)))

    def direct_cp(j):
        return rcopy(s0.at[j, ring(x - turn(j))], r1.at[1, j, 1], lr_s.at[1, j], lr_r.at[1, j], xdev(-turn(j)))

    def last_cp(j):
        return rcopy(s1.at[j, 0], r1.at[1, j, 2], lr_s.at[2, j], lr_r.at[2, j], xdev(turn(j)))

    def last_scatter(partial):
        def send(j):
            relay_cp(j).start()
            direct_cp(j).start()

        pair_sums(3, partial, send)

        def step(j):
            relay_cp(j).wait_recv()
            two_cp(2, j).wait_send()
            s1[j, 0] = s0[j, ring(x + turn(j))] + r1[1, j, 0]
            last_cp(j).start()

        loop(NC, step)

    def last_rows(j):
        direct_cp(j).wait_recv()
        last_cp(j).wait_recv()
        return s0[j, x] + r1[1, j, 1] + r1[1, j, 2]

    def mlp_hidden(q, sq, gain_row, wait_gu):
        acc[...] = jnp.zeros_like(acc)

        def consume(t, xs):
            wait_gu(2 * t)
            wait_gu(2 * t + 1)
            two = pl.ds(2 * t, 2)
            acc[:, :mlp] += fdot(xs, wg_v[two].reshape(2 * cw, mlp))
            acc[:, mlp:] += fdot(xs, wu_v[two].reshape(2 * cw, mlp))

        all_gather(q, sq, gain_row, consume)
        gv = acc[:, :mlp].astype(jnp.bfloat16).astype(jnp.float32)
        uv = acc[:, mlp:].astype(jnp.bfloat16).astype(jnp.float32)
        act[...] = (jax.nn.silu(gv) * uv).astype(jnp.bfloat16)

    def part_wo(j):
        ld_wo(j).wait()
        return fdot(ob[...], wo_v[j])

    all_reduce(0, part_wo)
    hid_cp.wait()
    sq = new_rows(0, None)

    def wait_self(j):
        ld_wg(j).wait()
        ld_wu(j).wait()

    mlp_hidden(0, sq, 0, wait_self)

    def start_cgu(j):
        ld_cg(j).start()
        ld_cu(j).start()

    loop(NC, start_cgu)

    def part_wd(j):
        ld_wd(j).wait()
        return fdot(act[...], wd_v[j])

    all_reduce(1, part_wd)
    loop(NC, lambda j: ld_cd(j).start())
    sq = new_rows(1, None)

    acc[:, :hw] = jnp.zeros((2 * half, hw), jnp.float32)

    def consume_q(t, xs):
        ld_cq(2 * t).wait()
        ld_cq(2 * t + 1).wait()
        acc[:, :hw] += fdot(xs, cq_v[pl.ds(2 * t, 2)].reshape(2 * cw, hw))

    all_gather(1, sq, 1, consume_q)
    qgain = qn_v[...].astype(jnp.float32)
    for h in range(heads):
        qh = acc[:, h * hd:(h + 1) * hd].astype(jnp.bfloat16).astype(jnp.float32)
        qinv = lax.rsqrt(jnp.mean(qh * qh, axis=1, keepdims=True) + NORM_EPS)
        q3[:, h, :] = (qh * qinv * qgain).astype(jnp.bfloat16).astype(jnp.float32)
    xv_cp.wait()

    nat = 16

    def whole(ref, b):
        return ref[pl.ds(b * per, per)].reshape(ntok, hd)

    def attend(t):
        for u in range(nat // 8):
            ld_kc(t * (nat // 8) + u).wait()
            ld_vc(t * (nat // 8) + u).wait()

        def scores(us):
            return [lax.dot_general(q3[t * nat + u].astype(jnp.bfloat16), whole(kc_v, t * nat + u), (((1,), (1,)), ((), ())),
                                    preferred_element_type=jnp.float32) * scale for u in us]

        def soften(us, scs):
            out = []
            for u, sc in zip(us, scs):
                valid = jnp.broadcast_to(xvs[u // 8][u % 8:u % 8 + 1], (8, ntok)) > 0
                sc = jnp.where(valid, sc, NEG_BIG)
                mx = jnp.max(sc, axis=1, keepdims=True)
                pr = jnp.where(valid, jnp.exp(sc - mx), 0.0)
                out.append((pr.astype(jnp.bfloat16), jnp.sum(pr, axis=1, keepdims=True)))
            return out

        def mix(us, prs):
            return [fdot(pr, whole(vc_v, t * nat + u)) / ls for u, (pr, ls) in zip(us, prs)]

        xvs = [xv_v[pl.ds(pl.multiple_of(t * nat + 8 * u, 8), 8), :] for u in range(nat // 8)]
        one, two = range(nat // 2), range(nat // 2, nat)
        sa = scores(one)
        sb = scores(two)
        oa = mix(one, soften(one, sa))
        o2 = mix(two, soften(two, sb))
        for u, o in enumerate(oa + o2):
            oc[t * nat + u] = o

    loop(2 * half // nat, attend)
    for h in range(heads):
        ob[:, h * hd:(h + 1) * hd] = oc[:, h, :].astype(jnp.bfloat16)

    def part_cwo(j):
        ld_cwo(j).wait()
        return fdot(ob[...], cwo_v[j])

    all_reduce(2, part_cwo)
    sq = new_rows(2, 0)

    def wait_cross(j):
        ld_cg(j).wait()
        ld_cu(j).wait()

    mlp_hidden(2, sq, 2, wait_cross)

    def part_cd(j):
        ld_cd(j).wait()
        return fdot(act[...], wd_v[j])

    last_scatter(part_cd)

    def parts_of(j):
        if j < NC // 2:
            return (lambda k: og.at[j, c, y, ring(x + k)], xdev), (lambda k: og.at[j, c, ring(y + k)], ydev)
        return (lambda k: og.at[j, c, ring(y + k), x], ydev), (lambda k: og.at[j, c, :, ring(x + k)], xdev)

    def fg(j, stage, k, s, what, dev):
        return rcopy(what, what, fg_s.at[j, 3 * stage + s], fg_r.at[j, 3 * stage + k], dev)

    plans = []
    for j in range(NC):
        d = 1 - 2 * (j % 2)
        stages = []
        for stage, (region, dev) in enumerate(parts_of(j)):
            own = [fg(j, stage, 0, 0, region(0), dev(d)), fg(j, stage, 1, 1, region(0), dev(-d))]
            if stage == 0:
                own.append(fg(j, stage, 2, 2, region(0), dev(2)))
            stages.append(dict(
                own=own,
                relay=[fg(j, stage, 2, 2, region(-d), dev(d))] if stage else [],
                got=[fg(j, stage, 0, 0, region(-d), sib), fg(j, stage, 1, 1, region(d), sib), fg(j, stage, 2, 2, region(2), sib)],
                pair=[fg(j, 2, i, i, region(k), sib) for i, k in enumerate((0, -d, d, 2))] if stage else [],
            ))
        plans.append(stages)
    order = range(NC)
    for j in order:
        og[j, c, y, x] = (hst[j, x] + fac[1, x][:, :1] * last_rows(j)).astype(jnp.bfloat16).astype(jnp.float32)
        for cp in plans[j][0]['own']:
            cp.start()
    for j in order:
        st, nx = plans[j]
        for cp in st['got']:
            cp.wait_recv()
        for cp in nx['own']:
            cp.start()
        nx['pair'][0].start()
    for j in order:
        st = plans[j][1]
        st['got'][0].wait_recv()
        st['relay'][0].start()
        st['pair'][1].start()
        st['got'][1].wait_recv()
        st['pair'][2].start()

    def result(j, cc):
        for yy in range(4):
            out_v[yy * 8 + cc * 4:yy * 8 + cc * 4 + 4, :, j * cw:(j + 1) * cw] = og[j, cc, yy].astype(jnp.bfloat16)

    for j in order:
        st = plans[j][1]
        st['got'][2].wait_recv()
        st['pair'][3].start()
    for j in order:
        for cp in plans[j][1]['pair']:
            cp.wait_recv()
        result(j, 0)
        result(j, 1)

    for j, d in ((0, 1), (1, -1)):
        y_relay(j, d).wait_send()
        y_direct(j, d).wait_send()
        y_final(j, d).wait_send()

    def drain(j):
        pair_cp(j).wait_send()
        swap_cp(j).wait_send()
        relay_cp(j).wait_send()
        direct_cp(j).wait_send()
        last_cp(j).wait_send()

    loop(NC, drain)
    for j in range(NC):
        for st in plans[j]:
            for cp in st['own'] + st['relay'] + st['pair']:
                cp.wait_send()


def tail(q, ko, vo, new_pos, hidden, gains, rowmask, gates, xvalid, k_cross, v_cross, wo, wg, wu, wd, cq, cwo, cg, cu, cd, heads, hd):
    batch, dim = hidden.shape
    mlp = wg.shape[1]
    ntok = xvalid.shape[1]
    slots = ko.shape[1]
    cw = dim // NC
    hw = heads * hd
    bl = batch // 4
    half = bl // 2
    f32, bf16 = jnp.float32, jnp.bfloat16
    anyspec = pl.BlockSpec(memory_space=pl.ANY)
    vmem = pl.BlockSpec(memory_space=pltpu.VMEM)
    smem = pl.BlockSpec(memory_space=pltpu.SMEM)
    dma = pltpu.SemaphoreType.DMA
    scratch = [
        pltpu.VMEM((4, bl, 8, hd), f32),
        pltpu.VMEM((bl, 8, hd), f32),
        pltpu.VMEM((bl, 8, hd), f32),
        pltpu.VMEM((4, 2, half, hw + hd), f32),
        pltpu.VMEM((2, half, hw + hd), f32),
        pltpu.VMEM((2, half, hw + hd), f32),
        pltpu.VMEM((2, half, hw + hd), f32),
        pltpu.VMEM((2, half, hw + hd), f32),
        pltpu.VMEM((bl, hw), bf16),
        pltpu.VMEM((4, 8, dim), bf16),
        pltpu.VMEM((NC, 4, 8, cw), f32),
        pltpu.VMEM((NC, hw, cw), bf16),
        pltpu.VMEM((NC, cw, mlp), bf16),
        pltpu.VMEM((NC, cw, mlp), bf16),
        pltpu.VMEM((NC, mlp, cw), bf16),
        pltpu.VMEM((NC, cw, hw), bf16),
        pltpu.VMEM((NC, hw, cw), bf16),
        pltpu.VMEM((bl * ntok // slots, slots, hd), bf16),
        pltpu.VMEM((bl * ntok // slots, slots, hd), bf16),
        pltpu.VMEM((bl, ntok), jnp.int32),
        pltpu.VMEM((NC, 2, half, cw), f32),
        pltpu.VMEM((NC, half, cw), f32),
        pltpu.VMEM((NC, 4, 8, cw), f32),
        pltpu.VMEM((NC, 4, 8, cw), f32),
        pltpu.VMEM((2, NC, 4, 8, cw), f32),
        pltpu.VMEM((2, NC, 4, 8, cw), f32),
        pltpu.VMEM((NC, 2, half, cw), f32),
        pltpu.VMEM((NC, 2, 4, 4, 8, cw), f32),
        pltpu.VMEM((bl, 2 * mlp), f32),
        pltpu.VMEM((bl, mlp), bf16),
        pltpu.VMEM((bl, 8, hd), f32),
        pltpu.VMEM((bl, 8, hd), f32),
        pltpu.VMEM((2, 4, 8, 128), f32),
        dma((3,)),
        dma((3, 4)),
        dma((6, NC)),
        dma((2, 8)),
        dma((3, 2)),
        dma((3, 2)),
        dma((NC,)),
        dma((NC,)),
        dma((2, NC)),
        dma((2, 2, NC)),
        dma((3, NC)),
        dma((3, NC)),
        dma((NC,)),
        dma((NC,)),
        dma((NC, 10)),
        dma((NC, 10)),
    ]
    out = pl.pallas_call(
        functools.partial(tail_kernel, (heads, hd, dim, mlp, ntok, slots)),
        out_shape=pltpu.VMEM((batch // 8, 8, dim), bf16),
        in_specs=[anyspec] * 3 + [smem, anyspec] + [vmem] * 5 + [smem] + [anyspec] * 12,
        out_specs=vmem,
        scratch_shapes=scratch,
        compiler_params=pltpu.CompilerParams(collective_id=0, has_side_effects=True, vmem_limit_bytes=61000000),
        name='tail',
    )(q.reshape(4, bl, 8, hd), ko.reshape(4, bl, slots, hd), vo.reshape(4, bl, slots, hd), new_pos, hidden.reshape(8, 4, 8, dim),
      *[g.reshape(-1, 128) for g in gains], rowmask.reshape(1, batch), gates,
      xvalid.reshape(4, bl, ntok), k_cross.reshape(4, bl * ntok // slots, slots, hd), v_cross.reshape(4, bl * ntok // slots, slots, hd),
      wo, wg, wu, wd, cq, cwo, cg, cu, cd)
    return out.reshape(batch, dim)


def solution(mesh):
    cache_spec = P('dp', 'sp', 'tp', None)
    cross_spec = P('dp', None, 'tp', None)
    row_spec = P('dp', None)
    vec_spec = P('dp')
    full_spec = P(None)
    col_spec = P(None, 'tp')
    split_rows = P('tp', None)
    in_specs = (row_spec, vec_spec, cache_spec, cache_spec, cross_spec, cross_spec, row_spec, vec_spec,
                full_spec, col_spec, col_spec, col_spec, split_rows, full_spec, col_spec, col_spec, split_rows,
                full_spec, col_spec, full_spec, split_rows, full_spec, full_spec, col_spec, col_spec, split_rows)
    out_specs = (row_spec, cache_spec, cache_spec)

    def local_step(hidden, new_pos, k_self, v_self, k_cross, v_cross, xvalid, rowmask,
                   self_attn_norm, self_wq, self_wk, self_wv, self_wo, self_mlp_norm,
                   self_wgate, self_wup, self_wdown, cross_attn_norm, cross_wq, cross_qnorm,
                   cross_wo, cross_gates, cross_mlp_norm, cross_wgate, cross_wup, cross_wdown):
        head_dim = k_self.shape[3]
        heads_local = self_wq.shape[1] // head_dim
        ko, vo, q = front(hidden, new_pos, k_self, v_self, self_attn_norm, self_wq, self_wk, self_wv,
                          heads_local, head_dim)
        gains = (self_mlp_norm, cross_attn_norm, cross_mlp_norm, cross_qnorm)
        h4 = tail(q, ko, vo, new_pos, hidden, gains, rowmask, cross_gates, xvalid, k_cross, v_cross, self_wo, self_wgate, self_wup, self_wdown,
                  cross_wq, cross_wo, cross_wgate, cross_wup, cross_wdown, heads_local, head_dim)
        return h4, ko.reshape(k_self.shape), vo.reshape(v_self.shape)

    return jax.shard_map(local_step, mesh=mesh, in_specs=in_specs, out_specs=out_specs, check_vma=False)
```
